768 devices in a mesh: gx: 4 (over x), gy: 12 (over z_lo, core), gz: 16 (over z_hi, y).
Axes of the slice: x: 4, y: 8, z: 12 (z_hi: 2, z_lo: 6; z = z_hi * 6 + z_lo), core: 2. Of those that a mesh axis runs over, the one named last changes fastest.
Arguments:
- conserved: float32 [5, 64, 96, 512], P(None, 'gz', 'gy', 'gx'), may hold values from -3 to 12, as said below
- metrics: float32 [9, 64, 96, 512], P(None, 'gz', 'gy', 'gx'), may hold values from -0.6 to 2, as said below
- inv_volume: float32 [64, 96, 512], P('gz', 'gy', 'gx'), may hold values from 0.5 to 2
- wake_donor: int32 [512], P('gx'), may hold values from -1 to 511, as said below
Outputs:
- section_state: float32 [5, 64, 96, 512], P(None, 'gz', 'gy', 'gx')
- time_rate: float32 [5, 64, 96, 512], P(None, 'gz', 'gy', 'gx')
The draws below stay inside these ranges and needn't reach their ends.
Inputs may be any that keep to these rules, and one draw needn't show every extreme that they name: `conserved`: each cell holds density rho of 0.5 to 2, pressure p of 0.5 to 2 and velocity components u of -1.5 to 1.5 as (rho, rho u, p / 0.4 + rho |u|^2 / 2). `metrics`: in each cell, row d (entries 3 d to 3 d + 2) has its entry 3 d + d between 0.5 and 2 and its other two entries at most 0.3 times that entry in magnitude. wake_donor[i] is either 512 - 1 - i or -1, and wake_donor[i] >= 0 exactly where wake_donor[511 - i] >= 0.
All inputs are finite; a program needn't handle non-finite values.
Results may differ from the reference program's by a relative error of at most 0.0001.
Values sent between devices are 32-bit elements; how exact they have to be, the bound alone decides.
A program may use at most 32 MiB of HBM per device.

```python
import math
import jax
import jax.numpy as jnp
from jax import lax

CY = 8
CZ = 4
NX = 512
NY = 96
NZ = 64


def draw_conserved(key, part):
    subkeys = jax.random.split(key, 3)
    grid_shape = (NZ, NY, NX)
    density = jnp.exp(jax.random.uniform(subkeys[0], grid_shape, jnp.float32, -0.6931, 0.6931))
    pressure = jnp.exp(jax.random.uniform(subkeys[1], grid_shape, jnp.float32, -0.6931, 0.6931))
    velocity = jnp.clip(0.5 * jax.random.normal(subkeys[2], (3,) + grid_shape, jnp.float32), -1.5, 1.5)
    energy = pressure / 0.4 + 0.5 * density * jnp.sum(velocity * velocity, axis=0)
    return jnp.concatenate([density[None], density[None] * velocity, energy[None]], axis=0).astype(jnp.float32)


def draw_metrics(key, part):
    subkeys = jax.random.split(key, 2)
    grid_shape = (NZ, NY, NX)
    diagonal = jnp.exp(jax.random.uniform(subkeys[0], (3,) + grid_shape, jnp.float32, -0.6931, 0.6931))
    ratios = jax.random.uniform(subkeys[1], (3, 3) + grid_shape, jnp.float32, -0.3, 0.3)
    entries = []
    for direction in range(3):
        for component in range(3):
            if component == direction:
                entries.append(diagonal[direction])
            else:
                entries.append(ratios[direction, component] * diagonal[direction])
    return jnp.stack(entries).astype(jnp.float32)


def draw_wake_donor(key, part):
    own_key = jax.random.fold_in(key, 4177)
    half_flags = jax.random.randint(own_key, (NX // 2,), 0, 2).astype(jnp.int32)
    flags = jnp.concatenate([half_flags, half_flags[::-1]], axis=0)
    column = jnp.arange(NX, dtype=jnp.int32)
    return jnp.where(flags > 0, NX - 1 - column, -1).astype(jnp.int32)


def steps_of(rng, shape, shards, low, top_value):
    def one(dim, parts):
        steps = jax.random.uniform(jax.random.fold_in(jax.random.fold_in(rng, 6), dim), (parts,), jnp.float32, low / len(shards), top_value / len(shards))
        return jnp.repeat(jnp.exp(steps), shape[dim] // parts).reshape((-1,) + (1,) * (len(shape) - dim - 1))

    gain = one(*shards[0])
    for cut in shards[1:]:
        gain = gain * one(*cut)
    return gain


def setup_inputs(seed: int = 0) -> dict:
    streams_of = jax.random.split(jax.random.key(seed), 5)
    return {
        "conserved": draw_conserved(jax.random.fold_in(streams_of[4], 71), 0),
        "metrics": draw_metrics(jax.random.fold_in(streams_of[4], 71), 0),
        "inv_volume": jnp.clip(jnp.exp(math.log(2.0) - 1.3862944 * jax.random.uniform(streams_of[2], (NZ, NY, NX), jnp.float32) ** steps_of(streams_of[2], (NZ, NY, NX), ((0, 16), (1, 12), (2, 4)), -0.2, 0.2)), 0.5, 2.0),
        "wake_donor": draw_wake_donor(jax.random.fold_in(streams_of[4], 71), 0),
    }


GAMMA = 1.4
WENO_EPS = 1e-06
STEP_SIZE = 0.08

def slab_of(values, start, amount, axis):
    return lax.slice_in_dim(values, start, start + amount, axis=values.ndim + axis)

def cross_of(first, second):
    return [first[1] * second[2] - first[2] * second[1], first[2] * second[0] - first[0] * second[2], first[0] * second[1] - first[1] * second[0]]

def inner_of(first, second):
    return first[0] * second[0] + first[1] * second[1] + first[2] * second[2]

def cell_terms(fields, metric_row):
    density = fields[0]
    velocity = fields[1:4] / density
    kinetic = 0.5 * lax.optimization_barrier(jnp.sum(fields[1:4] * velocity, axis=0))
    pressure = (GAMMA - 1.0) * (fields[4] - kinetic)
    contra = lax.optimization_barrier(jnp.sum(metric_row * velocity, axis=0))
    fluxes = jnp.stack([fields[0] * contra, fields[1] * contra + metric_row[0] * pressure, fields[2] * contra + metric_row[1] * pressure, fields[3] * contra + metric_row[2] * pressure, (fields[4] + pressure) * contra])
    sound_speed = jnp.sqrt(GAMMA * pressure / density)
    speeds = jnp.abs(contra) + sound_speed * jnp.sqrt(lax.optimization_barrier(jnp.sum(metric_row * metric_row, axis=0)))
    primitive = jnp.concatenate([density[None], velocity, pressure[None]], axis=0)
    return (primitive, fluxes, speeds)

def eigen_pair(state, metric_row, pick):
    density = state[0]
    velocity = [state[1], state[2], state[3]]
    pressure = state[4]
    row_size = jnp.sqrt(metric_row[0] ** 2 + metric_row[1] ** 2 + metric_row[2] ** 2)
    normal = [metric_row[member] / row_size for member in range(3)]
    axis_unit = [1.0 if member == pick else 0.0 for member in range(3)]
    raw_cross = cross_of(normal, axis_unit)
    raw_size = jnp.sqrt(raw_cross[0] ** 2 + raw_cross[1] ** 2 + raw_cross[2] ** 2)
    tangent = [raw_cross[member] / raw_size for member in range(3)]
    binormal = cross_of(normal, tangent)
    sound_speed = jnp.sqrt(GAMMA * pressure / density)
    inverse = 1.0 / sound_speed
    kinetic = 0.5 * inner_of(velocity, velocity)
    enthalpy = GAMMA / (GAMMA - 1.0) * pressure / density + kinetic
    normal_speed = inner_of(normal, velocity)
    tangent_speed = inner_of(tangent, velocity)
    binormal_speed = inner_of(binormal, velocity)
    factor = (GAMMA - 1.0) * inverse * inverse
    scaled = factor * kinetic
    left_rows = [[0.5 * (scaled + normal_speed * inverse)] + [0.5 * (-factor * velocity[member] - normal[member] * inverse) for member in range(3)] + [0.5 * factor], [1.0 - scaled] + [factor * velocity[member] for member in range(3)] + [-factor], [-tangent_speed] + tangent + [0.0], [-binormal_speed] + binormal + [0.0], [0.5 * (scaled - normal_speed * inverse)] + [0.5 * (-factor * velocity[member] + normal[member] * inverse) for member in range(3)] + [0.5 * factor]]
    right_columns = [[1.0] + [velocity[member] - sound_speed * normal[member] for member in range(3)] + [enthalpy - sound_speed * normal_speed], [1.0] + velocity + [kinetic], [0.0] + tangent + [tangent_speed], [0.0] + binormal + [binormal_speed], [1.0] + [velocity[member] + sound_speed * normal[member] for member in range(3)] + [enthalpy + sound_speed * normal_speed]]
    return (left_rows, right_columns)

def project_left(matrix, vector):
    return jnp.stack([sum((matrix[member][second] * vector[second] for second in range(5))) for member in range(5)])

def apply_right(matrix, vector):
    return jnp.stack([sum((matrix[second][member] * vector[second] for second in range(5))) for member in range(5)])

def weno_side(stencil):
    far_left, near_left, center, near_right, far_right = stencil
    guess_zero = (2.0 * far_left - 7.0 * near_left + 11.0 * center) / 6.0
    guess_one = (-near_left + 5.0 * center + 2.0 * near_right) / 6.0
    guess_two = (2.0 * center + 5.0 * near_right - far_right) / 6.0
    smooth_zero = 13.0 / 12.0 * (far_left - 2.0 * near_left + center) ** 2 + 0.25 * (far_left - 4.0 * near_left + 3.0 * center) ** 2
    smooth_one = 13.0 / 12.0 * (near_left - 2.0 * center + near_right) ** 2 + 0.25 * (near_left - near_right) ** 2
    smooth_two = 13.0 / 12.0 * (center - 2.0 * near_right + far_right) ** 2 + 0.25 * (3.0 * center - 4.0 * near_right + far_right) ** 2
    weight_zero = 0.1 / (WENO_EPS + smooth_zero) ** 2
    weight_one = 0.6 / (WENO_EPS + smooth_one) ** 2
    weight_two = 0.3 / (WENO_EPS + smooth_two) ** 2
    return (weight_zero * guess_zero + weight_one * guess_one + weight_two * guess_two) / (weight_zero + weight_one + weight_two)

def interface_flux(fields, metric_row, axis, pick):
    primitive, fluxes, speeds = cell_terms(fields, metric_row)
    faces_count = fields.shape[fields.ndim + axis] - 5
    mean_state = 0.5 * (slab_of(primitive, 2, faces_count, axis) + slab_of(primitive, 3, faces_count, axis))
    mean_row = 0.5 * (slab_of(metric_row, 2, faces_count, axis) + slab_of(metric_row, 3, faces_count, axis))
    left_rows, right_columns = eigen_pair(mean_state, mean_row, pick)
    max_speed = slab_of(speeds, 0, faces_count, axis)
    for offset in range(1, 6):
        max_speed = jnp.maximum(max_speed, slab_of(speeds, offset, faces_count, axis))
    upwind = []
    downwind = []
    for offset in range(6):
        state_chars = project_left(left_rows, slab_of(fields, offset, faces_count, axis))
        flux_chars = project_left(left_rows, slab_of(fluxes, offset, faces_count, axis))
        upwind.append(0.5 * (flux_chars + max_speed * state_chars))
        downwind.append(0.5 * (flux_chars - max_speed * state_chars))
    combined = weno_side(upwind[0:5]) + weno_side(downwind[5:0:-1])
    return apply_right(right_columns, combined)

def divergence(fields, metric_row, axis, pick):
    face_flux = interface_flux(fields, metric_row, axis, pick)
    cells_count = face_flux.shape[face_flux.ndim + axis] - 1
    return slab_of(face_flux, 1, cells_count, axis) - slab_of(face_flux, 0, cells_count, axis)

def blocked(fields, metric_row, axis, pick, block_dim, block):
    pieces = fields.shape[block_dim] // block

    def one_block(start):
        flow_part = lax.dynamic_slice_in_dim(fields, start, block, block_dim)
        row_part = lax.dynamic_slice_in_dim(metric_row, start, block, block_dim)
        return divergence(flow_part, row_part, axis, pick)
    starts = jnp.arange(pieces, dtype=jnp.int32) * block
    stacked = lax.map(one_block, starts)
    moved = jnp.moveaxis(stacked, 0, block_dim)
    dims = list(moved.shape)
    merged = dims[:block_dim] + [pieces * block] + dims[block_dim + 2:]
    return moved.reshape(merged)

def reference(conserved, metrics, inv_volume, wake_donor):
    edge_pad = ((0, 0), (0, 0), (0, 0), (3, 3))
    stream_flow = jnp.pad(conserved, edge_pad, mode='edge')
    stream_row = jnp.pad(metrics[0:3], edge_pad, mode='edge')
    momentum_sign = jnp.array([1.0, -1.0, -1.0, -1.0, 1.0], dtype=jnp.float32)[:, None, None, None]
    below_wall = conserved[:, :, 2::-1, :]
    below_row = metrics[3:6, :, 2::-1, :]
    is_wake = wake_donor >= 0
    source_column = jnp.where(is_wake, wake_donor, 0).astype(jnp.int32)
    low_flow = jnp.where(is_wake, jnp.take(below_wall, source_column, axis=3), below_wall * momentum_sign)
    low_row = jnp.where(is_wake, jnp.take(below_row, source_column, axis=3), below_row)
    normal_flow = jnp.concatenate([low_flow, conserved, jnp.repeat(conserved[:, :, -1:, :], 3, axis=2)], axis=2)
    normal_row = jnp.concatenate([low_row, metrics[3:6], jnp.repeat(metrics[3:6, :, -1:, :], 3, axis=2)], axis=2)
    span_flow = jnp.concatenate([conserved[:, -3:], conserved, conserved[:, :3]], axis=1)
    span_metric = metrics[6:9]
    span_row = jnp.concatenate([span_metric[:, -3:], span_metric, span_metric[:, :3]], axis=1)
    summed = blocked(stream_flow, stream_row, -1, 1, 1, CZ)
    summed = summed + blocked(normal_flow, normal_row, -2, 2, 1, CZ)
    summed = summed + blocked(span_flow, span_row, -3, 0, 2, CY)
    time_rate = -inv_volume[None] * summed
    return (conserved + STEP_SIZE * time_rate, time_rate)
```

```python
import jax
import jax.numpy as jnp
from jax import lax
from jax.experimental import pallas as pl
from jax.experimental.pallas import tpu as pltpu
from jax.sharding import PartitionSpec as P

GAMMA = 1.4
WENO_EPS = 1e-06
STEP_SIZE = 0.08
MESH = pl.DeviceIdType.MESH

XL, XH, YL, YH, ZL, ZH, MIR = range(7)
FLUX, SPEED, VEL, PRES, ROW = 5, 10, 11, 14, 15
CELL_ROWS = 18


def order_of(direction):
    return [direction % 3, (direction + 1) % 3, (direction + 2) % 3]


def cell_terms(fields, row):
    inverse = 1.0 / fields[0]
    velocity = [fields[1 + member] * inverse for member in range(3)]
    kinetic = 0.5 * sum(fields[1 + member] * velocity[member] for member in range(3))
    pressure = (GAMMA - 1.0) * (fields[4] - kinetic)
    contra = sum(row[member] * velocity[member] for member in range(3))
    fluxes = [fields[0] * contra]
    fluxes += [fields[1 + member] * contra + row[member] * pressure for member in range(3)]
    fluxes += [(fields[4] + pressure) * contra]
    size = sum(row[member] * row[member] for member in range(3))
    speed = jnp.abs(contra) + jnp.sqrt(GAMMA * pressure * inverse * size)
    return fluxes, speed, velocity, pressure


def weno_shift(d1, d2, d3, d4):
    s0, s1, s2 = d2 - d1, d3 - d2, d4 - d3
    q2 = d2 * d2 + WENO_EPS
    q3 = d3 * d3 + WENO_EPS
    b0 = s0 * ((4.0 / 3.0) * s0 + d2) + q2
    b1 = s1 * ((4.0 / 3.0) * s1 + d2) + q2
    b2 = s2 * ((4.0 / 3.0) * s2 - d3) + q3
    p01, p02, p12 = b0 * b1, b0 * b2, b1 * b2
    w0 = p12 * p12
    w1 = 6.0 * (p02 * p02)
    w2 = 3.0 * (p01 * p01)
    g0 = 2.0 * s0 + 3.0 * d2
    g1 = d2 + 2.0 * d3
    g2 = 3.0 * d3 - s2
    return (w0 * g0 + w1 * g1 + w2 * g2) / (w0 + w1 + w2)


def face_flux(get):
    alpha = get(SPEED, 0)
    for cell in range(1, 6):
        alpha = jnp.maximum(alpha, get(SPEED, cell))
    rho = 0.5 * (get(0, 2) + get(0, 3))
    ua, ub, uc = [0.5 * (get(VEL + m, 2) + get(VEL + m, 3)) for m in range(3)]
    pressure = 0.5 * (get(PRES, 2) + get(PRES, 3))
    sa, sb, sc = [get(ROW + m, 2) + get(ROW + m, 3) for m in range(3)]
    flat = sa * sa + sc * sc
    inv_flat = lax.rsqrt(flat)
    inv_size = lax.rsqrt(flat + sb * sb)
    na, nb, nc = sa * inv_size, sb * inv_size, sc * inv_size
    la, lc = -sc * inv_flat, sa * inv_flat
    ma, mb, mc = nb * lc, nc * la - na * lc, -nb * la
    c2 = GAMMA * pressure / rho
    ic = lax.rsqrt(c2)
    c = c2 * ic
    f = (GAMMA - 1.0) * ic * ic
    kinetic = 0.5 * (ua * ua + ub * ub + uc * uc)
    q = na * ua + nb * ub + nc * uc
    a = la * ua + lc * uc
    b = ma * ua + mb * ub + mc * uc
    f4 = 0.25 * f
    g4 = f4 * kinetic
    fa, fb, fc = f4 * ua, f4 * ub, f4 * uc
    i4 = 0.25 * ic
    q4, ia, ib, jc = i4 * q, i4 * na, i4 * nb, i4 * nc
    la2, lc2, a2 = 0.5 * la, 0.5 * lc, 0.5 * a
    ma2, mb2, mc2, b2 = 0.5 * ma, 0.5 * mb, 0.5 * mc, 0.5 * b

    def left(v):
        s = g4 * v[0] - (fa * v[1] + fb * v[2] + fc * v[3]) + f4 * v[4]
        t = q4 * v[0] - (ia * v[1] + ib * v[2] + jc * v[3])
        return [
            s + t,
            0.5 * v[0] - 2.0 * s,
            la2 * v[1] + lc2 * v[3] - a2 * v[0],
            ma2 * v[1] + mb2 * v[2] + mc2 * v[3] - b2 * v[0],
            s - t,
        ]

    up, down, middle = [], [], None
    for step in range(5):
        dq = [get(m, step + 1) - get(m, step) for m in range(5)]
        dg = [get(FLUX + m, step + 1) - get(FLUX + m, step) for m in range(5)]
        aq = [alpha * dq[m] for m in range(5)]
        if step < 4:
            up.append(left([dg[m] + aq[m] for m in range(5)]))
        if step > 0:
            down.append(left([dg[m] - aq[m] for m in range(5)]))
        if step == 2:
            middle = [0.5 * (get(FLUX + m, 2) + get(FLUX + m, 3) - aq[m]) for m in range(5)]
    chars = []
    for m in range(5):
        plus = weno_shift(up[0][m], up[1][m], up[2][m], up[3][m])
        minus = weno_shift(down[3][m], down[2][m], down[1][m], down[0][m])
        chars.append((1.0 / 6.0) * (plus - minus))
    ends = chars[0] + chars[4]
    total = ends + chars[1]
    along = c * (chars[4] - chars[0])
    energy = kinetic * total + (1.0 / (GAMMA - 1.0)) * c2 * ends + q * along + a * chars[2] + b * chars[3]
    return [
        middle[0] + total,
        middle[1] + (ua * total + na * along + la * chars[2] + ma * chars[3]),
        middle[2] + (ub * total + nb * along + mb * chars[3]),
        middle[3] + (uc * total + nc * along + lc * chars[2] + mc * chars[3]),
        middle[4] + energy,
    ]


def reversed_lanes(value):
    lane = lax.broadcasted_iota(jnp.int32, value.shape, 1)
    for bit in range(7):
        step = 1 << bit
        value = jnp.where((lane & step) == 0, pltpu.roll(value, 128 - step, 1), pltpu.roll(value, step, 1))
    return value


def kernel(
    q_hbm, s_hbm, inv_hbm, wake_hbm, rate_out, state_out,
    qv, sv, iv, wv, xl, xh, yl, yh, zl, zh, mir, ex, exh, ey, ez, fx, fy, fz, acc,
    send_sem, recv_sem, own_sem, far_in, row_in, go,
):
    gx, gy, gz = lax.axis_index("gx"), lax.axis_index("gy"), lax.axis_index("gz")
    y = lax.rem(gz, 8)
    late = gz >= 8
    edge_low, edge_high = y == 0, y == 7
    edge = jnp.logical_or(edge_low, edge_high)
    far_late = jnp.logical_and(late, edge)
    far_early = jnp.logical_and(jnp.logical_not(late), edge)
    beside_far = jnp.logical_and(late, jnp.logical_or(y == 1, y == 6))
    wall, top = gy == 0, gy == 11
    inflow, outflow = gx == 0, gx == 3
    not_ = jnp.logical_not
    both = jnp.logical_and

    up_z = (gx, gy, lax.rem(gz + 1, 16))
    down_z = (gx, gy, lax.rem(gz + 15, 16))
    partner = (gx, gy, jnp.where(edge_low, down_z[2], up_z[2]))
    inner = (gx, gy, jnp.where(edge_low, up_z[2], down_z[2]))
    outer = (gx, gy, jnp.where(y == 1, down_z[2], up_z[2]))
    row = [
        (not_(inflow), (gx - 1, gy, gz)),
        (not_(outflow), (gx + 1, gy, gz)),
        (not_(wall), (gx, gy - 1, gz)),
        (not_(top), (gx, gy + 1, gz)),
        (both(wall, jnp.logical_or(inflow, outflow)), (3 - gx, gy, gz)),
    ]
    spans = [(not_(edge_high), up_z, y + 1), (not_(edge_low), down_z, y - 1)]
    barrier = pltpu.get_barrier_semaphore()

    def signal(semaphore, target):
        pl.semaphore_signal(semaphore, inc=1, device_id=target, device_id_type=MESH)

    buffers = (xl, xh, yl, yh, zl, zh, mir)

    def copies(slot):
        target = {
            XL: (gx + 1, gy, gz),
            XH: (gx - 1, gy, gz),
            YL: (gx, gy + 1, gz),
            YH: (gx, gy - 1, gz),
            ZL: up_z,
            ZH: down_z,
            MIR: (3 - gx, gy, gz),
        }[slot]
        direction = {XL: 0, XH: 0, YL: 1, YH: 1, ZL: 2, ZH: 2, MIR: 1}[slot]
        low, amount = {ZL: (1, 3), ZH: (0, 3)}.get(slot, (0, 4))
        pieces = [
            (q_hbm.at[:, pl.ds(low, amount)], buffers[slot].at[pl.ds(0, 5)]),
            (s_hbm.at[pl.ds(3 * direction, 3), pl.ds(low, amount)], buffers[slot].at[pl.ds(5, 3)]),
        ]
        return [
            pltpu.make_async_remote_copy(
                src_ref=source,
                dst_ref=landing,
                send_sem=send_sem.at[slot, piece],
                recv_sem=recv_sem.at[slot, piece],
                device_id=target,
                device_id_type=MESH,
            )
            for piece, (source, landing) in enumerate(pieces)
        ]

    @pl.when(far_early)
    def _():
        signal(barrier, partner)

    @pl.when(far_late)
    def _():
        signal(barrier, inner)

    @pl.when(not_(far_late))
    def _():
        for there, target in row:
            @pl.when(there)
            def _():
                signal(barrier, target)
        for there, target, row_of in spans:
            target_far_late = both(late, jnp.logical_or(row_of == 0, row_of == 7))

            @pl.when(both(there, not_(target_far_late)))
            def _():
                signal(barrier, target)

    near_row = sum(there.astype(jnp.int32) for there, _ in row)
    near_span = sum(there.astype(jnp.int32) for there, _, _ in spans)
    pl.semaphore_wait(barrier, jnp.where(far_late, 1, near_row + near_span))

    def send_far():
        @pl.when(edge_high)
        def _():
            for copy in copies(ZL):
                copy.start()

        @pl.when(edge_low)
        def _():
            for copy in copies(ZH):
                copy.start()

    @pl.when(far_late)
    def _():
        send_far()
        signal(far_in, partner)

    own = [
        pltpu.make_async_copy(q_hbm, qv, own_sem.at[0]),
        pltpu.make_async_copy(s_hbm, sv, own_sem.at[1]),
        pltpu.make_async_copy(inv_hbm, iv, own_sem.at[2]),
        pltpu.make_async_copy(wake_hbm, wv, own_sem.at[3]),
    ]
    for copy in own:
        copy.start()

    @pl.when(far_late)
    def _():
        pl.semaphore_wait(go, 1)

    sends = [
        (XL, not_(outflow)),
        (XH, not_(inflow)),
        (YL, not_(top)),
        (YH, not_(wall)),
        (MIR, wall),
        (ZL, not_(edge_high)),
        (ZH, not_(edge_low)),
    ]
    for slot, there in sends:
        @pl.when(there)
        def _():
            for copy in copies(slot):
                copy.start()

    @pl.when(beside_far)
    def _():
        for there, target in row:
            @pl.when(there)
            def _():
                signal(row_in, target)
        pl.semaphore_wait(row_in, near_row)
        signal(go, outer)

    for copy in own:
        copy.wait()

    def arrive(slot):
        for copy in copies(slot):
            copy.wait_recv()

    lane = lax.broadcasted_iota(jnp.int32, (8, 128), 1)

    def fill(array, index):
        fields = [array[(m,) + index] for m in range(5)]
        metric = [array[(ROW + m,) + index] for m in range(3)]
        fluxes, speed, velocity, pressure = cell_terms(fields, metric)
        for m in range(5):
            array[(FLUX + m,) + index] = fluxes[m]
        array[(SPEED,) + index] = speed
        for m in range(3):
            array[(VEL + m,) + index] = velocity[m]
        array[(PRES,) + index] = pressure

    def raw_rows(direction):
        cyclic = order_of(direction)
        listed = [(0, 0, None), (4, 4, None)]
        for m in range(3):
            listed.append((1 + m, 1 + cyclic[m], None))
            listed.append((ROW + m, None, cyclic[m]))
        return listed

    @pl.when(not_(inflow))
    def _():
        arrive(XL)

    @pl.when(inflow)
    def _():
        for k in range(4):
            for f in range(5):
                xl[f, k] = jnp.broadcast_to(qv[f, k, :, 0:1], (8, 128))
            for f in range(3):
                xl[5 + f, k] = jnp.broadcast_to(sv[f, k, :, 0:1], (8, 128))

    @pl.when(not_(outflow))
    def _():
        arrive(XH)

    @pl.when(outflow)
    def _():
        for k in range(4):
            for f in range(5):
                xh[f, k] = jnp.broadcast_to(qv[f, k, :, 127:128], (8, 128))
            for f in range(3):
                xh[5 + f, k] = jnp.broadcast_to(sv[f, k, :, 127:128], (8, 128))

    for out, flow, metric in raw_rows(0):
        halo = flow if flow is not None else 5 + metric
        packed = None
        for k in range(4):
            centre = qv[flow, k] if flow is not None else sv[metric, k]
            ring = jnp.where(lane < 64, xh[halo, k], xl[halo, k])
            ex[out, k] = centre
            exh[out, k] = ring
            moved = pltpu.roll(jnp.where(lane < 64, ring, centre), (32 * k + 3) % 128, 1)
            packed = moved if packed is None else jnp.where(lane < 32 * k, packed, moved)
        ex[out, 4] = packed
        exh[out, 4] = packed

    def fill_x(k, carry):
        fill(ex, (k,))
        fill(exh, (k,))
        return carry

    lax.fori_loop(0, 5, fill_x, 0)

    def face_x(k, carry):
        cache = {}

        def get(r, cell):
            if (r, cell) not in cache:
                shift = 3 - cell
                centre = ex[r, k]
                if shift > 0:
                    centre = pltpu.roll(jnp.where(lane >= 128 - shift, exh[r, k], centre), shift, 1)
                elif shift < 0:
                    centre = pltpu.roll(jnp.where(lane < -shift, exh[r, k], centre), 128 + shift, 1)
                cache[(r, cell)] = centre
            return cache[(r, cell)]

        flux = face_flux(get)
        for m in range(5):
            fx[m, k] = flux[m]
        return carry

    lax.fori_loop(0, 5, face_x, 0)
    for k in range(4):
        for m in range(5):
            upper = pltpu.roll(fx[m, k], 127, 1)
            last = pltpu.roll(fx[m, 4], (124 - 32 * k) % 128, 1)
            acc[m, k] = jnp.where(lane == 127, last, upper) - fx[m, k]

    @pl.when(wall)
    def _():
        arrive(MIR)
        is_wake = jnp.broadcast_to(wv[0:1, :], (8, 128)) >= 0
        for f in range(8):
            for k in range(4):
                mirrored = reversed_lanes(mir[f, k])
                beside = qv[f, k] if f < 5 else sv[f - 2, k]
                if f in (1, 2, 3):
                    beside = -beside
                ghost = jnp.where(is_wake, mirrored, beside)
                for g in range(3):
                    yl[f, k, 7 - g : 8 - g, :] = ghost[g : g + 1, :]

    @pl.when(not_(wall))
    def _():
        arrive(YL)

    @pl.when(top)
    def _():
        for f in range(8):
            for k in range(4):
                source = qv[f, k, 7:8, :] if f < 5 else sv[f - 2, k, 7:8, :]
                yh[f, k] = jnp.broadcast_to(source, (8, 128))

    @pl.when(not_(top))
    def _():
        arrive(YH)

    for out, flow, metric in raw_rows(1):
        halo = flow if flow is not None else 5 + metric
        for k in range(4):
            base = 14 * k
            ey[out, base : base + 3, :] = yl[halo, k, 5:8, :]
            ey[out, base + 3 : base + 11, :] = qv[flow, k] if flow is not None else sv[3 + metric, k]
            ey[out, base + 11 : base + 14, :] = yh[halo, k, 0:3, :]
        ey[out, 56:64, :] = qv[flow, 3] if flow is not None else sv[3 + metric, 3]

    def fill_y(k, carry):
        fill(ey, (pl.ds(pl.multiple_of(8 * k, 8), 8),))
        return carry

    lax.fori_loop(0, 8, fill_y, 0)

    def face_y(k, carry):
        cache = {}

        def get(r, cell):
            if (r, cell) not in cache:
                cache[(r, cell)] = ey[r, pl.ds(8 * k + cell, 8), :]
            return cache[(r, cell)]

        flux = face_flux(get)
        for m in range(5):
            fy[m, pl.ds(pl.multiple_of(8 * k, 8), 8), :] = flux[m]
        return carry

    lax.fori_loop(0, 7, face_y, 0)
    cyclic = order_of(1)
    for k in range(4):
        for m in range(5):
            target = 1 + cyclic[m - 1] if 1 <= m <= 3 else m
            acc[target, k] += fy[m, 14 * k + 1 : 14 * k + 9, :] - fy[m, 14 * k : 14 * k + 8, :]

    def fill_z(first, last):
        def body(k, carry):
            fill(ez, (k,))
            return carry

        lax.fori_loop(first, last, body, 0)

    def take_z(halo_ref, base):
        for out, flow, metric in raw_rows(2):
            halo = flow if flow is not None else 5 + metric
            for k in range(3):
                ez[out, base + k] = halo_ref[halo, k]

    def face_z(k, carry):
        cache = {}

        def get(r, cell):
            if (r, cell) not in cache:
                cache[(r, cell)] = ez[r, k + cell]
            return cache[(r, cell)]

        flux = face_flux(get)
        for m in range(5):
            fz[m, k] = flux[m]
        return carry

    for out, flow, metric in raw_rows(2):
        for k in range(4):
            ez[out, 3 + k] = qv[flow, k] if flow is not None else sv[6 + metric, k]
    fill_z(3, 7)

    def low_z():
        arrive(ZL)
        take_z(zl, 0)
        fill_z(0, 3)

    def high_z():
        arrive(ZH)
        take_z(zh, 7)
        fill_z(7, 10)

    @pl.when(not_(edge_low))
    def _():
        low_z()

    @pl.when(not_(edge_high))
    def _():
        high_z()

    early_first = jnp.where(edge_low, 3, 0)
    early_last = jnp.where(edge_low, 5, jnp.where(edge_high, 2, 5))
    lax.fori_loop(early_first, early_last, face_z, 0)

    @pl.when(far_early)
    def _():
        pl.semaphore_wait(far_in, 1)
        send_far()

    @pl.when(edge_low)
    def _():
        low_z()

    @pl.when(edge_high)
    def _():
        high_z()

    late_first = jnp.where(edge_high, 2, 0)
    late_last = jnp.where(edge_low, 3, jnp.where(edge_high, 5, 0))
    lax.fori_loop(late_first, late_last, face_z, 0)

    cyclic = order_of(2)
    for m in range(5):
        target = 1 + cyclic[m - 1] if 1 <= m <= 3 else m
        for k in range(4):
            rate = -iv[k] * (acc[target, k] + (fz[m, k + 1] - fz[m, k]))
            rate_out[target, k] = rate
            state_out[target, k] = qv[target, k] + STEP_SIZE * rate

    for slot, there in sends:
        @pl.when(jnp.logical_or(there, edge if slot in (ZL, ZH) else there))
        def _():
            for copy in copies(slot):
                copy.wait_send()


def local(conserved, metrics, inv_volume, wake_donor):
    block = conserved.shape
    planes, rows, lanes = block[1:]
    wide = jax.ShapeDtypeStruct(block, jnp.float32)
    f32 = lambda *shape: pltpu.VMEM(shape, jnp.float32)
    rate, state = pl.pallas_call(
        kernel,
        out_shape=(wide, wide),
        in_specs=[pl.BlockSpec(memory_space=pltpu.HBM)] * 4,
        out_specs=[pl.BlockSpec(memory_space=pltpu.VMEM)] * 2,
        scratch_shapes=[
            f32(*block),
            f32(9, planes, rows, lanes),
            f32(planes, rows, lanes),
            pltpu.VMEM((1, lanes), jnp.int32),
            *[f32(8, planes, rows, lanes)] * 4,
            *[f32(8, 3, rows, lanes)] * 2,
            f32(8, planes, rows, lanes),
            f32(CELL_ROWS, 5, rows, lanes),
            f32(CELL_ROWS, 5, rows, lanes),
            f32(CELL_ROWS, 64, lanes),
            f32(CELL_ROWS, 10, rows, lanes),
            f32(5, 5, rows, lanes),
            f32(5, 56, lanes),
            f32(5, 5, rows, lanes),
            f32(*block),
            pltpu.SemaphoreType.DMA((7, 2)),
            pltpu.SemaphoreType.DMA((7, 2)),
            pltpu.SemaphoreType.DMA((4,)),
            pltpu.SemaphoreType.REGULAR,
            pltpu.SemaphoreType.REGULAR,
            pltpu.SemaphoreType.REGULAR,
        ],
        compiler_params=pltpu.CompilerParams(collective_id=0, has_side_effects=True),
    )(conserved, metrics, inv_volume, wake_donor[None])
    return state, rate


def solution(mesh):
    placed = (P(None, "gz", "gy", "gx"), P(None, "gz", "gy", "gx"), P("gz", "gy", "gx"), P("gx"))
    return jax.shard_map(
        local,
        mesh=mesh,
        in_specs=placed,
        out_specs=(P(None, "gz", "gy", "gx"), P(None, "gz", "gy", "gx")),
        check_vma=False,
    )
```

```python
import jax
import jax.numpy as jnp
from jax import lax
from jax.experimental import pallas as pl
from jax.experimental.pallas import tpu as pltpu
from jax.sharding import PartitionSpec as P

GAMMA = 1.4
WENO_EPS = 1e-06
STEP_SIZE = 0.08
MESH = pl.DeviceIdType.MESH

XL, XH, YL, YH, ZL, ZH, MIR = range(7)
FLUX, SPEED, VEL, PRES, ROW = 5, 10, 11, 14, 15
CELL_ROWS = 18


def order_of(direction):
    return [direction % 3, (direction + 1) % 3, (direction + 2) % 3]


def cell_terms(fields, row):
    inverse = 1.0 / fields[0]
    velocity = [fields[1 + member] * inverse for member in range(3)]
    kinetic = 0.5 * sum(fields[1 + member] * velocity[member] for member in range(3))
    pressure = (GAMMA - 1.0) * (fields[4] - kinetic)
    contra = sum(row[member] * velocity[member] for member in range(3))
    fluxes = [fields[0] * contra]
    fluxes += [fields[1 + member] * contra + row[member] * pressure for member in range(3)]
    fluxes += [(fields[4] + pressure) * contra]
    size = sum(row[member] * row[member] for member in range(3))
    speed = jnp.abs(contra) + jnp.sqrt(GAMMA * pressure * inverse * size)
    return fluxes, speed, velocity, pressure


def weno_shift(d1, d2, d3, d4):
    s0, s1, s2 = d2 - d1, d3 - d2, d4 - d3
    q2 = d2 * d2 + WENO_EPS
    q3 = d3 * d3 + WENO_EPS
    b0 = s0 * ((4.0 / 3.0) * s0 + d2) + q2
    b1 = s1 * ((4.0 / 3.0) * s1 + d2) + q2
    b2 = s2 * ((4.0 / 3.0) * s2 - d3) + q3
    p01, p02, p12 = b0 * b1, b0 * b2, b1 * b2
    w0 = p12 * p12
    w1 = 6.0 * (p02 * p02)
    w2 = 3.0 * (p01 * p01)
    g0 = 2.0 * s0 + 3.0 * d2
    g1 = d2 + 2.0 * d3
    g2 = 3.0 * d3 - s2
    return (w0 * g0 + w1 * g1 + w2 * g2) / (w0 + w1 + w2)


def face_flux(get):
    alpha = get(SPEED, 0)
    for cell in range(1, 6):
        alpha = jnp.maximum(alpha, get(SPEED, cell))
    rho = 0.5 * (get(0, 2) + get(0, 3))
    ua, ub, uc = [0.5 * (get(VEL + m, 2) + get(VEL + m, 3)) for m in range(3)]
    pressure = 0.5 * (get(PRES, 2) + get(PRES, 3))
    sa, sb, sc = [get(ROW + m, 2) + get(ROW + m, 3) for m in range(3)]
    flat = sa * sa + sc * sc
    inv_flat = lax.rsqrt(flat)
    inv_size = lax.rsqrt(flat + sb * sb)
    na, nb, nc = sa * inv_size, sb * inv_size, sc * inv_size
    la, lc = -sc * inv_flat, sa * inv_flat
    ma, mb, mc = nb * lc, nc * la - na * lc, -nb * la
    c2 = GAMMA * pressure / rho
    ic = lax.rsqrt(c2)
    c = c2 * ic
    f = (GAMMA - 1.0) * ic * ic
    kinetic = 0.5 * (ua * ua + ub * ub + uc * uc)
    q = na * ua + nb * ub + nc * uc
    a = la * ua + lc * uc
    b = ma * ua + mb * ub + mc * uc
    f4 = 0.25 * f
    g4 = f4 * kinetic
    fa, fb, fc = f4 * ua, f4 * ub, f4 * uc
    i4 = 0.25 * ic
    q4, ia, ib, jc = i4 * q, i4 * na, i4 * nb, i4 * nc
    la2, lc2, a2 = 0.5 * la, 0.5 * lc, 0.5 * a
    ma2, mb2, mc2, b2 = 0.5 * ma, 0.5 * mb, 0.5 * mc, 0.5 * b

    def left(v):
        s = g4 * v[0] - (fa * v[1] + fb * v[2] + fc * v[3]) + f4 * v[4]
        t = q4 * v[0] - (ia * v[1] + ib * v[2] + jc * v[3])
        return [
            s + t,
            0.5 * v[0] - 2.0 * s,
            la2 * v[1] + lc2 * v[3] - a2 * v[0],
            ma2 * v[1] + mb2 * v[2] + mc2 * v[3] - b2 * v[0],
            s - t,
        ]

    up, down, middle = [], [], None
    for step in range(5):
        dq = [get(m, step + 1) - get(m, step) for m in range(5)]
        dg = [get(FLUX + m, step + 1) - get(FLUX + m, step) for m in range(5)]
        aq = [alpha * dq[m] for m in range(5)]
        if step < 4:
            up.append(left([dg[m] + aq[m] for m in range(5)]))
        if step > 0:
            down.append(left([dg[m] - aq[m] for m in range(5)]))
        if step == 2:
            middle = [0.5 * (get(FLUX + m, 2) + get(FLUX + m, 3) - aq[m]) for m in range(5)]
    chars = []
    for m in range(5):
        plus = weno_shift(up[0][m], up[1][m], up[2][m], up[3][m])
        minus = weno_shift(down[3][m], down[2][m], down[1][m], down[0][m])
        chars.append((1.0 / 6.0) * (plus - minus))
    ends = chars[0] + chars[4]
    total = ends + chars[1]
    along = c * (chars[4] - chars[0])
    energy = kinetic * total + (1.0 / (GAMMA - 1.0)) * c2 * ends + q * along + a * chars[2] + b * chars[3]
    return [
        middle[0] + total,
        middle[1] + (ua * total + na * along + la * chars[2] + ma * chars[3]),
        middle[2] + (ub * total + nb * along + mb * chars[3]),
        middle[3] + (uc * total + nc * along + lc * chars[2] + mc * chars[3]),
        middle[4] + energy,
    ]


def reversed_lanes(value):
    lane = lax.broadcasted_iota(jnp.int32, value.shape, 1)
    for bit in range(7):
        step = 1 << bit
        value = jnp.where((lane & step) == 0, pltpu.roll(value, 128 - step, 1), pltpu.roll(value, step, 1))
    return value


def kernel(
    q_hbm, s_hbm, inv_hbm, wake_hbm, rate_out, state_out,
    qv, sv, iv, wv, xl, xh, yl, yh, zl, zh, mir, ex, exh, ey, ez, fx, fy, fz, acc,
    send_sem, recv_sem, own_sem, far_in, row_in, go,
):
    gx, gy, gz = lax.axis_index("gx"), lax.axis_index("gy"), lax.axis_index("gz")
    y = lax.rem(gz, 8)
    late = gz >= 8
    edge_low, edge_high = y == 0, y == 7
    edge = jnp.logical_or(edge_low, edge_high)
    far_late = jnp.logical_and(late, edge)
    far_early = jnp.logical_and(jnp.logical_not(late), edge)
    beside_far = jnp.logical_and(late, jnp.logical_or(y == 1, y == 6))
    wall, top = gy == 0, gy == 11
    inflow, outflow = gx == 0, gx == 3
    not_ = jnp.logical_not
    both = jnp.logical_and

    up_z = (gx, gy, lax.rem(gz + 1, 16))
    down_z = (gx, gy, lax.rem(gz + 15, 16))
    partner = (gx, gy, jnp.where(edge_low, down_z[2], up_z[2]))
    inner = (gx, gy, jnp.where(edge_low, up_z[2], down_z[2]))
    outer = (gx, gy, jnp.where(y == 1, down_z[2], up_z[2]))
    row = [
        (not_(inflow), (gx - 1, gy, gz)),
        (not_(outflow), (gx + 1, gy, gz)),
        (not_(wall), (gx, gy - 1, gz)),
        (not_(top), (gx, gy + 1, gz)),
        (both(wall, jnp.logical_or(inflow, outflow)), (3 - gx, gy, gz)),
    ]
    spans = [(not_(edge_high), up_z, y + 1), (not_(edge_low), down_z, y - 1)]
    barrier = pltpu.get_barrier_semaphore()

    def signal(semaphore, target):
        pl.semaphore_signal(semaphore, inc=1, device_id=target, device_id_type=MESH)

    buffers = (xl, xh, yl, yh, zl, zh, mir)

    def copies(slot):
        target = {
            XL: (gx + 1, gy, gz),
            XH: (gx - 1, gy, gz),
            YL: (gx, gy + 1, gz),
            YH: (gx, gy - 1, gz),
            ZL: up_z,
            ZH: down_z,
            MIR: (3 - gx, gy, gz),
        }[slot]
        direction = {XL: 0, XH: 0, YL: 1, YH: 1, ZL: 2, ZH: 2, MIR: 1}[slot]
        low, amount = {ZL: (1, 3), ZH: (0, 3)}.get(slot, (0, 4))
        pieces = [
            (q_hbm.at[:, pl.ds(low, amount)], buffers[slot].at[pl.ds(0, 5)]),
            (s_hbm.at[pl.ds(3 * direction, 3), pl.ds(low, amount)], buffers[slot].at[pl.ds(5, 3)]),
        ]
        return [
            pltpu.make_async_remote_copy(
                src_ref=source,
                dst_ref=landing,
                send_sem=send_sem.at[slot, piece],
                recv_sem=recv_sem.at[slot, piece],
                device_id=target,
                device_id_type=MESH,
            )
            for piece, (source, landing) in enumerate(pieces)
        ]

    @pl.when(far_early)
    def _():
        signal(barrier, partner)

    @pl.when(far_late)
    def _():
        signal(barrier, inner)

    @pl.when(not_(far_late))
    def _():
        for there, target in row:
            @pl.when(there)
            def _():
                signal(barrier, target)
        for there, target, row_of in spans:
            target_far_late = both(late, jnp.logical_or(row_of == 0, row_of == 7))

            @pl.when(both(there, not_(target_far_late)))
            def _():
                signal(barrier, target)

    near_row = sum(there.astype(jnp.int32) for there, _ in row)
    near_span = sum(there.astype(jnp.int32) for there, _, _ in spans)
    pl.semaphore_wait(barrier, jnp.where(far_late, 1, near_row + near_span))

    def send_far():
        @pl.when(edge_high)
        def _():
            for copy in copies(ZL):
                copy.start()

        @pl.when(edge_low)
        def _():
            for copy in copies(ZH):
                copy.start()

    rank = gy // 2

    @pl.when(both(far_late, rank < 2))
    def _():
        send_far()

    @pl.when(far_late)
    def _():
        signal(far_in, partner)

    own = [
        pltpu.make_async_copy(q_hbm, qv, own_sem.at[0]),
        pltpu.make_async_copy(s_hbm, sv, own_sem.at[1]),
        pltpu.make_async_copy(inv_hbm, iv, own_sem.at[2]),
        pltpu.make_async_copy(wake_hbm, wv, own_sem.at[3]),
    ]
    for copy in own:
        copy.start()

    @pl.when(both(far_late, both(rank >= 2, rank < 4)))
    def _():
        own[0].wait()
        own[1].wait()
        send_far()

    @pl.when(far_late)
    def _():
        pl.semaphore_wait(go, 1)

    @pl.when(both(far_late, rank >= 4))
    def _():
        send_far()

    sends = [
        (XL, not_(outflow)),
        (XH, not_(inflow)),
        (YL, not_(top)),
        (YH, not_(wall)),
        (MIR, wall),
        (ZL, not_(edge_high)),
        (ZH, not_(edge_low)),
    ]
    for slot, there in sends:
        @pl.when(there)
        def _():
            for copy in copies(slot):
                copy.start()

    @pl.when(beside_far)
    def _():
        for there, target in row:
            @pl.when(there)
            def _():
                signal(row_in, target)
        pl.semaphore_wait(row_in, near_row)
        signal(go, outer)

    @pl.when(not_(both(far_late, both(rank >= 2, rank < 4))))
    def _():
        own[0].wait()
        own[1].wait()

    own[2].wait()
    own[3].wait()

    def arrive(slot):
        for copy in copies(slot):
            copy.wait_recv()

    lane = lax.broadcasted_iota(jnp.int32, (8, 128), 1)

    def fill(array, index):
        fields = [array[(m,) + index] for m in range(5)]
        metric = [array[(ROW + m,) + index] for m in range(3)]
        fluxes, speed, velocity, pressure = cell_terms(fields, metric)
        for m in range(5):
            array[(FLUX + m,) + index] = fluxes[m]
        array[(SPEED,) + index] = speed
        for m in range(3):
            array[(VEL + m,) + index] = velocity[m]
        array[(PRES,) + index] = pressure

    def raw_rows(direction):
        cyclic = order_of(direction)
        listed = [(0, 0, None), (4, 4, None)]
        for m in range(3):
            listed.append((1 + m, 1 + cyclic[m], None))
            listed.append((ROW + m, None, cyclic[m]))
        return listed

    @pl.when(not_(inflow))
    def _():
        arrive(XL)

    @pl.when(inflow)
    def _():
        for k in range(4):
            for f in range(5):
                xl[f, k] = jnp.broadcast_to(qv[f, k, :, 0:1], (8, 128))
            for f in range(3):
                xl[5 + f, k] = jnp.broadcast_to(sv[f, k, :, 0:1], (8, 128))

    @pl.when(not_(outflow))
    def _():
        arrive(XH)

    @pl.when(outflow)
    def _():
        for k in range(4):
            for f in range(5):
                xh[f, k] = jnp.broadcast_to(qv[f, k, :, 127:128], (8, 128))
            for f in range(3):
                xh[5 + f, k] = jnp.broadcast_to(sv[f, k, :, 127:128], (8, 128))

    for out, flow, metric in raw_rows(0):
        halo = flow if flow is not None else 5 + metric
        packed = None
        for k in range(4):
            centre = qv[flow, k] if flow is not None else sv[metric, k]
            ring = jnp.where(lane < 64, xh[halo, k], xl[halo, k])
            ex[out, k] = centre
            exh[out, k] = ring
            moved = pltpu.roll(jnp.where(lane < 64, ring, centre), (32 * k + 3) % 128, 1)
            packed = moved if packed is None else jnp.where(lane < 32 * k, packed, moved)
        ex[out, 4] = packed
        exh[out, 4] = packed

    def fill_x(k, carry):
        fill(ex, (k,))
        fill(exh, (k,))
        return carry

    lax.fori_loop(0, 5, fill_x, 0)

    def face_x(k, carry):
        cache = {}

        def get(r, cell):
            if (r, cell) not in cache:
                shift = 3 - cell
                centre = ex[r, k]
                if shift > 0:
                    centre = pltpu.roll(jnp.where(lane >= 128 - shift, exh[r, k], centre), shift, 1)
                elif shift < 0:
                    centre = pltpu.roll(jnp.where(lane < -shift, exh[r, k], centre), 128 + shift, 1)
                cache[(r, cell)] = centre
            return cache[(r, cell)]

        flux = face_flux(get)
        for m in range(5):
            fx[m, k] = flux[m]
        return carry

    lax.fori_loop(0, 5, face_x, 0)
    for k in range(4):
        for m in range(5):
            upper = pltpu.roll(fx[m, k], 127, 1)
            last = pltpu.roll(fx[m, 4], (124 - 32 * k) % 128, 1)
            acc[m, k] = jnp.where(lane == 127, last, upper) - fx[m, k]

    @pl.when(wall)
    def _():
        arrive(MIR)
        is_wake = jnp.broadcast_to(wv[0:1, :], (8, 128)) >= 0
        for f in range(8):
            for k in range(4):
                mirrored = reversed_lanes(mir[f, k])
                beside = qv[f, k] if f < 5 else sv[f - 2, k]
                if f in (1, 2, 3):
                    beside = -beside
                ghost = jnp.where(is_wake, mirrored, beside)
                for g in range(3):
                    yl[f, k, 7 - g : 8 - g, :] = ghost[g : g + 1, :]

    @pl.when(not_(wall))
    def _():
        arrive(YL)

    @pl.when(top)
    def _():
        for f in range(8):
            for k in range(4):
                source = qv[f, k, 7:8, :] if f < 5 else sv[f - 2, k, 7:8, :]
                yh[f, k] = jnp.broadcast_to(source, (8, 128))

    @pl.when(not_(top))
    def _():
        arrive(YH)

    for out, flow, metric in raw_rows(1):
        halo = flow if flow is not None else 5 + metric
        for k in range(4):
            base = 14 * k
            ey[out, base : base + 3, :] = yl[halo, k, 5:8, :]
            ey[out, base + 3 : base + 11, :] = qv[flow, k] if flow is not None else sv[3 + metric, k]
            ey[out, base + 11 : base + 14, :] = yh[halo, k, 0:3, :]
        ey[out, 56:64, :] = qv[flow, 3] if flow is not None else sv[3 + metric, 3]

    def fill_y(k, carry):
        fill(ey, (pl.ds(pl.multiple_of(8 * k, 8), 8),))
        return carry

    lax.fori_loop(0, 8, fill_y, 0)

    def face_y(k, carry):
        cache = {}

        def get(r, cell):
            if (r, cell) not in cache:
                cache[(r, cell)] = ey[r, pl.ds(8 * k + cell, 8), :]
            return cache[(r, cell)]

        flux = face_flux(get)
        for m in range(5):
            fy[m, pl.ds(pl.multiple_of(8 * k, 8), 8), :] = flux[m]
        return carry

    lax.fori_loop(0, 7, face_y, 0)
    cyclic = order_of(1)
    for k in range(4):
        for m in range(5):
            target = 1 + cyclic[m - 1] if 1 <= m <= 3 else m
            acc[target, k] += fy[m, 14 * k + 1 : 14 * k + 9, :] - fy[m, 14 * k : 14 * k + 8, :]

    def fill_z(first, last):
        def body(k, carry):
            fill(ez, (k,))
            return carry

        lax.fori_loop(first, last, body, 0)

    def take_z(halo_ref, base):
        for out, flow, metric in raw_rows(2):
            halo = flow if flow is not None else 5 + metric
            for k in range(3):
                ez[out, base + k] = halo_ref[halo, k]

    def face_z(k, carry):
        cache = {}

        def get(r, cell):
            if (r, cell) not in cache:
                cache[(r, cell)] = ez[r, k + cell]
            return cache[(r, cell)]

        flux = face_flux(get)
        for m in range(5):
            fz[m, k] = flux[m]
        return carry

    for out, flow, metric in raw_rows(2):
        for k in range(4):
            ez[out, 3 + k] = qv[flow, k] if flow is not None else sv[6 + metric, k]
    fill_z(3, 7)

    def low_z():
        arrive(ZL)
        take_z(zl, 0)
        fill_z(0, 3)

    def high_z():
        arrive(ZH)
        take_z(zh, 7)
        fill_z(7, 10)

    @pl.when(not_(edge_low))
    def _():
        low_z()

    @pl.when(not_(edge_high))
    def _():
        high_z()

    early_first = jnp.where(edge_low, 3, 0)
    early_last = jnp.where(edge_low, 5, jnp.where(edge_high, 2, 5))
    lax.fori_loop(early_first, early_last, face_z, 0)

    @pl.when(far_early)
    def _():
        pl.semaphore_wait(far_in, 1)
        send_far()

    @pl.when(edge_low)
    def _():
        low_z()

    @pl.when(edge_high)
    def _():
        high_z()

    late_first = jnp.where(edge_high, 2, 0)
    late_last = jnp.where(edge_low, 3, jnp.where(edge_high, 5, 0))
    lax.fori_loop(late_first, late_last, face_z, 0)

    cyclic = order_of(2)
    for m in range(5):
        target = 1 + cyclic[m - 1] if 1 <= m <= 3 else m
        for k in range(4):
            rate = -iv[k] * (acc[target, k] + (fz[m, k + 1] - fz[m, k]))
            rate_out[target, k] = rate
            state_out[target, k] = qv[target, k] + STEP_SIZE * rate

    for slot, there in sends:
        @pl.when(jnp.logical_or(there, edge if slot in (ZL, ZH) else there))
        def _():
            for copy in copies(slot):
                copy.wait_send()


def deliver(state, rate, state_out, rate_out, sem):
    copies = [
        pltpu.make_async_copy(state, state_out, sem.at[0]),
        pltpu.make_async_copy(rate, rate_out, sem.at[1]),
    ]
    for copy in copies:
        copy.start()
    for copy in copies:
        copy.wait()


def local(conserved, metrics, inv_volume, wake_donor):
    block = conserved.shape
    planes, rows, lanes = block[1:]
    wide = pltpu.VMEM(block, jnp.float32)
    f32 = lambda *shape: pltpu.VMEM(shape, jnp.float32)
    rate, state = pl.pallas_call(
        kernel,
        out_shape=(wide, wide),
        in_specs=[pl.BlockSpec(memory_space=pltpu.HBM)] * 4,
        out_specs=[pl.BlockSpec(memory_space=pltpu.VMEM)] * 2,
        scratch_shapes=[
            f32(*block),
            f32(9, planes, rows, lanes),
            f32(planes, rows, lanes),
            pltpu.VMEM((1, lanes), jnp.int32),
            *[f32(8, planes, rows, lanes)] * 4,
            *[f32(8, 3, rows, lanes)] * 2,
            f32(8, planes, rows, lanes),
            f32(CELL_ROWS, 5, rows, lanes),
            f32(CELL_ROWS, 5, rows, lanes),
            f32(CELL_ROWS, 64, lanes),
            f32(CELL_ROWS, 10, rows, lanes),
            f32(5, 5, rows, lanes),
            f32(5, 56, lanes),
            f32(5, 5, rows, lanes),
            f32(*block),
            pltpu.SemaphoreType.DMA((7, 2)),
            pltpu.SemaphoreType.DMA((7, 2)),
            pltpu.SemaphoreType.DMA((4,)),
            pltpu.SemaphoreType.REGULAR,
            pltpu.SemaphoreType.REGULAR,
            pltpu.SemaphoreType.REGULAR,
        ],
        compiler_params=pltpu.CompilerParams(collective_id=0, has_side_effects=True),
    )(conserved, metrics, inv_volume, wake_donor[None])
    return pl.pallas_call(
        deliver,
        out_shape=(jax.ShapeDtypeStruct(block, jnp.float32),) * 2,
        in_specs=[pl.BlockSpec(memory_space=pl.ANY)] * 2,
        out_specs=[pl.BlockSpec(memory_space=pltpu.HBM)] * 2,
        scratch_shapes=[pltpu.SemaphoreType.DMA((2,))],
    )(pltpu.with_memory_space_constraint(state, pltpu.VMEM), pltpu.with_memory_space_constraint(rate, pltpu.VMEM))


def solution(mesh):
    placed = (P(None, "gz", "gy", "gx"), P(None, "gz", "gy", "gx"), P("gz", "gy", "gx"), P("gx"))
    return jax.shard_map(
        local,
        mesh=mesh,
        in_specs=placed,
        out_specs=(P(None, "gz", "gy", "gx"), P(None, "gz", "gy", "gx")),
        check_vma=False,
    )
```

```python
import jax
import jax.numpy as jnp
from jax import lax
from jax.experimental import pallas as pl
from jax.experimental.pallas import tpu as pltpu
from jax.sharding import PartitionSpec as P

GAMMA = 1.4
WENO_EPS = 1e-06
STEP_SIZE = 0.08
MESH = pl.DeviceIdType.MESH

XL, XH, YL, YH, ZL, ZH, MIR, ZLX, ZHX, PASS = range(10)
FLUX, SPEED, VEL, PRES, ROW = 5, 10, 11, 14, 15
CELL_ROWS = 18


def order_of(direction):
    return [direction % 3, (direction + 1) % 3, (direction + 2) % 3]


def cell_terms(fields, row):
    inverse = 1.0 / fields[0]
    velocity = [fields[1 + member] * inverse for member in range(3)]
    kinetic = 0.5 * sum(fields[1 + member] * velocity[member] for member in range(3))
    pressure = (GAMMA - 1.0) * (fields[4] - kinetic)
    contra = sum(row[member] * velocity[member] for member in range(3))
    fluxes = [fields[0] * contra]
    fluxes += [fields[1 + member] * contra + row[member] * pressure for member in range(3)]
    fluxes += [(fields[4] + pressure) * contra]
    size = sum(row[member] * row[member] for member in range(3))
    speed = jnp.abs(contra) + jnp.sqrt(GAMMA * pressure * inverse * size)
    return fluxes, speed, velocity, pressure


def weno_shift(d1, d2, d3, d4):
    s0, s1, s2 = d2 - d1, d3 - d2, d4 - d3
    q2 = d2 * d2 + WENO_EPS
    q3 = d3 * d3 + WENO_EPS
    b0 = s0 * ((4.0 / 3.0) * s0 + d2) + q2
    b1 = s1 * ((4.0 / 3.0) * s1 + d2) + q2
    b2 = s2 * ((4.0 / 3.0) * s2 - d3) + q3
    p01, p02, p12 = b0 * b1, b0 * b2, b1 * b2
    w0 = p12 * p12
    w1 = 6.0 * (p02 * p02)
    w2 = 3.0 * (p01 * p01)
    g0 = 2.0 * s0 + 3.0 * d2
    g1 = d2 + 2.0 * d3
    g2 = 3.0 * d3 - s2
    return (w0 * g0 + w1 * g1 + w2 * g2) / (w0 + w1 + w2)


def face_flux(get):
    alpha = get(SPEED, 0)
    for cell in range(1, 6):
        alpha = jnp.maximum(alpha, get(SPEED, cell))
    rho = 0.5 * (get(0, 2) + get(0, 3))
    ua, ub, uc = [0.5 * (get(VEL + m, 2) + get(VEL + m, 3)) for m in range(3)]
    pressure = 0.5 * (get(PRES, 2) + get(PRES, 3))
    sa, sb, sc = [get(ROW + m, 2) + get(ROW + m, 3) for m in range(3)]
    flat = sa * sa + sc * sc
    inv_flat = lax.rsqrt(flat)
    inv_size = lax.rsqrt(flat + sb * sb)
    na, nb, nc = sa * inv_size, sb * inv_size, sc * inv_size
    la, lc = -sc * inv_flat, sa * inv_flat
    ma, mb, mc = nb * lc, nc * la - na * lc, -nb * la
    c2 = GAMMA * pressure / rho
    ic = lax.rsqrt(c2)
    c = c2 * ic
    f = (GAMMA - 1.0) * ic * ic
    kinetic = 0.5 * (ua * ua + ub * ub + uc * uc)
    q = na * ua + nb * ub + nc * uc
    a = la * ua + lc * uc
    b = ma * ua + mb * ub + mc * uc
    f4 = 0.25 * f
    g4 = f4 * kinetic
    fa, fb, fc = f4 * ua, f4 * ub, f4 * uc
    i4 = 0.25 * ic
    q4, ia, ib, jc = i4 * q, i4 * na, i4 * nb, i4 * nc
    la2, lc2, a2 = 0.5 * la, 0.5 * lc, 0.5 * a
    ma2, mb2, mc2, b2 = 0.5 * ma, 0.5 * mb, 0.5 * mc, 0.5 * b

    def left(v):
        s = g4 * v[0] - (fa * v[1] + fb * v[2] + fc * v[3]) + f4 * v[4]
        t = q4 * v[0] - (ia * v[1] + ib * v[2] + jc * v[3])
        return [
            s + t,
            0.5 * v[0] - 2.0 * s,
            la2 * v[1] + lc2 * v[3] - a2 * v[0],
            ma2 * v[1] + mb2 * v[2] + mc2 * v[3] - b2 * v[0],
            s - t,
        ]

    up, down, middle = [], [], None
    for step in range(5):
        dq = [get(m, step + 1) - get(m, step) for m in range(5)]
        dg = [get(FLUX + m, step + 1) - get(FLUX + m, step) for m in range(5)]
        aq = [alpha * dq[m] for m in range(5)]
        if step < 4:
            up.append(left([dg[m] + aq[m] for m in range(5)]))
        if step > 0:
            down.append(left([dg[m] - aq[m] for m in range(5)]))
        if step == 2:
            middle = [0.5 * (get(FLUX + m, 2) + get(FLUX + m, 3) - aq[m]) for m in range(5)]
    chars = []
    for m in range(5):
        plus = weno_shift(up[0][m], up[1][m], up[2][m], up[3][m])
        minus = weno_shift(down[3][m], down[2][m], down[1][m], down[0][m])
        chars.append((1.0 / 6.0) * (plus - minus))
    ends = chars[0] + chars[4]
    total = ends + chars[1]
    along = c * (chars[4] - chars[0])
    energy = kinetic * total + (1.0 / (GAMMA - 1.0)) * c2 * ends + q * along + a * chars[2] + b * chars[3]
    return [
        middle[0] + total,
        middle[1] + (ua * total + na * along + la * chars[2] + ma * chars[3]),
        middle[2] + (ub * total + nb * along + mb * chars[3]),
        middle[3] + (uc * total + nc * along + lc * chars[2] + mc * chars[3]),
        middle[4] + energy,
    ]


def reversed_lanes(value):
    lane = lax.broadcasted_iota(jnp.int32, value.shape, 1)
    for bit in range(7):
        step = 1 << bit
        value = jnp.where((lane & step) == 0, pltpu.roll(value, 128 - step, 1), pltpu.roll(value, step, 1))
    return value


def kernel(
    q_hbm, s_hbm, inv_hbm, wake_hbm, rate_out, state_out,
    qv, sv, iv, wv, xl, xh, yl, yh, zl, zh, mir, ex, exh, ey, ez, fx, fy, fz, acc,
    send_sem, recv_sem, own_sem, far_in, row_in, go,
):
    gx, gy, gz = lax.axis_index("gx"), lax.axis_index("gy"), lax.axis_index("gz")
    y = lax.rem(gz, 8)
    late = gz >= 8
    edge_low, edge_high = y == 0, y == 7
    edge = jnp.logical_or(edge_low, edge_high)
    far_late = jnp.logical_and(late, edge)
    far_early = jnp.logical_and(jnp.logical_not(late), edge)
    beside = jnp.logical_or(y == 1, y == 6)
    beside_far = jnp.logical_and(late, beside)
    corner = jnp.logical_and(gx == 0, gy == 0)
    lone, lone_far = jnp.logical_and(corner, gz == 0), jnp.logical_and(corner, gz == 15)
    by_x, by_y, by_z, by_mirror = [
        jnp.logical_and(jnp.logical_and(gx == i, gy == j), gz == k) for i, j, k in ((1, 0, 0), (0, 1, 0), (0, 0, 1), (3, 0, 0))
    ]
    adjacent = jnp.logical_or(jnp.logical_or(by_x, by_y), jnp.logical_or(by_z, by_mirror))
    relay = jnp.logical_and(jnp.logical_and(gz < 8, beside), jnp.logical_not(jnp.logical_and(corner, gz == 1)))
    wall, top = gy == 0, gy == 11
    inflow, outflow = gx == 0, gx == 3
    not_ = jnp.logical_not
    both = jnp.logical_and

    up_z = (gx, gy, lax.rem(gz + 1, 16))
    down_z = (gx, gy, lax.rem(gz + 15, 16))
    partner = (gx, gy, jnp.where(edge_low, down_z[2], up_z[2]))
    inner = (gx, gy, jnp.where(edge_low, up_z[2], down_z[2]))
    beyond = (gx, gy, jnp.where(jnp.logical_or(edge_low, y == 1), lax.rem(gz + 14, 16), lax.rem(gz + 2, 16)))
    outer = (gx, gy, jnp.where(y == 1, down_z[2], up_z[2]))
    row = [
        (not_(inflow), (gx - 1, gy, gz)),
        (not_(outflow), (gx + 1, gy, gz)),
        (not_(wall), (gx, gy - 1, gz)),
        (not_(top), (gx, gy + 1, gz)),
        (both(wall, jnp.logical_or(inflow, outflow)), (3 - gx, gy, gz)),
    ]
    spans = [(not_(edge_high), up_z, y + 1), (not_(edge_low), down_z, y - 1)]
    barrier = pltpu.get_barrier_semaphore()

    def signal(semaphore, target):
        pl.semaphore_signal(semaphore, inc=1, device_id=target, device_id_type=MESH)

    buffers = (xl, xh, yl, yh, zl, zh, mir, zl, zh)

    def copies(slot):
        target = {
            XL: (gx + 1, gy, gz),
            XH: (gx - 1, gy, gz),
            YL: (gx, gy + 1, gz),
            YH: (gx, gy - 1, gz),
            ZL: up_z,
            ZH: down_z,
            MIR: (3 - gx, gy, gz),
            ZLX: up_z,
            ZHX: down_z,
        }[slot]
        direction = {XL: 0, XH: 0, YL: 1, YH: 1, MIR: 1}.get(slot, 2)
        low, amount = {ZL: (1, 3), ZH: (0, 3), ZLX: (0, 1), ZHX: (3, 1)}.get(slot, (0, 4))
        pieces = [
            (q_hbm.at[:, pl.ds(low, amount)], buffers[slot].at[pl.ds(0, 5), pl.ds(low, amount)]),
            (s_hbm.at[pl.ds(3 * direction, 3), pl.ds(low, amount)], buffers[slot].at[pl.ds(5, 3), pl.ds(low, amount)]),
        ]
        return [
            pltpu.make_async_remote_copy(
                src_ref=source,
                dst_ref=landing,
                send_sem=send_sem.at[slot, piece],
                recv_sem=recv_sem.at[slot, piece],
                device_id=target,
                device_id_type=MESH,
            )
            for piece, (source, landing) in enumerate(pieces)
        ]

    def passes(slot, held):
        low = {ZL: 1, ZH: 0}[slot]
        return [
            pltpu.make_async_remote_copy(
                src_ref=held.at[pl.ds(first, amount), pl.ds(low, 3)],
                dst_ref=buffers[slot].at[pl.ds(first, amount), pl.ds(low, 3)],
                send_sem=send_sem.at[PASS, piece],
                recv_sem=recv_sem.at[slot, piece],
                device_id=beyond,
                device_id_type=MESH,
            )
            for piece, (first, amount) in enumerate(((0, 5), (5, 3)))
        ]

    @pl.when(far_early)
    def _():
        signal(barrier, partner)

    @pl.when(relay)
    def _():
        signal(barrier, beyond)

    @pl.when(far_late)
    def _():
        signal(barrier, inner)

    @pl.when(not_(jnp.logical_or(far_late, lone)))
    def _():
        for there, target in row:
            @pl.when(there)
            def _():
                signal(barrier, target)
        for there, target, row_of in spans:
            target_far_late = both(late, jnp.logical_or(row_of == 0, row_of == 7))

            @pl.when(both(there, not_(target_far_late)))
            def _():
                signal(barrier, target)

    near_row = sum(there.astype(jnp.int32) for there, _ in row)
    near_span = sum(there.astype(jnp.int32) for there, _, _ in spans)
    pl.semaphore_wait(barrier, jnp.where(lone_far, 1, jnp.where(far_late, 2, near_row + near_span - adjacent.astype(jnp.int32))))

    def send_far():
        @pl.when(edge_high)
        def _():
            for copy in copies(ZL):
                copy.start()

        @pl.when(edge_low)
        def _():
            for copy in copies(ZH):
                copy.start()

    @pl.when(far_late)
    def _():
        signal(far_in, (gx, gy, jnp.where(lone_far, partner[2], beyond[2])))

    turn = gy // 2

    @pl.when(both(far_late, both(edge_high, turn == 3)))
    def _():
        pl.delay(1000)

    @pl.when(both(far_late, both(edge_high, turn == 5)))
    def _():
        pl.delay(2000)

    @pl.when(far_late)
    def _():
        send_far()

    own = [
        pltpu.make_async_copy(q_hbm, qv, own_sem.at[0]),
        pltpu.make_async_copy(s_hbm, sv, own_sem.at[1]),
        pltpu.make_async_copy(inv_hbm, iv, own_sem.at[2]),
        pltpu.make_async_copy(wake_hbm, wv, own_sem.at[3]),
    ]
    for copy in own:
        copy.start()

    @pl.when(far_late)
    def _():
        pl.semaphore_wait(go, 1)

    sends = [
        (XL, not_(outflow)),
        (XH, not_(inflow)),
        (YL, not_(top)),
        (YH, not_(wall)),
        (MIR, wall),
        (ZL, not_(edge_high)),
        (ZH, not_(edge_low)),
        (ZLX, both(both(edge_low, not_(late)), not_(lone))),
        (ZHX, both(edge_high, not_(late))),
    ]
    to_lone = {XH: by_x, YH: by_y, ZH: by_z, MIR: by_mirror}
    for slot, there in sends:
        @pl.when(both(there, not_(to_lone[slot])) if slot in to_lone else there)
        def _():
            for copy in copies(slot):
                copy.start()

    @pl.when(lone)
    def _():
        for target in ((1, 0, 0), (0, 1, 0), (0, 0, 1), (3, 0, 0)):
            signal(row_in, target)

    @pl.when(beside_far)
    def _():
        for there, target in row:
            @pl.when(there)
            def _():
                signal(row_in, target)
        pl.semaphore_wait(row_in, near_row)
        signal(go, outer)

    for copy in own:
        copy.wait()

    def arrive(slot):
        for copy in copies(slot):
            copy.wait_recv()

    lane = lax.broadcasted_iota(jnp.int32, (8, 128), 1)

    def fill(array, index):
        fields = [array[(m,) + index] for m in range(5)]
        metric = [array[(ROW + m,) + index] for m in range(3)]
        fluxes, speed, velocity, pressure = cell_terms(fields, metric)
        for m in range(5):
            array[(FLUX + m,) + index] = fluxes[m]
        array[(SPEED,) + index] = speed
        for m in range(3):
            array[(VEL + m,) + index] = velocity[m]
        array[(PRES,) + index] = pressure

    def raw_rows(direction):
        cyclic = order_of(direction)
        listed = [(0, 0, None), (4, 4, None)]
        for m in range(3):
            listed.append((1 + m, 1 + cyclic[m], None))
            listed.append((ROW + m, None, cyclic[m]))
        return listed

    @pl.when(adjacent)
    def _():
        pl.semaphore_wait(row_in, 1)
        for slot, there in to_lone.items():
            @pl.when(there)
            def _():
                for copy in copies(slot):
                    copy.start()

    @pl.when(not_(inflow))
    def _():
        arrive(XL)

    @pl.when(inflow)
    def _():
        for k in range(4):
            for f in range(5):
                xl[f, k] = jnp.broadcast_to(qv[f, k, :, 0:1], (8, 128))
            for f in range(3):
                xl[5 + f, k] = jnp.broadcast_to(sv[f, k, :, 0:1], (8, 128))

    @pl.when(not_(outflow))
    def _():
        arrive(XH)

    @pl.when(outflow)
    def _():
        for k in range(4):
            for f in range(5):
                xh[f, k] = jnp.broadcast_to(qv[f, k, :, 127:128], (8, 128))
            for f in range(3):
                xh[5 + f, k] = jnp.broadcast_to(sv[f, k, :, 127:128], (8, 128))

    for out, flow, metric in raw_rows(0):
        halo = flow if flow is not None else 5 + metric
        packed = None
        for k in range(4):
            centre = qv[flow, k] if flow is not None else sv[metric, k]
            ring = jnp.where(lane < 64, xh[halo, k], xl[halo, k])
            ex[out, k] = centre
            exh[out, k] = ring
            moved = pltpu.roll(jnp.where(lane < 64, ring, centre), (32 * k + 3) % 128, 1)
            packed = moved if packed is None else jnp.where(lane < 32 * k, packed, moved)
        ex[out, 4] = packed
        exh[out, 4] = packed

    def fill_x(k, carry):
        fill(ex, (k,))
        fill(exh, (k,))
        return carry

    lax.fori_loop(0, 5, fill_x, 0)

    def face_x(k, carry):
        cache = {}

        def get(r, cell):
            if (r, cell) not in cache:
                shift = 3 - cell
                centre = ex[r, k]
                if shift > 0:
                    centre = pltpu.roll(jnp.where(lane >= 128 - shift, exh[r, k], centre), shift, 1)
                elif shift < 0:
                    centre = pltpu.roll(jnp.where(lane < -shift, exh[r, k], centre), 128 + shift, 1)
                cache[(r, cell)] = centre
            return cache[(r, cell)]

        flux = face_flux(get)
        for m in range(5):
            fx[m, k] = flux[m]
        return carry

    lax.fori_loop(0, 5, face_x, 0)
    for k in range(4):
        for m in range(5):
            upper = pltpu.roll(fx[m, k], 127, 1)
            last = pltpu.roll(fx[m, 4], (124 - 32 * k) % 128, 1)
            acc[m, k] = jnp.where(lane == 127, last, upper) - fx[m, k]

    @pl.when(wall)
    def _():
        arrive(MIR)
        is_wake = jnp.broadcast_to(wv[0:1, :], (8, 128)) >= 0
        for f in range(8):
            for k in range(4):
                mirrored = reversed_lanes(mir[f, k])
                beside = qv[f, k] if f < 5 else sv[f - 2, k]
                if f in (1, 2, 3):
                    beside = -beside
                ghost = jnp.where(is_wake, mirrored, beside)
                for g in range(3):
                    yl[f, k, 7 - g : 8 - g, :] = ghost[g : g + 1, :]

    @pl.when(not_(wall))
    def _():
        arrive(YL)

    @pl.when(top)
    def _():
        for f in range(8):
            for k in range(4):
                source = qv[f, k, 7:8, :] if f < 5 else sv[f - 2, k, 7:8, :]
                yh[f, k] = jnp.broadcast_to(source, (8, 128))

    @pl.when(not_(top))
    def _():
        arrive(YH)

    for out, flow, metric in raw_rows(1):
        halo = flow if flow is not None else 5 + metric
        for k in range(4):
            base = 14 * k
            ey[out, base : base + 3, :] = yl[halo, k, 5:8, :]
            ey[out, base + 3 : base + 11, :] = qv[flow, k] if flow is not None else sv[3 + metric, k]
            ey[out, base + 11 : base + 14, :] = yh[halo, k, 0:3, :]
        ey[out, 56:64, :] = qv[flow, 3] if flow is not None else sv[3 + metric, 3]

    def fill_y(k, carry):
        fill(ey, (pl.ds(pl.multiple_of(8 * k, 8), 8),))
        return carry

    lax.fori_loop(0, 8, fill_y, 0)

    def face_y(k, carry):
        cache = {}

        def get(r, cell):
            if (r, cell) not in cache:
                cache[(r, cell)] = ey[r, pl.ds(8 * k + cell, 8), :]
            return cache[(r, cell)]

        flux = face_flux(get)
        for m in range(5):
            fy[m, pl.ds(pl.multiple_of(8 * k, 8), 8), :] = flux[m]
        return carry

    lax.fori_loop(0, 7, face_y, 0)
    cyclic = order_of(1)
    for k in range(4):
        for m in range(5):
            target = 1 + cyclic[m - 1] if 1 <= m <= 3 else m
            acc[target, k] += fy[m, 14 * k + 1 : 14 * k + 9, :] - fy[m, 14 * k : 14 * k + 8, :]

    def fill_z(first, last):
        def body(k, carry):
            fill(ez, (k,))
            return carry

        lax.fori_loop(first, last, body, 0)

    def take_z(halo_ref, base, low):
        for out, flow, metric in raw_rows(2):
            halo = flow if flow is not None else 5 + metric
            for k in range(3):
                ez[out, base + k] = halo_ref[halo, low + k]

    def face_z(k, carry):
        cache = {}

        def get(r, cell):
            if (r, cell) not in cache:
                cache[(r, cell)] = ez[r, k + cell]
            return cache[(r, cell)]

        flux = face_flux(get)
        for m in range(5):
            fz[m, k] = flux[m]
        return carry

    for out, flow, metric in raw_rows(2):
        for k in range(4):
            ez[out, 3 + k] = qv[flow, k] if flow is not None else sv[6 + metric, k]
    fill_z(3, 7)

    def low_z():
        arrive(ZL)
        take_z(zl, 0, 1)
        fill_z(0, 3)

    def high_z():
        arrive(ZH)
        take_z(zh, 7, 0)
        fill_z(7, 10)

    @pl.when(not_(edge_low))
    def _():
        low_z()

    @pl.when(not_(edge_high))
    def _():
        high_z()

    early_first = jnp.where(edge_low, 3, 0)
    early_last = jnp.where(edge_low, 5, jnp.where(edge_high, 2, 5))
    lax.fori_loop(early_first, early_last, face_z, 0)

    @pl.when(lone)
    def _():
        pl.semaphore_wait(far_in, 1)
        send_far()

    @pl.when(edge_low)
    def _():
        low_z()

    @pl.when(edge_high)
    def _():
        high_z()

    late_first = jnp.where(edge_high, 2, 0)
    late_last = jnp.where(edge_low, 3, jnp.where(edge_high, 5, 0))
    lax.fori_loop(late_first, late_last, face_z, 0)

    cyclic = order_of(2)
    for m in range(5):
        target = 1 + cyclic[m - 1] if 1 <= m <= 3 else m
        for k in range(4):
            rate = -iv[k] * (acc[target, k] + (fz[m, k + 1] - fz[m, k]))
            rate_out[target, k] = rate
            state_out[target, k] = qv[target, k] + STEP_SIZE * rate

    @pl.when(both(relay, y == 1))
    def _():
        arrive(ZLX)
        pl.semaphore_wait(far_in, 1)
        for copy in passes(ZH, zl):
            copy.start()

    @pl.when(both(relay, y == 6))
    def _():
        arrive(ZHX)
        pl.semaphore_wait(far_in, 1)
        for copy in passes(ZL, zh):
            copy.start()

    @pl.when(relay)
    def _():
        for copy in passes(ZH, zl):
            copy.wait_send()

    for slot, there in sends:
        @pl.when(jnp.logical_or(there, {ZL: far_late, ZH: jnp.logical_or(far_late, lone)}.get(slot, there)))
        def _():
            for copy in copies(slot):
                copy.wait_send()


def deliver(state, rate, state_out, rate_out, sem):
    copies = [
        pltpu.make_async_copy(state, state_out, sem.at[0]),
        pltpu.make_async_copy(rate, rate_out, sem.at[1]),
    ]
    for copy in copies:
        copy.start()
    for copy in copies:
        copy.wait()


def local(conserved, metrics, inv_volume, wake_donor):
    block = conserved.shape
    planes, rows, lanes = block[1:]
    wide = pltpu.VMEM(block, jnp.float32)
    f32 = lambda *shape: pltpu.VMEM(shape, jnp.float32)
    rate, state = pl.pallas_call(
        kernel,
        out_shape=(wide, wide),
        in_specs=[pl.BlockSpec(memory_space=pltpu.HBM)] * 4,
        out_specs=[pl.BlockSpec(memory_space=pltpu.VMEM)] * 2,
        scratch_shapes=[
            f32(*block),
            f32(9, planes, rows, lanes),
            f32(planes, rows, lanes),
            pltpu.VMEM((1, lanes), jnp.int32),
            *[f32(8, planes, rows, lanes)] * 4,
            *[f32(8, planes, rows, lanes)] * 2,
            f32(8, planes, rows, lanes),
            f32(CELL_ROWS, 5, rows, lanes),
            f32(CELL_ROWS, 5, rows, lanes),
            f32(CELL_ROWS, 64, lanes),
            f32(CELL_ROWS, 10, rows, lanes),
            f32(5, 5, rows, lanes),
            f32(5, 56, lanes),
            f32(5, 5, rows, lanes),
            f32(*block),
            pltpu.SemaphoreType.DMA((10, 2)),
            pltpu.SemaphoreType.DMA((10, 2)),
            pltpu.SemaphoreType.DMA((4,)),
            pltpu.SemaphoreType.REGULAR,
            pltpu.SemaphoreType.REGULAR,
            pltpu.SemaphoreType.REGULAR,
        ],
        compiler_params=pltpu.CompilerParams(collective_id=0, has_side_effects=True),
    )(conserved, metrics, inv_volume, wake_donor[None])
    return pl.pallas_call(
        deliver,
        out_shape=(jax.ShapeDtypeStruct(block, jnp.float32),) * 2,
        in_specs=[pl.BlockSpec(memory_space=pl.ANY)] * 2,
        out_specs=[pl.BlockSpec(memory_space=pltpu.HBM)] * 2,
        scratch_shapes=[pltpu.SemaphoreType.DMA((2,))],
    )(pltpu.with_memory_space_constraint(state, pltpu.VMEM), pltpu.with_memory_space_constraint(rate, pltpu.VMEM))


def solution(mesh):
    placed = (P(None, "gz", "gy", "gx"), P(None, "gz", "gy", "gx"), P("gz", "gy", "gx"), P("gx"))
    return jax.shard_map(
        local,
        mesh=mesh,
        in_specs=placed,
        out_specs=(P(None, "gz", "gy", "gx"), P(None, "gz", "gy", "gx")),
        check_vma=False,
    )
```

```python
import jax
import jax.numpy as jnp
from jax import lax
from jax.experimental import pallas as pl
from jax.experimental.pallas import tpu as pltpu
from jax.sharding import PartitionSpec as P

GAMMA = 1.4
WENO_EPS = 1e-06
STEP_SIZE = 0.08
MESH = pl.DeviceIdType.MESH

XL, XH, YL, YH, ZL, ZH, MIR, ZLX, ZHX = range(9)
FLUX, SPEED, VEL, PRES, ROW = 5, 10, 11, 14, 15
CELL_ROWS = 18


def order_of(direction):
    return [direction % 3, (direction + 1) % 3, (direction + 2) % 3]


def cell_terms(fields, row):
    inverse = 1.0 / fields[0]
    velocity = [fields[1 + member] * inverse for member in range(3)]
    kinetic = 0.5 * sum(fields[1 + member] * velocity[member] for member in range(3))
    pressure = (GAMMA - 1.0) * (fields[4] - kinetic)
    contra = sum(row[member] * velocity[member] for member in range(3))
    fluxes = [fields[0] * contra]
    fluxes += [fields[1 + member] * contra + row[member] * pressure for member in range(3)]
    fluxes += [(fields[4] + pressure) * contra]
    size = sum(row[member] * row[member] for member in range(3))
    speed = jnp.abs(contra) + jnp.sqrt(GAMMA * pressure * inverse * size)
    return fluxes, speed, velocity, pressure


def weno_shift(d1, d2, d3, d4):
    s0, s1, s2 = d2 - d1, d3 - d2, d4 - d3
    q2 = d2 * d2 + WENO_EPS
    q3 = d3 * d3 + WENO_EPS
    b0 = s0 * ((4.0 / 3.0) * s0 + d2) + q2
    b1 = s1 * ((4.0 / 3.0) * s1 + d2) + q2
    b2 = s2 * ((4.0 / 3.0) * s2 - d3) + q3
    p01, p02, p12 = b0 * b1, b0 * b2, b1 * b2
    w0 = p12 * p12
    w1 = 6.0 * (p02 * p02)
    w2 = 3.0 * (p01 * p01)
    g0 = 2.0 * s0 + 3.0 * d2
    g1 = d2 + 2.0 * d3
    g2 = 3.0 * d3 - s2
    return (w0 * g0 + w1 * g1 + w2 * g2) / (w0 + w1 + w2)


def face_flux(get):
    alpha = get(SPEED, 0)
    for cell in range(1, 6):
        alpha = jnp.maximum(alpha, get(SPEED, cell))
    rho = 0.5 * (get(0, 2) + get(0, 3))
    ua, ub, uc = [0.5 * (get(VEL + m, 2) + get(VEL + m, 3)) for m in range(3)]
    pressure = 0.5 * (get(PRES, 2) + get(PRES, 3))
    sa, sb, sc = [get(ROW + m, 2) + get(ROW + m, 3) for m in range(3)]
    flat = sa * sa + sc * sc
    inv_flat = lax.rsqrt(flat)
    inv_size = lax.rsqrt(flat + sb * sb)
    na, nb, nc = sa * inv_size, sb * inv_size, sc * inv_size
    la, lc = -sc * inv_flat, sa * inv_flat
    ma, mb, mc = nb * lc, nc * la - na * lc, -nb * la
    c2 = GAMMA * pressure / rho
    ic = lax.rsqrt(c2)
    c = c2 * ic
    f = (GAMMA - 1.0) * ic * ic
    kinetic = 0.5 * (ua * ua + ub * ub + uc * uc)
    q = na * ua + nb * ub + nc * uc
    a = la * ua + lc * uc
    b = ma * ua + mb * ub + mc * uc
    f4 = 0.25 * f
    g4 = f4 * kinetic
    fa, fb, fc = f4 * ua, f4 * ub, f4 * uc
    i4 = 0.25 * ic
    q4, ia, ib, jc = i4 * q, i4 * na, i4 * nb, i4 * nc
    la2, lc2, a2 = 0.5 * la, 0.5 * lc, 0.5 * a
    ma2, mb2, mc2, b2 = 0.5 * ma, 0.5 * mb, 0.5 * mc, 0.5 * b

    def left(v):
        s = g4 * v[0] - (fa * v[1] + fb * v[2] + fc * v[3]) + f4 * v[4]
        t = q4 * v[0] - (ia * v[1] + ib * v[2] + jc * v[3])
        return [
            s + t,
            0.5 * v[0] - 2.0 * s,
            la2 * v[1] + lc2 * v[3] - a2 * v[0],
            ma2 * v[1] + mb2 * v[2] + mc2 * v[3] - b2 * v[0],
            s - t,
        ]

    up, down, middle = [], [], None
    for step in range(5):
        dq = [get(m, step + 1) - get(m, step) for m in range(5)]
        dg = [get(FLUX + m, step + 1) - get(FLUX + m, step) for m in range(5)]
        aq = [alpha * dq[m] for m in range(5)]
        if step < 4:
            up.append(left([dg[m] + aq[m] for m in range(5)]))
        if step > 0:
            down.append(left([dg[m] - aq[m] for m in range(5)]))
        if step == 2:
            middle = [0.5 * (get(FLUX + m, 2) + get(FLUX + m, 3) - aq[m]) for m in range(5)]
    chars = []
    for m in range(5):
        plus = weno_shift(up[0][m], up[1][m], up[2][m], up[3][m])
        minus = weno_shift(down[3][m], down[2][m], down[1][m], down[0][m])
        chars.append((1.0 / 6.0) * (plus - minus))
    ends = chars[0] + chars[4]
    total = ends + chars[1]
    along = c * (chars[4] - chars[0])
    energy = kinetic * total + (1.0 / (GAMMA - 1.0)) * c2 * ends + q * along + a * chars[2] + b * chars[3]
    return [
        middle[0] + total,
        middle[1] + (ua * total + na * along + la * chars[2] + ma * chars[3]),
        middle[2] + (ub * total + nb * along + mb * chars[3]),
        middle[3] + (uc * total + nc * along + lc * chars[2] + mc * chars[3]),
        middle[4] + energy,
    ]


def reversed_lanes(value):
    lane = lax.broadcasted_iota(jnp.int32, value.shape, 1)
    for bit in range(7):
        step = 1 << bit
        value = jnp.where((lane & step) == 0, pltpu.roll(value, 128 - step, 1), pltpu.roll(value, step, 1))
    return value


def kernel(
    q_hbm, s_hbm, inv_hbm, wake_hbm, rate_out, state_out,
    qv, sv, iv, wv, xl, xh, yl, yh, zl, zh, mir, ex, exh, ey, ez, fx, fy, fz, acc,
    send_sem, recv_sem, own_sem, far_send, far_recv, far_in, row_in, go,
):
    gx, gy, gz = lax.axis_index("gx"), lax.axis_index("gy"), lax.axis_index("gz")
    y = lax.rem(gz, 8)
    late = gz >= 8
    edge_low, edge_high = y == 0, y == 7
    edge = jnp.logical_or(edge_low, edge_high)
    far_late = jnp.logical_and(late, edge)
    far_early = jnp.logical_and(jnp.logical_not(late), edge)
    beside = jnp.logical_or(y == 1, y == 6)
    beside_far = jnp.logical_and(late, beside)
    corner = jnp.logical_and(gx == 0, gy == 0)
    lone, lone_far = jnp.logical_and(corner, gz == 0), jnp.logical_and(corner, gz == 15)
    by_x, by_y, by_z, by_mirror = [
        jnp.logical_and(jnp.logical_and(gx == i, gy == j), gz == k) for i, j, k in ((1, 0, 0), (0, 1, 0), (0, 0, 1), (3, 0, 0))
    ]
    adjacent = jnp.logical_or(jnp.logical_or(by_x, by_y), jnp.logical_or(by_z, by_mirror))
    relay = jnp.logical_and(jnp.logical_and(gz < 8, beside), jnp.logical_not(jnp.logical_and(corner, gz == 1)))
    wall, top = gy == 0, gy == 11
    inflow, outflow = gx == 0, gx == 3
    not_ = jnp.logical_not
    both = jnp.logical_and

    up_z = (gx, gy, lax.rem(gz + 1, 16))
    down_z = (gx, gy, lax.rem(gz + 15, 16))
    partner = (gx, gy, jnp.where(edge_low, down_z[2], up_z[2]))
    inner = (gx, gy, jnp.where(edge_low, up_z[2], down_z[2]))
    beyond = (gx, gy, jnp.where(jnp.logical_or(edge_low, y == 1), lax.rem(gz + 14, 16), lax.rem(gz + 2, 16)))
    outer = (gx, gy, jnp.where(y == 1, down_z[2], up_z[2]))
    row = [
        (not_(inflow), (gx - 1, gy, gz)),
        (not_(outflow), (gx + 1, gy, gz)),
        (not_(wall), (gx, gy - 1, gz)),
        (not_(top), (gx, gy + 1, gz)),
        (both(wall, jnp.logical_or(inflow, outflow)), (3 - gx, gy, gz)),
    ]
    spans = [(not_(edge_high), up_z, y + 1), (not_(edge_low), down_z, y - 1)]
    barrier = pltpu.get_barrier_semaphore()

    def signal(semaphore, target):
        pl.semaphore_signal(semaphore, inc=1, device_id=target, device_id_type=MESH)

    buffers = (xl, xh, yl, yh, zl, zh, mir, zl, zh)

    def copies(slot):
        target = {
            XL: (gx + 1, gy, gz),
            XH: (gx - 1, gy, gz),
            YL: (gx, gy + 1, gz),
            YH: (gx, gy - 1, gz),
            ZL: up_z,
            ZH: down_z,
            MIR: (3 - gx, gy, gz),
            ZLX: up_z,
            ZHX: down_z,
        }[slot]
        direction = {XL: 0, XH: 0, YL: 1, YH: 1, MIR: 1}.get(slot, 2)
        low, amount = {ZL: (1, 3), ZH: (0, 3), ZLX: (0, 1), ZHX: (3, 1)}.get(slot, (0, 4))
        pieces = [
            (q_hbm.at[:, pl.ds(low, amount)], buffers[slot].at[pl.ds(0, 5), pl.ds(low, amount)]),
            (s_hbm.at[pl.ds(3 * direction, 3), pl.ds(low, amount)], buffers[slot].at[pl.ds(5, 3), pl.ds(low, amount)]),
        ]
        return [
            pltpu.make_async_remote_copy(
                src_ref=source,
                dst_ref=landing,
                send_sem=send_sem.at[slot, piece],
                recv_sem=recv_sem.at[slot, piece],
                device_id=target,
                device_id_type=MESH,
            )
            for piece, (source, landing) in enumerate(pieces)
        ]

    def far_copies(slot, flow, metric, target):
        listed = []
        for stage in range(3):
            plane = {ZL: 3 - stage, ZH: stage}[slot]
            for source, landing in (
                (flow.at[:, plane], buffers[slot].at[pl.ds(0, 5), plane]),
                (metric.at[:, plane], buffers[slot].at[pl.ds(5, 3), plane]),
            ):
                listed.append(
                    pltpu.make_async_remote_copy(
                        src_ref=source,
                        dst_ref=landing,
                        send_sem=far_send,
                        recv_sem=far_recv.at[stage],
                        device_id=target,
                        device_id_type=MESH,
                    )
                )
        return listed

    def far_arrive(slot, stage):
        plane = 3 - stage if slot == ZL else stage
        pltpu.make_async_remote_copy(
            src_ref=buffers[slot].at[:, plane],
            dst_ref=buffers[slot].at[:, plane],
            send_sem=far_send,
            recv_sem=far_recv.at[stage],
            device_id=partner,
            device_id_type=MESH,
        ).wait_recv()

    def far_sent():
        pltpu.make_async_remote_copy(
            src_ref=zl.at[:, pl.ds(0, 3)],
            dst_ref=zl.at[:, pl.ds(0, 3)],
            send_sem=far_send,
            recv_sem=far_recv.at[0],
            device_id=partner,
            device_id_type=MESH,
        ).wait_send()

    def send_far():
        flow, metric = q_hbm, s_hbm.at[pl.ds(6, 3)]

        @pl.when(edge_high)
        def _():
            for copy in far_copies(ZL, flow, metric, partner):
                copy.start()

        @pl.when(edge_low)
        def _():
            for copy in far_copies(ZH, flow, metric, partner):
                copy.start()

    @pl.when(far_late)
    def _():
        pl.semaphore_wait(barrier, jnp.where(lone_far, 1, 2))

    @pl.when(far_late)
    def _():
        signal(far_in, (gx, gy, jnp.where(lone_far, partner[2], beyond[2])))

    turn = gy // 2

    @pl.when(both(far_late, both(edge_high, turn == 3)))
    def _():
        pl.delay(1000)

    @pl.when(both(far_late, both(edge_high, turn == 5)))
    def _():
        pl.delay(2000)

    @pl.when(far_late)
    def _():
        send_far()

    @pl.when(far_early)
    def _():
        signal(barrier, partner)

    @pl.when(relay)
    def _():
        signal(barrier, beyond)

    @pl.when(far_late)
    def _():
        signal(barrier, inner)

    @pl.when(not_(jnp.logical_or(far_late, lone)))
    def _():
        for there, target in row:
            @pl.when(there)
            def _():
                signal(barrier, target)
        for there, target, row_of in spans:
            target_far_late = both(late, jnp.logical_or(row_of == 0, row_of == 7))

            @pl.when(both(there, not_(target_far_late)))
            def _():
                signal(barrier, target)

    near_row = sum(there.astype(jnp.int32) for there, _ in row)
    near_span = sum(there.astype(jnp.int32) for there, _, _ in spans)

    @pl.when(not_(far_late))
    def _():
        pl.semaphore_wait(barrier, near_row + near_span - adjacent.astype(jnp.int32))


    own = [
        pltpu.make_async_copy(q_hbm, qv, own_sem.at[0]),
        pltpu.make_async_copy(s_hbm, sv, own_sem.at[1]),
        pltpu.make_async_copy(inv_hbm, iv, own_sem.at[2]),
        pltpu.make_async_copy(wake_hbm, wv, own_sem.at[3]),
    ]
    for copy in own:
        copy.start()

    @pl.when(far_late)
    def _():
        pl.semaphore_wait(go, 1)

    sends = [
        (XL, not_(outflow)),
        (XH, not_(inflow)),
        (YL, not_(top)),
        (YH, not_(wall)),
        (MIR, wall),
        (ZL, not_(edge_high)),
        (ZH, not_(edge_low)),
        (ZLX, both(both(edge_low, not_(late)), not_(lone))),
        (ZHX, both(edge_high, not_(late))),
    ]
    to_lone = {XH: by_x, YH: by_y, ZH: by_z, MIR: by_mirror}
    for slot, there in sends:
        @pl.when(both(there, not_(to_lone[slot])) if slot in to_lone else there)
        def _():
            for copy in copies(slot):
                copy.start()

    @pl.when(lone)
    def _():
        for target in ((1, 0, 0), (0, 1, 0), (0, 0, 1), (3, 0, 0)):
            signal(row_in, target)

    @pl.when(beside_far)
    def _():
        for there, target in row:
            @pl.when(there)
            def _():
                signal(row_in, target)
        pl.semaphore_wait(row_in, near_row)
        signal(go, outer)

    for copy in own:
        copy.wait()

    def arrive(slot):
        for copy in copies(slot):
            copy.wait_recv()

    lane = lax.broadcasted_iota(jnp.int32, (8, 128), 1)

    def fill(array, index):
        fields = [array[(m,) + index] for m in range(5)]
        metric = [array[(ROW + m,) + index] for m in range(3)]
        fluxes, speed, velocity, pressure = cell_terms(fields, metric)
        for m in range(5):
            array[(FLUX + m,) + index] = fluxes[m]
        array[(SPEED,) + index] = speed
        for m in range(3):
            array[(VEL + m,) + index] = velocity[m]
        array[(PRES,) + index] = pressure

    def raw_rows(direction):
        cyclic = order_of(direction)
        listed = [(0, 0, None), (4, 4, None)]
        for m in range(3):
            listed.append((1 + m, 1 + cyclic[m], None))
            listed.append((ROW + m, None, cyclic[m]))
        return listed

    @pl.when(adjacent)
    def _():
        pl.semaphore_wait(row_in, 1)
        for slot, there in to_lone.items():
            @pl.when(there)
            def _():
                for copy in copies(slot):
                    copy.start()

    @pl.when(not_(inflow))
    def _():
        arrive(XL)

    @pl.when(inflow)
    def _():
        for k in range(4):
            for f in range(5):
                xl[f, k] = jnp.broadcast_to(qv[f, k, :, 0:1], (8, 128))
            for f in range(3):
                xl[5 + f, k] = jnp.broadcast_to(sv[f, k, :, 0:1], (8, 128))

    @pl.when(not_(outflow))
    def _():
        arrive(XH)

    @pl.when(outflow)
    def _():
        for k in range(4):
            for f in range(5):
                xh[f, k] = jnp.broadcast_to(qv[f, k, :, 127:128], (8, 128))
            for f in range(3):
                xh[5 + f, k] = jnp.broadcast_to(sv[f, k, :, 127:128], (8, 128))

    for out, flow, metric in raw_rows(0):
        halo = flow if flow is not None else 5 + metric
        packed = None
        for k in range(4):
            centre = qv[flow, k] if flow is not None else sv[metric, k]
            ring = jnp.where(lane < 64, xh[halo, k], xl[halo, k])
            ex[out, k] = centre
            exh[out, k] = ring
            moved = pltpu.roll(jnp.where(lane < 64, ring, centre), (32 * k + 3) % 128, 1)
            packed = moved if packed is None else jnp.where(lane < 32 * k, packed, moved)
        ex[out, 4] = packed
        exh[out, 4] = packed

    def fill_x(k, carry):
        fill(ex, (k,))
        fill(exh, (k,))
        return carry

    lax.fori_loop(0, 5, fill_x, 0)

    def face_x(k, carry):
        cache = {}

        def get(r, cell):
            if (r, cell) not in cache:
                shift = 3 - cell
                centre = ex[r, k]
                if shift > 0:
                    centre = pltpu.roll(jnp.where(lane >= 128 - shift, exh[r, k], centre), shift, 1)
                elif shift < 0:
                    centre = pltpu.roll(jnp.where(lane < -shift, exh[r, k], centre), 128 + shift, 1)
                cache[(r, cell)] = centre
            return cache[(r, cell)]

        flux = face_flux(get)
        for m in range(5):
            fx[m, k] = flux[m]
        return carry

    lax.fori_loop(0, 5, face_x, 0)
    for k in range(4):
        for m in range(5):
            upper = pltpu.roll(fx[m, k], 127, 1)
            last = pltpu.roll(fx[m, 4], (124 - 32 * k) % 128, 1)
            acc[m, k] = jnp.where(lane == 127, last, upper) - fx[m, k]

    @pl.when(wall)
    def _():
        arrive(MIR)
        is_wake = jnp.broadcast_to(wv[0:1, :], (8, 128)) >= 0
        for f in range(8):
            for k in range(4):
                mirrored = reversed_lanes(mir[f, k])
                beside = qv[f, k] if f < 5 else sv[f - 2, k]
                if f in (1, 2, 3):
                    beside = -beside
                ghost = jnp.where(is_wake, mirrored, beside)
                for g in range(3):
                    yl[f, k, 7 - g : 8 - g, :] = ghost[g : g + 1, :]

    @pl.when(not_(wall))
    def _():
        arrive(YL)

    @pl.when(top)
    def _():
        for f in range(8):
            for k in range(4):
                source = qv[f, k, 7:8, :] if f < 5 else sv[f - 2, k, 7:8, :]
                yh[f, k] = jnp.broadcast_to(source, (8, 128))

    @pl.when(not_(top))
    def _():
        arrive(YH)

    for out, flow, metric in raw_rows(1):
        halo = flow if flow is not None else 5 + metric
        for k in range(4):
            base = 14 * k
            ey[out, base : base + 3, :] = yl[halo, k, 5:8, :]
            ey[out, base + 3 : base + 11, :] = qv[flow, k] if flow is not None else sv[3 + metric, k]
            ey[out, base + 11 : base + 14, :] = yh[halo, k, 0:3, :]
        ey[out, 56:64, :] = qv[flow, 3] if flow is not None else sv[3 + metric, 3]

    def fill_y(k, carry):
        fill(ey, (pl.ds(pl.multiple_of(8 * k, 8), 8),))
        return carry

    lax.fori_loop(0, 8, fill_y, 0)

    def face_y(k, carry):
        cache = {}

        def get(r, cell):
            if (r, cell) not in cache:
                cache[(r, cell)] = ey[r, pl.ds(8 * k + cell, 8), :]
            return cache[(r, cell)]

        flux = face_flux(get)
        for m in range(5):
            fy[m, pl.ds(pl.multiple_of(8 * k, 8), 8), :] = flux[m]
        return carry

    lax.fori_loop(0, 7, face_y, 0)
    cyclic = order_of(1)
    for k in range(4):
        for m in range(5):
            target = 1 + cyclic[m - 1] if 1 <= m <= 3 else m
            acc[target, k] += fy[m, 14 * k + 1 : 14 * k + 9, :] - fy[m, 14 * k : 14 * k + 8, :]

    def fill_z(first, last):
        def body(k, carry):
            fill(ez, (k,))
            return carry

        lax.fori_loop(first, last, body, 0)

    def take_plane(halo_ref, cell, plane):
        for out, flow, metric in raw_rows(2):
            halo = flow if flow is not None else 5 + metric
            ez[out, cell] = halo_ref[halo, plane]

    def take_z(halo_ref, base, low):
        for k in range(3):
            take_plane(halo_ref, base + k, low + k)

    def face_z(k, carry):
        cache = {}

        def get(r, cell):
            if (r, cell) not in cache:
                cache[(r, cell)] = ez[r, k + cell]
            return cache[(r, cell)]

        flux = face_flux(get)
        for m in range(5):
            fz[m, k] = flux[m]
        return carry

    for out, flow, metric in raw_rows(2):
        for k in range(4):
            ez[out, 3 + k] = qv[flow, k] if flow is not None else sv[6 + metric, k]
    fill_z(3, 7)

    def low_z():
        arrive(ZL)
        take_z(zl, 0, 1)
        fill_z(0, 3)

    def high_z():
        arrive(ZH)
        take_z(zh, 7, 0)
        fill_z(7, 10)

    @pl.when(not_(edge_low))
    def _():
        low_z()

    @pl.when(not_(edge_high))
    def _():
        high_z()

    early_first = jnp.where(edge_low, 3, 0)
    early_last = jnp.where(edge_low, 5, jnp.where(edge_high, 2, 5))
    lax.fori_loop(early_first, early_last, face_z, 0)

    @pl.when(lone)
    def _():
        pl.semaphore_wait(far_in, 1)
        send_far()

    @pl.when(edge)
    def _():
        def body(stage, carry):
            @pl.when(edge_low)
            def _():
                far_arrive(ZL, stage)
                take_plane(zl, 2 - stage, 3 - stage)
                fill(ez, (2 - stage,))

            @pl.when(edge_high)
            def _():
                far_arrive(ZH, stage)
                take_plane(zh, 7 + stage, stage)
                fill(ez, (7 + stage,))

            return face_z(jnp.where(edge_low, 2 - stage, 2 + stage), carry)

        lax.fori_loop(0, 3, body, 0)

    cyclic = order_of(2)
    for m in range(5):
        target = 1 + cyclic[m - 1] if 1 <= m <= 3 else m
        for k in range(4):
            rate = -iv[k] * (acc[target, k] + (fz[m, k + 1] - fz[m, k]))
            rate_out[target, k] = rate
            state_out[target, k] = qv[target, k] + STEP_SIZE * rate

    @pl.when(both(relay, y == 1))
    def _():
        arrive(ZLX)
        pl.semaphore_wait(far_in, 1)
        for copy in far_copies(ZH, zl.at[pl.ds(0, 5)], zl.at[pl.ds(5, 3)], beyond):
            copy.start()

    @pl.when(both(relay, y == 6))
    def _():
        arrive(ZHX)
        pl.semaphore_wait(far_in, 1)
        for copy in far_copies(ZL, zh.at[pl.ds(0, 5)], zh.at[pl.ds(5, 3)], beyond):
            copy.start()

    @pl.when(jnp.logical_or(relay, jnp.logical_or(far_late, lone)))
    def _():
        far_sent()

    for slot, there in sends:
        @pl.when(there)
        def _():
            for copy in copies(slot):
                copy.wait_send()


def deliver(state, rate, state_out, rate_out, sem):
    copies = [
        pltpu.make_async_copy(state, state_out, sem.at[0]),
        pltpu.make_async_copy(rate, rate_out, sem.at[1]),
    ]
    for copy in copies:
        copy.start()
    for copy in copies:
        copy.wait()


def local(conserved, metrics, inv_volume, wake_donor):
    block = conserved.shape
    planes, rows, lanes = block[1:]
    wide = pltpu.VMEM(block, jnp.float32)
    f32 = lambda *shape: pltpu.VMEM(shape, jnp.float32)
    rate, state = pl.pallas_call(
        kernel,
        out_shape=(wide, wide),
        in_specs=[pl.BlockSpec(memory_space=pltpu.HBM)] * 4,
        out_specs=[pl.BlockSpec(memory_space=pltpu.VMEM)] * 2,
        scratch_shapes=[
            f32(*block),
            f32(9, planes, rows, lanes),
            f32(planes, rows, lanes),
            pltpu.VMEM((1, lanes), jnp.int32),
            *[f32(8, planes, rows, lanes)] * 4,
            *[f32(8, planes, rows, lanes)] * 2,
            f32(8, planes, rows, lanes),
            f32(CELL_ROWS, 5, rows, lanes),
            f32(CELL_ROWS, 5, rows, lanes),
            f32(CELL_ROWS, 64, lanes),
            f32(CELL_ROWS, 10, rows, lanes),
            f32(5, 5, rows, lanes),
            f32(5, 56, lanes),
            f32(5, 5, rows, lanes),
            f32(*block),
            pltpu.SemaphoreType.DMA((9, 2)),
            pltpu.SemaphoreType.DMA((9, 2)),
            pltpu.SemaphoreType.DMA((4,)),
            pltpu.SemaphoreType.DMA,
            pltpu.SemaphoreType.DMA((3,)),
            pltpu.SemaphoreType.REGULAR,
            pltpu.SemaphoreType.REGULAR,
            pltpu.SemaphoreType.REGULAR,
        ],
        compiler_params=pltpu.CompilerParams(collective_id=0, has_side_effects=True),
    )(conserved, metrics, inv_volume, wake_donor[None])
    return pl.pallas_call(
        deliver,
        out_shape=(jax.ShapeDtypeStruct(block, jnp.float32),) * 2,
        in_specs=[pl.BlockSpec(memory_space=pl.ANY)] * 2,
        out_specs=[pl.BlockSpec(memory_space=pltpu.HBM)] * 2,
        scratch_shapes=[pltpu.SemaphoreType.DMA((2,))],
    )(pltpu.with_memory_space_constraint(state, pltpu.VMEM), pltpu.with_memory_space_constraint(rate, pltpu.VMEM))


def solution(mesh):
    placed = (P(None, "gz", "gy", "gx"), P(None, "gz", "gy", "gx"), P("gz", "gy", "gx"), P("gx"))
    return jax.shard_map(
        local,
        mesh=mesh,
        in_specs=placed,
        out_specs=(P(None, "gz", "gy", "gx"), P(None, "gz", "gy", "gx")),
        check_vma=False,
    )
```

```python
import jax
import jax.numpy as jnp
from jax import lax
from jax.experimental import pallas as pl
from jax.experimental.pallas import tpu as pltpu
from jax.sharding import PartitionSpec as P

GAMMA = 1.4
WENO_EPS = 1e-06
STEP_SIZE = 0.08
MESH = pl.DeviceIdType.MESH

XL, XH, YL, YH, ZL, ZH, MIR, ZLX, ZHX = range(9)
FLUX, SPEED, VEL, PRES, ROW = 5, 10, 11, 14, 15
CELL_ROWS = 18


def order_of(direction):
    return [direction % 3, (direction + 1) % 3, (direction + 2) % 3]


def cell_terms(fields, row):
    inverse = 1.0 / fields[0]
    velocity = [fields[1 + member] * inverse for member in range(3)]
    kinetic = 0.5 * sum(fields[1 + member] * velocity[member] for member in range(3))
    pressure = (GAMMA - 1.0) * (fields[4] - kinetic)
    contra = sum(row[member] * velocity[member] for member in range(3))
    fluxes = [fields[0] * contra]
    fluxes += [fields[1 + member] * contra + row[member] * pressure for member in range(3)]
    fluxes += [(fields[4] + pressure) * contra]
    size = sum(row[member] * row[member] for member in range(3))
    speed = jnp.abs(contra) + jnp.sqrt(GAMMA * pressure * inverse * size)
    return fluxes, speed, velocity, pressure


def weno_shift(d1, d2, d3, d4):
    s0, s1, s2 = d2 - d1, d3 - d2, d4 - d3
    q2 = d2 * d2 + WENO_EPS
    q3 = d3 * d3 + WENO_EPS
    b0 = s0 * ((4.0 / 3.0) * s0 + d2) + q2
    b1 = s1 * ((4.0 / 3.0) * s1 + d2) + q2
    b2 = s2 * ((4.0 / 3.0) * s2 - d3) + q3
    p01, p02, p12 = b0 * b1, b0 * b2, b1 * b2
    w0 = p12 * p12
    w1 = 6.0 * (p02 * p02)
    w2 = 3.0 * (p01 * p01)
    g0 = 2.0 * s0 + 3.0 * d2
    g1 = d2 + 2.0 * d3
    g2 = 3.0 * d3 - s2
    return (w0 * g0 + w1 * g1 + w2 * g2) / (w0 + w1 + w2)


def face_flux(get):
    alpha = get(SPEED, 0)
    for cell in range(1, 6):
        alpha = jnp.maximum(alpha, get(SPEED, cell))
    rho = 0.5 * (get(0, 2) + get(0, 3))
    ua, ub, uc = [0.5 * (get(VEL + m, 2) + get(VEL + m, 3)) for m in range(3)]
    pressure = 0.5 * (get(PRES, 2) + get(PRES, 3))
    sa, sb, sc = [get(ROW + m, 2) + get(ROW + m, 3) for m in range(3)]
    flat = sa * sa + sc * sc
    inv_flat = lax.rsqrt(flat)
    inv_size = lax.rsqrt(flat + sb * sb)
    na, nb, nc = sa * inv_size, sb * inv_size, sc * inv_size
    la, lc = -sc * inv_flat, sa * inv_flat
    ma, mb, mc = nb * lc, nc * la - na * lc, -nb * la
    c2 = GAMMA * pressure / rho
    ic = lax.rsqrt(c2)
    c = c2 * ic
    f = (GAMMA - 1.0) * ic * ic
    kinetic = 0.5 * (ua * ua + ub * ub + uc * uc)
    q = na * ua + nb * ub + nc * uc
    a = la * ua + lc * uc
    b = ma * ua + mb * ub + mc * uc
    f4 = 0.25 * f
    g4 = f4 * kinetic
    fa, fb, fc = f4 * ua, f4 * ub, f4 * uc
    i4 = 0.25 * ic
    q4, ia, ib, jc = i4 * q, i4 * na, i4 * nb, i4 * nc
    la2, lc2, a2 = 0.5 * la, 0.5 * lc, 0.5 * a
    ma2, mb2, mc2, b2 = 0.5 * ma, 0.5 * mb, 0.5 * mc, 0.5 * b

    def left(v):
        s = g4 * v[0] - (fa * v[1] + fb * v[2] + fc * v[3]) + f4 * v[4]
        t = q4 * v[0] - (ia * v[1] + ib * v[2] + jc * v[3])
        return [
            s + t,
            0.5 * v[0] - 2.0 * s,
            la2 * v[1] + lc2 * v[3] - a2 * v[0],
            ma2 * v[1] + mb2 * v[2] + mc2 * v[3] - b2 * v[0],
            s - t,
        ]

    up, down, middle = [], [], None
    for step in range(5):
        dq = [get(m, step + 1) - get(m, step) for m in range(5)]
        dg = [get(FLUX + m, step + 1) - get(FLUX + m, step) for m in range(5)]
        aq = [alpha * dq[m] for m in range(5)]
        if step < 4:
            up.append(left([dg[m] + aq[m] for m in range(5)]))
        if step > 0:
            down.append(left([dg[m] - aq[m] for m in range(5)]))
        if step == 2:
            middle = [0.5 * (get(FLUX + m, 2) + get(FLUX + m, 3) - aq[m]) for m in range(5)]
    chars = []
    for m in range(5):
        plus = weno_shift(up[0][m], up[1][m], up[2][m], up[3][m])
        minus = weno_shift(down[3][m], down[2][m], down[1][m], down[0][m])
        chars.append((1.0 / 6.0) * (plus - minus))
    ends = chars[0] + chars[4]
    total = ends + chars[1]
    along = c * (chars[4] - chars[0])
    energy = kinetic * total + (1.0 / (GAMMA - 1.0)) * c2 * ends + q * along + a * chars[2] + b * chars[3]
    return [
        middle[0] + total,
        middle[1] + (ua * total + na * along + la * chars[2] + ma * chars[3]),
        middle[2] + (ub * total + nb * along + mb * chars[3]),
        middle[3] + (uc * total + nc * along + lc * chars[2] + mc * chars[3]),
        middle[4] + energy,
    ]


def reversed_lanes(value):
    lane = lax.broadcasted_iota(jnp.int32, value.shape, 1)
    for bit in range(7):
        step = 1 << bit
        value = jnp.where((lane & step) == 0, pltpu.roll(value, 128 - step, 1), pltpu.roll(value, step, 1))
    return value


def kernel(
    q_hbm, s_hbm, inv_hbm, wake_hbm, rate_out, state_out,
    qv, sv, iv, wv, xl, xh, yl, yh, zl, zh, mir, ex, exh, ey, ez, fx, fy, fz, acc,
    send_sem, recv_sem, own_sem, far_send, far_recv, word,
):
    gx, gy, gz = lax.axis_index("gx"), lax.axis_index("gy"), lax.axis_index("gz")
    y = lax.rem(gz, 8)
    late = gz >= 8
    edge_low, edge_high = y == 0, y == 7
    edge = jnp.logical_or(edge_low, edge_high)
    far_late = jnp.logical_and(late, edge)
    far_early = jnp.logical_and(jnp.logical_not(late), edge)
    beside = jnp.logical_or(y == 1, y == 6)
    beside_far = jnp.logical_and(late, beside)
    corner = jnp.logical_and(gx == 0, gy == 0)
    lone, lone_far = jnp.logical_and(corner, gz == 0), jnp.logical_and(corner, gz == 15)
    by_x, by_y, by_z, by_mirror = [
        jnp.logical_and(jnp.logical_and(gx == i, gy == j), gz == k) for i, j, k in ((1, 0, 0), (0, 1, 0), (0, 0, 1), (3, 0, 0))
    ]
    adjacent = jnp.logical_or(jnp.logical_or(by_x, by_y), jnp.logical_or(by_z, by_mirror))
    relay = jnp.logical_and(jnp.logical_and(gz < 8, beside), jnp.logical_not(jnp.logical_and(corner, gz == 1)))
    wall, top = gy == 0, gy == 11
    inflow, outflow = gx == 0, gx == 3
    not_ = jnp.logical_not
    both = jnp.logical_and

    up_z = (gx, gy, lax.rem(gz + 1, 16))
    down_z = (gx, gy, lax.rem(gz + 15, 16))
    partner = (gx, gy, jnp.where(edge_low, down_z[2], up_z[2]))
    inner = (gx, gy, jnp.where(edge_low, up_z[2], down_z[2]))
    beyond = (gx, gy, jnp.where(jnp.logical_or(edge_low, y == 1), lax.rem(gz + 14, 16), lax.rem(gz + 2, 16)))
    outer = (gx, gy, jnp.where(y == 1, down_z[2], up_z[2]))
    row = [
        (not_(inflow), (gx - 1, gy, gz)),
        (not_(outflow), (gx + 1, gy, gz)),
        (not_(wall), (gx, gy - 1, gz)),
        (not_(top), (gx, gy + 1, gz)),
        (both(wall, jnp.logical_or(inflow, outflow)), (3 - gx, gy, gz)),
    ]
    spans = [(not_(edge_high), up_z, y + 1), (not_(edge_low), down_z, y - 1)]
    barrier = pltpu.get_barrier_semaphore()

    def signal(semaphore, target):
        pl.semaphore_signal(semaphore, inc=1, device_id=target, device_id_type=MESH)

    buffers = (xl, xh, yl, yh, zl, zh, mir, zl, zh)

    def copies(slot):
        target = {
            XL: (gx + 1, gy, gz),
            XH: (gx - 1, gy, gz),
            YL: (gx, gy + 1, gz),
            YH: (gx, gy - 1, gz),
            ZL: up_z,
            ZH: down_z,
            MIR: (3 - gx, gy, gz),
            ZLX: up_z,
            ZHX: down_z,
        }[slot]
        direction = {XL: 0, XH: 0, YL: 1, YH: 1, MIR: 1}.get(slot, 2)
        low, amount = {ZL: (1, 3), ZH: (0, 3), ZLX: (0, 1), ZHX: (3, 1)}.get(slot, (0, 4))
        pieces = [
            (q_hbm.at[:, pl.ds(low, amount)], buffers[slot].at[pl.ds(0, 5), pl.ds(low, amount)]),
            (s_hbm.at[pl.ds(3 * direction, 3), pl.ds(low, amount)], buffers[slot].at[pl.ds(5, 3), pl.ds(low, amount)]),
        ]
        return [
            pltpu.make_async_remote_copy(
                src_ref=source,
                dst_ref=landing,
                send_sem=send_sem.at[0 if slot in (XL, XH) else 1 if slot in (YL, YH, MIR) else 2],
                recv_sem=recv_sem.at[{ZLX: ZL, ZHX: ZH}.get(slot, slot)],
                device_id=target,
                device_id_type=MESH,
            )
            for source, landing in pieces
        ]

    def far_copies(slot, flow, metric, target):
        listed = []
        for stage in range(3):
            plane = {ZL: 3 - stage, ZH: stage}[slot]
            for source, landing in (
                (flow.at[:, plane], buffers[slot].at[pl.ds(0, 5), plane]),
                (metric.at[:, plane], buffers[slot].at[pl.ds(5, 3), plane]),
            ):
                listed.append(
                    pltpu.make_async_remote_copy(
                        src_ref=source,
                        dst_ref=landing,
                        send_sem=far_send,
                        recv_sem=far_recv.at[stage],
                        device_id=target,
                        device_id_type=MESH,
                    )
                )
        return listed

    def far_arrive(slot, stage):
        plane = 3 - stage if slot == ZL else stage
        pltpu.make_async_remote_copy(
            src_ref=buffers[slot].at[:, plane],
            dst_ref=buffers[slot].at[:, plane],
            send_sem=far_send,
            recv_sem=far_recv.at[stage],
            device_id=partner,
            device_id_type=MESH,
        ).wait_recv()

    def far_sent():
        pltpu.make_async_remote_copy(
            src_ref=zl.at[:, pl.ds(0, 3)],
            dst_ref=zl.at[:, pl.ds(0, 3)],
            send_sem=far_send,
            recv_sem=far_recv.at[0],
            device_id=partner,
            device_id_type=MESH,
        ).wait_send()

    def send_far():
        flow, metric = q_hbm, s_hbm.at[pl.ds(6, 3)]

        @pl.when(edge_high)
        def _():
            for copy in far_copies(ZL, flow, metric, partner):
                copy.start()

        @pl.when(edge_low)
        def _():
            for copy in far_copies(ZH, flow, metric, partner):
                copy.start()

    @pl.when(far_late)
    def _():
        pl.semaphore_wait(barrier, jnp.where(lone_far, 1, 2))

    @pl.when(far_late)
    def _():
        signal(word, (gx, gy, jnp.where(lone_far, partner[2], beyond[2])))

    turn = gy // 2

    @pl.when(both(far_late, both(edge_high, turn == 3)))
    def _():
        pl.delay(1000)

    @pl.when(both(far_late, both(edge_high, turn == 5)))
    def _():
        pl.delay(2000)

    @pl.when(far_late)
    def _():
        send_far()

    @pl.when(far_early)
    def _():
        signal(barrier, partner)

    @pl.when(relay)
    def _():
        signal(barrier, beyond)

    @pl.when(far_late)
    def _():
        signal(barrier, inner)

    @pl.when(not_(jnp.logical_or(far_late, lone)))
    def _():
        for there, target in row:
            @pl.when(there)
            def _():
                signal(barrier, target)
        for there, target, row_of in spans:
            target_far_late = both(late, jnp.logical_or(row_of == 0, row_of == 7))

            @pl.when(both(there, not_(target_far_late)))
            def _():
                signal(barrier, target)

    near_row = sum(there.astype(jnp.int32) for there, _ in row)
    near_span = sum(there.astype(jnp.int32) for there, _, _ in spans)

    @pl.when(not_(far_late))
    def _():
        pl.semaphore_wait(barrier, near_row + near_span - adjacent.astype(jnp.int32))


    own = [
        pltpu.make_async_copy(q_hbm, qv, own_sem.at[0]),
        pltpu.make_async_copy(s_hbm, sv, own_sem.at[0]),
        pltpu.make_async_copy(inv_hbm, iv, own_sem.at[1]),
        pltpu.make_async_copy(wake_hbm, wv, own_sem.at[2]),
    ]
    for copy in own:
        copy.start()

    @pl.when(far_late)
    def _():
        pl.semaphore_wait(word, 1)

    sends = [
        (XL, not_(outflow)),
        (XH, not_(inflow)),
        (YL, not_(top)),
        (YH, not_(wall)),
        (MIR, wall),
        (ZL, not_(edge_high)),
        (ZH, not_(edge_low)),
        (ZLX, both(both(edge_low, not_(late)), not_(lone))),
        (ZHX, both(edge_high, not_(late))),
    ]
    to_lone = {XH: by_x, YH: by_y, ZH: by_z, MIR: by_mirror}
    for slot, there in sends:
        @pl.when(both(there, not_(to_lone[slot])) if slot in to_lone else there)
        def _():
            for copy in copies(slot):
                copy.start()

    @pl.when(lone)
    def _():
        for target in ((1, 0, 0), (0, 1, 0), (0, 0, 1), (3, 0, 0)):
            signal(word, target)

    @pl.when(beside_far)
    def _():
        for there, target in row:
            @pl.when(there)
            def _():
                signal(word, target)
        pl.semaphore_wait(word, near_row)
        signal(word, outer)

    pltpu.make_async_copy(ex.at[pl.ds(0, 14), pl.ds(0, 4)], exh.at[pl.ds(0, 14), pl.ds(0, 4)], own_sem.at[0]).wait()
    own[2].wait()
    own[3].wait()

    def awaited(ref, slot, group):
        return pltpu.make_async_remote_copy(
            src_ref=ref,
            dst_ref=ref,
            send_sem=send_sem.at[group],
            recv_sem=recv_sem.at[slot],
            device_id=up_z,
            device_id_type=MESH,
        )

    def arrive(slot, low=0, amount=4):
        awaited(buffers[slot].at[:, pl.ds(low, amount)], slot, 0).wait_recv()

    def sent(group, fields, amount):
        awaited(ex.at[pl.ds(0, fields), pl.ds(0, amount)], 0, group).wait_send()

    lane = lax.broadcasted_iota(jnp.int32, (8, 128), 1)

    def fill(array, index):
        fields = [array[(m,) + index] for m in range(5)]
        metric = [array[(ROW + m,) + index] for m in range(3)]
        fluxes, speed, velocity, pressure = cell_terms(fields, metric)
        for m in range(5):
            array[(FLUX + m,) + index] = fluxes[m]
        array[(SPEED,) + index] = speed
        for m in range(3):
            array[(VEL + m,) + index] = velocity[m]
        array[(PRES,) + index] = pressure

    def raw_rows(direction):
        cyclic = order_of(direction)
        listed = [(0, 0, None), (4, 4, None)]
        for m in range(3):
            listed.append((1 + m, 1 + cyclic[m], None))
            listed.append((ROW + m, None, cyclic[m]))
        return listed

    @pl.when(adjacent)
    def _():
        pl.semaphore_wait(word, 1)
        for slot, there in to_lone.items():
            @pl.when(there)
            def _():
                for copy in copies(slot):
                    copy.start()

    @pl.when(not_(inflow))
    def _():
        arrive(XL)

    @pl.when(inflow)
    def _():
        for k in range(4):
            for f in range(5):
                xl[f, k] = jnp.broadcast_to(qv[f, k, :, 0:1], (8, 128))
            for f in range(3):
                xl[5 + f, k] = jnp.broadcast_to(sv[f, k, :, 0:1], (8, 128))

    @pl.when(not_(outflow))
    def _():
        arrive(XH)

    @pl.when(outflow)
    def _():
        for k in range(4):
            for f in range(5):
                xh[f, k] = jnp.broadcast_to(qv[f, k, :, 127:128], (8, 128))
            for f in range(3):
                xh[5 + f, k] = jnp.broadcast_to(sv[f, k, :, 127:128], (8, 128))

    for out, flow, metric in raw_rows(0):
        halo = flow if flow is not None else 5 + metric
        packed = None
        for k in range(4):
            centre = qv[flow, k] if flow is not None else sv[metric, k]
            ring = jnp.where(lane < 64, xh[halo, k], xl[halo, k])
            ex[out, k] = centre
            exh[out, k] = ring
            moved = pltpu.roll(jnp.where(lane < 64, ring, centre), (32 * k + 3) % 128, 1)
            packed = moved if packed is None else jnp.where(lane < 32 * k, packed, moved)
        ex[out, 4] = packed
        exh[out, 4] = packed

    def fill_x(k, carry):
        fill(ex, (k,))
        fill(exh, (k,))
        return carry

    lax.fori_loop(0, 5, fill_x, 0)

    def face_x(k, carry):
        cache = {}

        def get(r, cell):
            if (r, cell) not in cache:
                shift = 3 - cell
                centre = ex[r, k]
                if shift > 0:
                    centre = pltpu.roll(jnp.where(lane >= 128 - shift, exh[r, k], centre), shift, 1)
                elif shift < 0:
                    centre = pltpu.roll(jnp.where(lane < -shift, exh[r, k], centre), 128 + shift, 1)
                cache[(r, cell)] = centre
            return cache[(r, cell)]

        flux = face_flux(get)
        for m in range(5):
            fx[m, k] = flux[m]
        return carry

    lax.fori_loop(0, 5, face_x, 0)
    for k in range(4):
        for m in range(5):
            upper = pltpu.roll(fx[m, k], 127, 1)
            last = pltpu.roll(fx[m, 4], (124 - 32 * k) % 128, 1)
            acc[m, k] = jnp.where(lane == 127, last, upper) - fx[m, k]

    @pl.when(wall)
    def _():
        arrive(MIR)
        is_wake = jnp.broadcast_to(wv[0:1, :], (8, 128)) >= 0
        for f in range(8):
            for k in range(4):
                mirrored = reversed_lanes(mir[f, k])
                beside = qv[f, k] if f < 5 else sv[f - 2, k]
                if f in (1, 2, 3):
                    beside = -beside
                ghost = jnp.where(is_wake, mirrored, beside)
                for g in range(3):
                    yl[f, k, 7 - g : 8 - g, :] = ghost[g : g + 1, :]

    @pl.when(not_(wall))
    def _():
        arrive(YL)

    @pl.when(top)
    def _():
        for f in range(8):
            for k in range(4):
                source = qv[f, k, 7:8, :] if f < 5 else sv[f - 2, k, 7:8, :]
                yh[f, k] = jnp.broadcast_to(source, (8, 128))

    @pl.when(not_(top))
    def _():
        arrive(YH)

    for out, flow, metric in raw_rows(1):
        halo = flow if flow is not None else 5 + metric
        for k in range(4):
            base = 14 * k
            ey[out, base : base + 3, :] = yl[halo, k, 5:8, :]
            ey[out, base + 3 : base + 11, :] = qv[flow, k] if flow is not None else sv[3 + metric, k]
            ey[out, base + 11 : base + 14, :] = yh[halo, k, 0:3, :]
        ey[out, 56:64, :] = qv[flow, 3] if flow is not None else sv[3 + metric, 3]

    def fill_y(k, carry):
        fill(ey, (pl.ds(pl.multiple_of(8 * k, 8), 8),))
        return carry

    lax.fori_loop(0, 8, fill_y, 0)

    def face_y(k, carry):
        cache = {}

        def get(r, cell):
            if (r, cell) not in cache:
                cache[(r, cell)] = ey[r, pl.ds(8 * k + cell, 8), :]
            return cache[(r, cell)]

        flux = face_flux(get)
        for m in range(5):
            fy[m, pl.ds(pl.multiple_of(8 * k, 8), 8), :] = flux[m]
        return carry

    lax.fori_loop(0, 7, face_y, 0)
    cyclic = order_of(1)
    for k in range(4):
        for m in range(5):
            target = 1 + cyclic[m - 1] if 1 <= m <= 3 else m
            acc[target, k] += fy[m, 14 * k + 1 : 14 * k + 9, :] - fy[m, 14 * k : 14 * k + 8, :]

    def fill_z(first, last):
        def body(k, carry):
            fill(ez, (k,))
            return carry

        lax.fori_loop(first, last, body, 0)

    def take_plane(halo_ref, cell, plane):
        for out, flow, metric in raw_rows(2):
            halo = flow if flow is not None else 5 + metric
            ez[out, cell] = halo_ref[halo, plane]

    def take_z(halo_ref, base, low):
        for k in range(3):
            take_plane(halo_ref, base + k, low + k)

    def face_z(k, carry):
        cache = {}

        def get(r, cell):
            if (r, cell) not in cache:
                cache[(r, cell)] = ez[r, k + cell]
            return cache[(r, cell)]

        flux = face_flux(get)
        for m in range(5):
            fz[m, k] = flux[m]
        return carry

    for out, flow, metric in raw_rows(2):
        for k in range(4):
            ez[out, 3 + k] = qv[flow, k] if flow is not None else sv[6 + metric, k]
    fill_z(3, 7)

    def low_z():
        passing = both(relay, y == 1)

        @pl.when(passing)
        def _():
            arrive(ZL)

        @pl.when(not_(passing))
        def _():
            arrive(ZL, 1, 3)

        take_z(zl, 0, 1)
        fill_z(0, 3)

    def high_z():
        passing = both(relay, y == 6)

        @pl.when(passing)
        def _():
            arrive(ZH)

        @pl.when(not_(passing))
        def _():
            arrive(ZH, 0, 3)

        take_z(zh, 7, 0)
        fill_z(7, 10)

    @pl.when(not_(edge_low))
    def _():
        low_z()

    @pl.when(not_(edge_high))
    def _():
        high_z()

    early_first = jnp.where(edge_low, 3, 0)
    early_last = jnp.where(edge_low, 5, jnp.where(edge_high, 2, 5))
    lax.fori_loop(early_first, early_last, face_z, 0)

    @pl.when(lone)
    def _():
        pl.semaphore_wait(word, 1)
        send_far()

    extra = both(edge, both(not_(late), not_(lone)))
    for group, fields, amount, there in (
        (0, 16, 4, not_(jnp.logical_or(inflow, outflow))),
        (0, 8, 4, jnp.logical_or(inflow, outflow)),
        (1, 16, 4, not_(top)),
        (1, 8, 4, top),
        (2, 16, 3, not_(edge)),
        (2, 8, 4, extra),
        (2, 8, 3, both(edge, not_(extra))),
    ):
        @pl.when(there)
        def _():
            sent(group, fields, amount)

    spanwise = order_of(2)

    def finish(k):
        for m in range(5):
            target = 1 + spanwise[m - 1] if 1 <= m <= 3 else m
            rate = -iv[k] * (acc[target, k] + (fz[m, k + 1] - fz[m, k]))
            rate_out[target, k] = rate
            state_out[target, k] = qv[target, k] + STEP_SIZE * rate

    @pl.when(not_(edge))
    def _():
        for k in range(4):
            finish(k)

    @pl.when(edge)
    def _():
        finish(jnp.where(edge_low, 3, 0))

        def body(stage, carry):
            @pl.when(edge_low)
            def _():
                far_arrive(ZL, stage)
                take_plane(zl, 2 - stage, 3 - stage)
                fill(ez, (2 - stage,))

            @pl.when(edge_high)
            def _():
                far_arrive(ZH, stage)
                take_plane(zh, 7 + stage, stage)
                fill(ez, (7 + stage,))

            carry = face_z(jnp.where(edge_low, 2 - stage, 2 + stage), carry)
            finish(jnp.where(edge_low, 2 - stage, 1 + stage))
            return carry

        lax.fori_loop(0, 3, body, 0)

    @pl.when(both(relay, y == 1))
    def _():
        pl.semaphore_wait(word, 1)

        @pl.when(turn == 3)
        def _():
            pl.delay(1000)

        @pl.when(turn == 5)
        def _():
            pl.delay(2000)

        for copy in far_copies(ZH, zl.at[pl.ds(0, 5)], zl.at[pl.ds(5, 3)], beyond):
            copy.start()

    @pl.when(both(relay, y == 6))
    def _():
        pl.semaphore_wait(word, 1)
        for copy in far_copies(ZL, zh.at[pl.ds(0, 5)], zh.at[pl.ds(5, 3)], beyond):
            copy.start()

    @pl.when(jnp.logical_or(relay, jnp.logical_or(far_late, lone)))
    def _():
        far_sent()


def deliver(state, rate, state_out, rate_out, sem):
    copies = [
        pltpu.make_async_copy(state, state_out, sem.at[0]),
        pltpu.make_async_copy(rate, rate_out, sem.at[1]),
    ]
    for copy in copies:
        copy.start()
    for copy in copies:
        copy.wait()


def local(conserved, metrics, inv_volume, wake_donor):
    block = conserved.shape
    planes, rows, lanes = block[1:]
    wide = pltpu.VMEM(block, jnp.float32)
    f32 = lambda *shape: pltpu.VMEM(shape, jnp.float32)
    rate, state = pl.pallas_call(
        kernel,
        out_shape=(wide, wide),
        in_specs=[pl.BlockSpec(memory_space=pltpu.HBM)] * 4,
        out_specs=[pl.BlockSpec(memory_space=pltpu.VMEM)] * 2,
        scratch_shapes=[
            f32(*block),
            f32(9, planes, rows, lanes),
            f32(planes, rows, lanes),
            pltpu.VMEM((1, lanes), jnp.int32),
            *[f32(8, planes, rows, lanes)] * 4,
            *[f32(8, planes, rows, lanes)] * 2,
            f32(8, planes, rows, lanes),
            f32(CELL_ROWS, 5, rows, lanes),
            f32(CELL_ROWS, 5, rows, lanes),
            f32(CELL_ROWS, 64, lanes),
            f32(CELL_ROWS, 10, rows, lanes),
            f32(5, 5, rows, lanes),
            f32(5, 56, lanes),
            f32(5, 5, rows, lanes),
            f32(*block),
            pltpu.SemaphoreType.DMA((3,)),
            pltpu.SemaphoreType.DMA((7,)),
            pltpu.SemaphoreType.DMA((3,)),
            pltpu.SemaphoreType.DMA,
            pltpu.SemaphoreType.DMA((3,)),
            pltpu.SemaphoreType.REGULAR,
        ],
        compiler_params=pltpu.CompilerParams(collective_id=0, has_side_effects=True),
    )(conserved, metrics, inv_volume, wake_donor[None])
    return pl.pallas_call(
        deliver,
        out_shape=(jax.ShapeDtypeStruct(block, jnp.float32),) * 2,
        in_specs=[pl.BlockSpec(memory_space=pl.ANY)] * 2,
        out_specs=[pl.BlockSpec(memory_space=pltpu.HBM)] * 2,
        scratch_shapes=[pltpu.SemaphoreType.DMA((2,))],
    )(pltpu.with_memory_space_constraint(state, pltpu.VMEM), pltpu.with_memory_space_constraint(rate, pltpu.VMEM))


def solution(mesh):
    placed = (P(None, "gz", "gy", "gx"), P(None, "gz", "gy", "gx"), P("gz", "gy", "gx"), P("gx"))
    return jax.shard_map(
        local,
        mesh=mesh,
        in_specs=placed,
        out_specs=(P(None, "gz", "gy", "gx"), P(None, "gz", "gy", "gx")),
        check_vma=False,
    )
```

```python
import jax
import jax.numpy as jnp
from jax import lax
from jax.experimental import pallas as pl
from jax.experimental.pallas import tpu as pltpu
from jax.sharding import PartitionSpec as P

GAMMA = 1.4
WENO_EPS = 1e-06
STEP_SIZE = 0.08
MESH = pl.DeviceIdType.MESH

XL, XH, YL, YH, ZL, ZH, MIR, ZLX, ZHX = range(9)
FLUX, SPEED, VEL, PRES, ROW = 5, 10, 11, 14, 15
CELL_ROWS = 18


def order_of(direction):
    return [direction % 3, (direction + 1) % 3, (direction + 2) % 3]


def cell_terms(fields, row):
    inverse = 1.0 / fields[0]
    velocity = [fields[1 + member] * inverse for member in range(3)]
    kinetic = 0.5 * sum(fields[1 + member] * velocity[member] for member in range(3))
    pressure = (GAMMA - 1.0) * (fields[4] - kinetic)
    contra = sum(row[member] * velocity[member] for member in range(3))
    fluxes = [fields[0] * contra]
    fluxes += [fields[1 + member] * contra + row[member] * pressure for member in range(3)]
    fluxes += [(fields[4] + pressure) * contra]
    size = sum(row[member] * row[member] for member in range(3))
    speed = jnp.abs(contra) + jnp.sqrt(GAMMA * pressure * inverse * size)
    return fluxes, speed, velocity, pressure


def weno_shift(d1, d2, d3, d4):
    s0, s1, s2 = d2 - d1, d3 - d2, d4 - d3
    q2 = d2 * d2 + WENO_EPS
    q3 = d3 * d3 + WENO_EPS
    b0 = s0 * ((4.0 / 3.0) * s0 + d2) + q2
    b1 = s1 * ((4.0 / 3.0) * s1 + d2) + q2
    b2 = s2 * ((4.0 / 3.0) * s2 - d3) + q3
    p01, p02, p12 = b0 * b1, b0 * b2, b1 * b2
    w0 = p12 * p12
    w1 = 6.0 * (p02 * p02)
    w2 = 3.0 * (p01 * p01)
    g0 = 2.0 * s0 + 3.0 * d2
    g1 = d2 + 2.0 * d3
    g2 = 3.0 * d3 - s2
    return (w0 * g0 + w1 * g1 + w2 * g2) / (w0 + w1 + w2)


def face_flux(get):
    alpha = get(SPEED, 0)
    for cell in range(1, 6):
        alpha = jnp.maximum(alpha, get(SPEED, cell))
    rho = 0.5 * (get(0, 2) + get(0, 3))
    ua, ub, uc = [0.5 * (get(VEL + m, 2) + get(VEL + m, 3)) for m in range(3)]
    pressure = 0.5 * (get(PRES, 2) + get(PRES, 3))
    sa, sb, sc = [get(ROW + m, 2) + get(ROW + m, 3) for m in range(3)]
    flat = sa * sa + sc * sc
    inv_flat = lax.rsqrt(flat)
    inv_size = lax.rsqrt(flat + sb * sb)
    na, nb, nc = sa * inv_size, sb * inv_size, sc * inv_size
    la, lc = -sc * inv_flat, sa * inv_flat
    ma, mb, mc = nb * lc, nc * la - na * lc, -nb * la
    c2 = GAMMA * pressure / rho
    ic = lax.rsqrt(c2)
    c = c2 * ic
    f = (GAMMA - 1.0) * ic * ic
    kinetic = 0.5 * (ua * ua + ub * ub + uc * uc)
    q = na * ua + nb * ub + nc * uc
    a = la * ua + lc * uc
    b = ma * ua + mb * ub + mc * uc
    f4 = 0.25 * f
    g4 = f4 * kinetic
    fa, fb, fc = f4 * ua, f4 * ub, f4 * uc
    i4 = 0.25 * ic
    q4, ia, ib, jc = i4 * q, i4 * na, i4 * nb, i4 * nc
    la2, lc2, a2 = 0.5 * la, 0.5 * lc, 0.5 * a
    ma2, mb2, mc2, b2 = 0.5 * ma, 0.5 * mb, 0.5 * mc, 0.5 * b

    def left(v):
        s = g4 * v[0] - (fa * v[1] + fb * v[2] + fc * v[3]) + f4 * v[4]
        t = q4 * v[0] - (ia * v[1] + ib * v[2] + jc * v[3])
        return [
            s + t,
            0.5 * v[0] - 2.0 * s,
            la2 * v[1] + lc2 * v[3] - a2 * v[0],
            ma2 * v[1] + mb2 * v[2] + mc2 * v[3] - b2 * v[0],
            s - t,
        ]

    up, down, middle = [], [], None
    for step in range(5):
        dq = [get(m, step + 1) - get(m, step) for m in range(5)]
        dg = [get(FLUX + m, step + 1) - get(FLUX + m, step) for m in range(5)]
        aq = [alpha * dq[m] for m in range(5)]
        if step < 4:
            up.append(left([dg[m] + aq[m] for m in range(5)]))
        if step > 0:
            down.append(left([dg[m] - aq[m] for m in range(5)]))
        if step == 2:
            middle = [0.5 * (get(FLUX + m, 2) + get(FLUX + m, 3) - aq[m]) for m in range(5)]
    chars = []
    for m in range(5):
        plus = weno_shift(up[0][m], up[1][m], up[2][m], up[3][m])
        minus = weno_shift(down[3][m], down[2][m], down[1][m], down[0][m])
        chars.append((1.0 / 6.0) * (plus - minus))
    ends = chars[0] + chars[4]
    total = ends + chars[1]
    along = c * (chars[4] - chars[0])
    energy = kinetic * total + (1.0 / (GAMMA - 1.0)) * c2 * ends + q * along + a * chars[2] + b * chars[3]
    return [
        middle[0] + total,
        middle[1] + (ua * total + na * along + la * chars[2] + ma * chars[3]),
        middle[2] + (ub * total + nb * along + mb * chars[3]),
        middle[3] + (uc * total + nc * along + lc * chars[2] + mc * chars[3]),
        middle[4] + energy,
    ]


def reversed_lanes(value):
    lane = lax.broadcasted_iota(jnp.int32, value.shape, 1)
    for bit in range(7):
        step = 1 << bit
        value = jnp.where((lane & step) == 0, pltpu.roll(value, 128 - step, 1), pltpu.roll(value, step, 1))
    return value


def kernel(
    q_hbm, s_hbm, inv_hbm, wake_hbm, rate_out, state_out,
    qv, sv, iv, wv, xl, xh, yl, yh, zl, zh, mir, ex, exh, ey, ez, fx, fy, fz, acc,
    send_sem, recv_sem, own_sem, far_send, far_recv, word,
):
    gx, gy, gz = lax.axis_index("gx"), lax.axis_index("gy"), lax.axis_index("gz")
    y = lax.rem(gz, 8)
    late = gz >= 8
    edge_low, edge_high = y == 0, y == 7
    edge = jnp.logical_or(edge_low, edge_high)
    far_late = jnp.logical_and(late, edge)
    far_early = jnp.logical_and(jnp.logical_not(late), edge)
    beside = jnp.logical_or(y == 1, y == 6)
    beside_far = jnp.logical_and(late, beside)
    corner = jnp.logical_and(gx == 0, gy == 0)
    lone, lone_far = jnp.logical_and(corner, gz == 0), jnp.logical_and(corner, gz == 15)
    by_x, by_y, by_z, by_mirror = [
        jnp.logical_and(jnp.logical_and(gx == i, gy == j), gz == k) for i, j, k in ((1, 0, 0), (0, 1, 0), (0, 0, 1), (3, 0, 0))
    ]
    adjacent = jnp.logical_or(jnp.logical_or(by_x, by_y), jnp.logical_or(by_z, by_mirror))
    relay = jnp.logical_and(jnp.logical_and(gz < 8, beside), jnp.logical_not(jnp.logical_and(corner, gz == 1)))
    wall, top = gy == 0, gy == 11
    inflow, outflow = gx == 0, gx == 3
    not_ = jnp.logical_not
    both = jnp.logical_and

    up_z = (gx, gy, lax.rem(gz + 1, 16))
    down_z = (gx, gy, lax.rem(gz + 15, 16))
    partner = (gx, gy, jnp.where(edge_low, down_z[2], up_z[2]))
    inner = (gx, gy, jnp.where(edge_low, up_z[2], down_z[2]))
    beyond = (gx, gy, jnp.where(jnp.logical_or(edge_low, y == 1), lax.rem(gz + 14, 16), lax.rem(gz + 2, 16)))
    outer = (gx, gy, jnp.where(y == 1, down_z[2], up_z[2]))
    row = [
        (not_(inflow), (gx - 1, gy, gz)),
        (not_(outflow), (gx + 1, gy, gz)),
        (not_(wall), (gx, gy - 1, gz)),
        (not_(top), (gx, gy + 1, gz)),
        (both(wall, jnp.logical_or(inflow, outflow)), (3 - gx, gy, gz)),
    ]
    spans = [(not_(edge_high), up_z, y + 1), (not_(edge_low), down_z, y - 1)]
    barrier = pltpu.get_barrier_semaphore()

    def signal(semaphore, target):
        pl.semaphore_signal(semaphore, inc=1, device_id=target, device_id_type=MESH)

    buffers = (xl, xh, yl, yh, zl, zh, mir, zl, zh)

    direction_of = {XL: 0, XH: 0, YL: 1, YH: 1, MIR: 1, ZL: 2, ZH: 2, ZLX: 2, ZHX: 2}

    def copies(slot):
        target = {
            XL: (gx + 1, gy, gz),
            XH: (gx - 1, gy, gz),
            YL: (gx, gy + 1, gz),
            YH: (gx, gy - 1, gz),
            ZL: up_z,
            ZH: down_z,
            MIR: (3 - gx, gy, gz),
            ZLX: up_z,
            ZHX: down_z,
        }[slot]
        direction = direction_of[slot]
        low, amount = {ZL: (1, 3), ZH: (0, 3), ZLX: (0, 1), ZHX: (3, 1)}.get(slot, (0, 4))
        pieces = [
            (q_hbm.at[:, pl.ds(low, amount)], buffers[slot].at[pl.ds(0, 5), pl.ds(low, amount)]),
            (s_hbm.at[pl.ds(3 * direction, 3), pl.ds(low, amount)], buffers[slot].at[pl.ds(5, 3), pl.ds(low, amount)]),
        ]
        return [
            pltpu.make_async_remote_copy(
                src_ref=source,
                dst_ref=landing,
                send_sem=send_sem.at[direction_of[slot]],
                recv_sem=recv_sem.at[direction_of[slot]],
                device_id=target,
                device_id_type=MESH,
            )
            for source, landing in pieces
        ]

    def far_copies(slot, flow, metric, target):
        listed = []
        for stage in range(3):
            plane = {ZL: 3 - stage, ZH: stage}[slot]
            for source, landing in (
                (flow.at[:, plane], buffers[slot].at[pl.ds(0, 5), plane]),
                (metric.at[:, plane], buffers[slot].at[pl.ds(5, 3), plane]),
            ):
                listed.append(
                    pltpu.make_async_remote_copy(
                        src_ref=source,
                        dst_ref=landing,
                        send_sem=far_send,
                        recv_sem=far_recv.at[stage],
                        device_id=target,
                        device_id_type=MESH,
                    )
                )
        return listed

    def far_arrive(slot, stage):
        plane = 3 - stage if slot == ZL else stage
        pltpu.make_async_remote_copy(
            src_ref=buffers[slot].at[:, plane],
            dst_ref=buffers[slot].at[:, plane],
            send_sem=far_send,
            recv_sem=far_recv.at[stage],
            device_id=partner,
            device_id_type=MESH,
        ).wait_recv()

    def far_sent():
        pltpu.make_async_remote_copy(
            src_ref=zl.at[:, pl.ds(0, 3)],
            dst_ref=zl.at[:, pl.ds(0, 3)],
            send_sem=far_send,
            recv_sem=far_recv.at[0],
            device_id=partner,
            device_id_type=MESH,
        ).wait_send()

    def send_far():
        flow, metric = q_hbm, s_hbm.at[pl.ds(6, 3)]

        @pl.when(edge_high)
        def _():
            for copy in far_copies(ZL, flow, metric, partner):
                copy.start()

        @pl.when(edge_low)
        def _():
            for copy in far_copies(ZH, flow, metric, partner):
                copy.start()

    @pl.when(far_late)
    def _():
        pl.semaphore_wait(barrier, jnp.where(lone_far, 1, 2))

    @pl.when(far_late)
    def _():
        signal(word, (gx, gy, jnp.where(lone_far, partner[2], beyond[2])))

    turn = gy // 2

    @pl.when(both(far_late, both(edge_high, turn == 3)))
    def _():
        pl.delay(1000)

    @pl.when(both(far_late, both(edge_high, turn == 5)))
    def _():
        pl.delay(2000)

    @pl.when(far_late)
    def _():
        send_far()

    @pl.when(far_early)
    def _():
        signal(barrier, partner)

    @pl.when(relay)
    def _():
        signal(barrier, beyond)

    @pl.when(far_late)
    def _():
        signal(barrier, inner)

    @pl.when(not_(jnp.logical_or(far_late, lone)))
    def _():
        for there, target in row:
            @pl.when(there)
            def _():
                signal(barrier, target)
        for there, target, row_of in spans:
            target_far_late = both(late, jnp.logical_or(row_of == 0, row_of == 7))

            @pl.when(both(there, not_(target_far_late)))
            def _():
                signal(barrier, target)

    near_row = sum(there.astype(jnp.int32) for there, _ in row)
    near_span = sum(there.astype(jnp.int32) for there, _, _ in spans)

    @pl.when(not_(far_late))
    def _():
        pl.semaphore_wait(barrier, near_row + near_span - adjacent.astype(jnp.int32))


    own = [
        pltpu.make_async_copy(q_hbm, qv, own_sem.at[0]),
        pltpu.make_async_copy(s_hbm, sv, own_sem.at[0]),
        pltpu.make_async_copy(inv_hbm, iv, own_sem.at[0]),
        pltpu.make_async_copy(wake_hbm, wv, own_sem.at[1]),
    ]
    for copy in own:
        copy.start()

    @pl.when(far_late)
    def _():
        pl.semaphore_wait(word, 1)

    sends = [
        (XL, not_(outflow)),
        (XH, not_(inflow)),
        (YL, not_(top)),
        (YH, not_(wall)),
        (MIR, wall),
        (ZL, not_(edge_high)),
        (ZH, not_(edge_low)),
        (ZLX, both(both(edge_low, not_(late)), not_(lone))),
        (ZHX, both(edge_high, not_(late))),
    ]
    to_lone = {XH: by_x, YH: by_y, ZH: by_z, MIR: by_mirror}
    for slot, there in sends:
        @pl.when(both(there, not_(to_lone[slot])) if slot in to_lone else there)
        def _():
            for copy in copies(slot):
                copy.start()

    @pl.when(lone)
    def _():
        for target in ((1, 0, 0), (0, 1, 0), (0, 0, 1), (3, 0, 0)):
            signal(word, target)

    @pl.when(beside_far)
    def _():
        for there, target in row:
            @pl.when(there)
            def _():
                signal(word, target)
        pl.semaphore_wait(word, near_row)
        signal(word, outer)

    pltpu.make_async_copy(ex.at[pl.ds(0, 15), pl.ds(0, 4)], exh.at[pl.ds(0, 15), pl.ds(0, 4)], own_sem.at[0]).wait()
    own[3].wait()

    def all_of(direction, fields, amount):
        ref = ex.at[pl.ds(0, fields), pl.ds(0, amount)]
        return pltpu.make_async_remote_copy(
            src_ref=ref,
            dst_ref=ref,
            send_sem=send_sem.at[direction],
            recv_sem=recv_sem.at[direction],
            device_id=up_z,
            device_id_type=MESH,
        )

    def arrive(direction, counts):
        for fields, amount, there in counts:
            @pl.when(there)
            def _():
                all_of(direction, fields, amount).wait_recv()

    lane = lax.broadcasted_iota(jnp.int32, (8, 128), 1)

    def fill(array, index):
        fields = [array[(m,) + index] for m in range(5)]
        metric = [array[(ROW + m,) + index] for m in range(3)]
        fluxes, speed, velocity, pressure = cell_terms(fields, metric)
        for m in range(5):
            array[(FLUX + m,) + index] = fluxes[m]
        array[(SPEED,) + index] = speed
        for m in range(3):
            array[(VEL + m,) + index] = velocity[m]
        array[(PRES,) + index] = pressure

    def raw_rows(direction):
        cyclic = order_of(direction)
        listed = [(0, 0, None), (4, 4, None)]
        for m in range(3):
            listed.append((1 + m, 1 + cyclic[m], None))
            listed.append((ROW + m, None, cyclic[m]))
        return listed

    @pl.when(adjacent)
    def _():
        pl.semaphore_wait(word, 1)
        for slot, there in to_lone.items():
            @pl.when(there)
            def _():
                for copy in copies(slot):
                    copy.start()

    x_end = jnp.logical_or(inflow, outflow)
    arrive(0, ((16, 4, not_(x_end)), (8, 4, x_end)))

    @pl.when(inflow)
    def _():
        for k in range(4):
            for f in range(5):
                xl[f, k] = jnp.broadcast_to(qv[f, k, :, 0:1], (8, 128))
            for f in range(3):
                xl[5 + f, k] = jnp.broadcast_to(sv[f, k, :, 0:1], (8, 128))

    @pl.when(outflow)
    def _():
        for k in range(4):
            for f in range(5):
                xh[f, k] = jnp.broadcast_to(qv[f, k, :, 127:128], (8, 128))
            for f in range(3):
                xh[5 + f, k] = jnp.broadcast_to(sv[f, k, :, 127:128], (8, 128))

    for out, flow, metric in raw_rows(0):
        halo = flow if flow is not None else 5 + metric
        packed = None
        for k in range(4):
            centre = qv[flow, k] if flow is not None else sv[metric, k]
            ring = jnp.where(lane < 64, xh[halo, k], xl[halo, k])
            ex[out, k] = centre
            exh[out, k] = ring
            moved = pltpu.roll(jnp.where(lane < 64, ring, centre), (32 * k + 3) % 128, 1)
            packed = moved if packed is None else jnp.where(lane < 32 * k, packed, moved)
        ex[out, 4] = packed
        exh[out, 4] = packed

    def fill_x(k, carry):
        fill(ex, (k,))
        fill(exh, (k,))
        return carry

    lax.fori_loop(0, 5, fill_x, 0)

    def face_x(k, carry):
        cache = {}

        def get(r, cell):
            if (r, cell) not in cache:
                shift = 3 - cell
                centre = ex[r, k]
                if shift > 0:
                    centre = pltpu.roll(jnp.where(lane >= 128 - shift, exh[r, k], centre), shift, 1)
                elif shift < 0:
                    centre = pltpu.roll(jnp.where(lane < -shift, exh[r, k], centre), 128 + shift, 1)
                cache[(r, cell)] = centre
            return cache[(r, cell)]

        flux = face_flux(get)
        for m in range(5):
            fx[m, k] = flux[m]
        return carry

    lax.fori_loop(0, 5, face_x, 0)
    for k in range(4):
        for m in range(5):
            upper = pltpu.roll(fx[m, k], 127, 1)
            last = pltpu.roll(fx[m, 4], (124 - 32 * k) % 128, 1)
            acc[m, k] = jnp.where(lane == 127, last, upper) - fx[m, k]

    arrive(1, ((16, 4, not_(top)), (8, 4, top)))

    @pl.when(wall)
    def _():
        is_wake = jnp.broadcast_to(wv[0:1, :], (8, 128)) >= 0
        for f in range(8):
            for k in range(4):
                mirrored = reversed_lanes(mir[f, k])
                beside = qv[f, k] if f < 5 else sv[f - 2, k]
                if f in (1, 2, 3):
                    beside = -beside
                ghost = jnp.where(is_wake, mirrored, beside)
                for g in range(3):
                    yl[f, k, 7 - g : 8 - g, :] = ghost[g : g + 1, :]

    @pl.when(top)
    def _():
        for f in range(8):
            for k in range(4):
                source = qv[f, k, 7:8, :] if f < 5 else sv[f - 2, k, 7:8, :]
                yh[f, k] = jnp.broadcast_to(source, (8, 128))

    for out, flow, metric in raw_rows(1):
        halo = flow if flow is not None else 5 + metric
        for k in range(4):
            base = 14 * k
            ey[out, base : base + 3, :] = yl[halo, k, 5:8, :]
            ey[out, base + 3 : base + 11, :] = qv[flow, k] if flow is not None else sv[3 + metric, k]
            ey[out, base + 11 : base + 14, :] = yh[halo, k, 0:3, :]
        ey[out, 56:64, :] = qv[flow, 3] if flow is not None else sv[3 + metric, 3]

    def fill_y(k, carry):
        fill(ey, (pl.ds(pl.multiple_of(8 * k, 8), 8),))
        return carry

    lax.fori_loop(0, 8, fill_y, 0)

    def face_y(k, carry):
        cache = {}

        def get(r, cell):
            if (r, cell) not in cache:
                cache[(r, cell)] = ey[r, pl.ds(8 * k + cell, 8), :]
            return cache[(r, cell)]

        flux = face_flux(get)
        for m in range(5):
            fy[m, pl.ds(pl.multiple_of(8 * k, 8), 8), :] = flux[m]
        return carry

    lax.fori_loop(0, 7, face_y, 0)
    cyclic = order_of(1)
    for k in range(4):
        for m in range(5):
            target = 1 + cyclic[m - 1] if 1 <= m <= 3 else m
            acc[target, k] += fy[m, 14 * k + 1 : 14 * k + 9, :] - fy[m, 14 * k : 14 * k + 8, :]

    def fill_z(first, last):
        def body(k, carry):
            fill(ez, (k,))
            return carry

        lax.fori_loop(first, last, body, 0)

    def take_plane(halo_ref, cell, plane):
        for out, flow, metric in raw_rows(2):
            halo = flow if flow is not None else 5 + metric
            ez[out, cell] = halo_ref[halo, plane]

    def take_z(halo_ref, base, low):
        for k in range(3):
            take_plane(halo_ref, base + k, low + k)

    def face_z(k, carry):
        cache = {}

        def get(r, cell):
            if (r, cell) not in cache:
                cache[(r, cell)] = ez[r, k + cell]
            return cache[(r, cell)]

        flux = face_flux(get)
        for m in range(5):
            fz[m, k] = flux[m]
        return carry

    for out, flow, metric in raw_rows(2):
        for k in range(4):
            ez[out, 3 + k] = qv[flow, k] if flow is not None else sv[6 + metric, k]
    fill_z(3, 7)

    def low_z():
        take_z(zl, 0, 1)
        fill_z(0, 3)

    def high_z():
        take_z(zh, 7, 0)
        fill_z(7, 10)

    arrive(2, ((14, 4, relay), (16, 3, not_(jnp.logical_or(relay, edge))), (8, 3, edge)))

    @pl.when(not_(edge_low))
    def _():
        low_z()

    @pl.when(not_(edge_high))
    def _():
        high_z()

    early_first = jnp.where(edge_low, 3, 0)
    early_last = jnp.where(edge_low, 5, jnp.where(edge_high, 2, 5))
    lax.fori_loop(early_first, early_last, face_z, 0)

    @pl.when(lone)
    def _():
        pl.semaphore_wait(word, 1)
        send_far()

    extra = both(edge, both(not_(late), not_(lone)))
    for direction, fields, amount, there in (
        (0, 16, 4, not_(x_end)),
        (0, 8, 4, x_end),
        (1, 16, 4, not_(top)),
        (1, 8, 4, top),
        (2, 16, 3, not_(edge)),
        (2, 8, 4, extra),
        (2, 8, 3, both(edge, not_(extra))),
    ):
        @pl.when(there)
        def _():
            all_of(direction, fields, amount).wait_send()

    spanwise = order_of(2)

    def finish(k):
        for m in range(5):
            target = 1 + spanwise[m - 1] if 1 <= m <= 3 else m
            rate = -iv[k] * (acc[target, k] + (fz[m, k + 1] - fz[m, k]))
            rate_out[target, k] = rate
            state_out[target, k] = qv[target, k] + STEP_SIZE * rate

    @pl.when(not_(edge))
    def _():
        for k in range(4):
            finish(k)

    @pl.when(edge)
    def _():
        finish(jnp.where(edge_low, 3, 0))

        def body(stage, carry):
            @pl.when(edge_low)
            def _():
                far_arrive(ZL, stage)
                take_plane(zl, 2 - stage, 3 - stage)
                fill(ez, (2 - stage,))

            @pl.when(edge_high)
            def _():
                far_arrive(ZH, stage)
                take_plane(zh, 7 + stage, stage)
                fill(ez, (7 + stage,))

            carry = face_z(jnp.where(edge_low, 2 - stage, 2 + stage), carry)
            finish(jnp.where(edge_low, 2 - stage, 1 + stage))
            return carry

        lax.fori_loop(0, 3, body, 0)

    @pl.when(both(relay, y == 1))
    def _():
        pl.semaphore_wait(word, 1)

        @pl.when(turn == 3)
        def _():
            pl.delay(1000)

        @pl.when(turn == 5)
        def _():
            pl.delay(2000)

        for copy in far_copies(ZH, zl.at[pl.ds(0, 5)], zl.at[pl.ds(5, 3)], beyond):
            copy.start()

    @pl.when(both(relay, y == 6))
    def _():
        pl.semaphore_wait(word, 1)
        for copy in far_copies(ZL, zh.at[pl.ds(0, 5)], zh.at[pl.ds(5, 3)], beyond):
            copy.start()

    @pl.when(jnp.logical_or(relay, jnp.logical_or(far_late, lone)))
    def _():
        far_sent()


def deliver(state, rate, state_out, rate_out, sem):
    whole = [
        pltpu.make_async_copy(state, state_out, sem.at[0]),
        pltpu.make_async_copy(rate, rate_out, sem.at[1]),
    ]
    for m in range(state.shape[0]):
        pltpu.make_async_copy(state.at[m], state_out.at[m], sem.at[0]).start()
        pltpu.make_async_copy(rate.at[m], rate_out.at[m], sem.at[1]).start()
    for copy in whole:
        copy.wait()


def local(conserved, metrics, inv_volume, wake_donor):
    block = conserved.shape
    planes, rows, lanes = block[1:]
    wide = pltpu.VMEM(block, jnp.float32)
    f32 = lambda *shape: pltpu.VMEM(shape, jnp.float32)
    rate, state = pl.pallas_call(
        kernel,
        out_shape=(wide, wide),
        in_specs=[pl.BlockSpec(memory_space=pltpu.HBM)] * 4,
        out_specs=[pl.BlockSpec(memory_space=pltpu.VMEM)] * 2,
        scratch_shapes=[
            f32(*block),
            f32(9, planes, rows, lanes),
            f32(planes, rows, lanes),
            pltpu.VMEM((1, lanes), jnp.int32),
            *[f32(8, planes, rows, lanes)] * 4,
            *[f32(8, planes, rows, lanes)] * 2,
            f32(8, planes, rows, lanes),
            f32(CELL_ROWS, 5, rows, lanes),
            f32(CELL_ROWS, 5, rows, lanes),
            f32(CELL_ROWS, 64, lanes),
            f32(CELL_ROWS, 10, rows, lanes),
            f32(5, 5, rows, lanes),
            f32(5, 56, lanes),
            f32(5, 5, rows, lanes),
            f32(*block),
            pltpu.SemaphoreType.DMA((3,)),
            pltpu.SemaphoreType.DMA((3,)),
            pltpu.SemaphoreType.DMA((2,)),
            pltpu.SemaphoreType.DMA,
            pltpu.SemaphoreType.DMA((3,)),
            pltpu.SemaphoreType.REGULAR,
        ],
        compiler_params=pltpu.CompilerParams(collective_id=0, has_side_effects=True),
    )(conserved, metrics, inv_volume, wake_donor[None])
    return pl.pallas_call(
        deliver,
        out_shape=(jax.ShapeDtypeStruct(block, jnp.float32),) * 2,
        in_specs=[pl.BlockSpec(memory_space=pl.ANY)] * 2,
        out_specs=[pl.BlockSpec(memory_space=pltpu.HBM)] * 2,
        scratch_shapes=[pltpu.SemaphoreType.DMA((2,))],
    )(pltpu.with_memory_space_constraint(state, pltpu.VMEM), pltpu.with_memory_space_constraint(rate, pltpu.VMEM))


def solution(mesh):
    placed = (P(None, "gz", "gy", "gx"), P(None, "gz", "gy", "gx"), P("gz", "gy", "gx"), P("gx"))
    return jax.shard_map(
        local,
        mesh=mesh,
        in_specs=placed,
        out_specs=(P(None, "gz", "gy", "gx"), P(None, "gz", "gy", "gx")),
        check_vma=False,
    )
```

```python
import jax
import jax.numpy as jnp
from jax import lax
from jax.experimental import pallas as pl
from jax.experimental.pallas import tpu as pltpu
from jax.sharding import PartitionSpec as P

GAMMA = 1.4
WENO_EPS = 1e-06
STEP_SIZE = 0.08
MESH = pl.DeviceIdType.MESH

XL, XH, YL, YH, ZL, ZH, MIR, ZLX, ZHX = range(9)
FLUX, SPEED, VEL, PRES, ROW = 5, 10, 11, 14, 15
CELL_ROWS = 18


def order_of(direction):
    return [direction % 3, (direction + 1) % 3, (direction + 2) % 3]


def cell_terms(fields, row):
    inverse = 1.0 / fields[0]
    velocity = [fields[1 + member] * inverse for member in range(3)]
    kinetic = 0.5 * sum(fields[1 + member] * velocity[member] for member in range(3))
    pressure = (GAMMA - 1.0) * (fields[4] - kinetic)
    contra = sum(row[member] * velocity[member] for member in range(3))
    fluxes = [fields[0] * contra]
    fluxes += [fields[1 + member] * contra + row[member] * pressure for member in range(3)]
    fluxes += [(fields[4] + pressure) * contra]
    size = sum(row[member] * row[member] for member in range(3))
    speed = jnp.abs(contra) + jnp.sqrt(GAMMA * pressure * inverse * size)
    return fluxes, speed, velocity, pressure


def weno_shift(d1, d2, d3, d4):
    s0, s1, s2 = d2 - d1, d3 - d2, d4 - d3
    q2 = d2 * d2 + WENO_EPS
    q3 = d3 * d3 + WENO_EPS
    b0 = s0 * ((4.0 / 3.0) * s0 + d2) + q2
    b1 = s1 * ((4.0 / 3.0) * s1 + d2) + q2
    b2 = s2 * ((4.0 / 3.0) * s2 - d3) + q3
    p01, p02, p12 = b0 * b1, b0 * b2, b1 * b2
    w0 = p12 * p12
    w1 = 6.0 * (p02 * p02)
    w2 = 3.0 * (p01 * p01)
    g0 = 2.0 * s0 + 3.0 * d2
    g1 = d2 + 2.0 * d3
    g2 = 3.0 * d3 - s2
    return (w0 * g0 + w1 * g1 + w2 * g2) / (w0 + w1 + w2)


def face_flux(get):
    alpha = get(SPEED, 0)
    for cell in range(1, 6):
        alpha = jnp.maximum(alpha, get(SPEED, cell))
    rho = 0.5 * (get(0, 2) + get(0, 3))
    ua, ub, uc = [0.5 * (get(VEL + m, 2) + get(VEL + m, 3)) for m in range(3)]
    pressure = 0.5 * (get(PRES, 2) + get(PRES, 3))
    sa, sb, sc = [get(ROW + m, 2) + get(ROW + m, 3) for m in range(3)]
    flat = sa * sa + sc * sc
    inv_flat = lax.rsqrt(flat)
    inv_size = lax.rsqrt(flat + sb * sb)
    na, nb, nc = sa * inv_size, sb * inv_size, sc * inv_size
    la, lc = -sc * inv_flat, sa * inv_flat
    ma, mb, mc = nb * lc, nc * la - na * lc, -nb * la
    c2 = GAMMA * pressure / rho
    ic = lax.rsqrt(c2)
    c = c2 * ic
    f = (GAMMA - 1.0) * ic * ic
    kinetic = 0.5 * (ua * ua + ub * ub + uc * uc)
    q = na * ua + nb * ub + nc * uc
    a = la * ua + lc * uc
    b = ma * ua + mb * ub + mc * uc
    f4 = 0.25 * f
    g4 = f4 * kinetic
    fa, fb, fc = f4 * ua, f4 * ub, f4 * uc
    i4 = 0.25 * ic
    q4, ia, ib, jc = i4 * q, i4 * na, i4 * nb, i4 * nc
    la2, lc2, a2 = 0.5 * la, 0.5 * lc, 0.5 * a
    ma2, mb2, mc2, b2 = 0.5 * ma, 0.5 * mb, 0.5 * mc, 0.5 * b

    def left(v):
        s = g4 * v[0] - (fa * v[1] + fb * v[2] + fc * v[3]) + f4 * v[4]
        t = q4 * v[0] - (ia * v[1] + ib * v[2] + jc * v[3])
        return [
            s + t,
            0.5 * v[0] - 2.0 * s,
            la2 * v[1] + lc2 * v[3] - a2 * v[0],
            ma2 * v[1] + mb2 * v[2] + mc2 * v[3] - b2 * v[0],
            s - t,
        ]

    up, down, middle = [], [], None
    for step in range(5):
        dq = [get(m, step + 1) - get(m, step) for m in range(5)]
        dg = [get(FLUX + m, step + 1) - get(FLUX + m, step) for m in range(5)]
        aq = [alpha * dq[m] for m in range(5)]
        if step < 4:
            up.append(left([dg[m] + aq[m] for m in range(5)]))
        if step > 0:
            down.append(left([dg[m] - aq[m] for m in range(5)]))
        if step == 2:
            middle = [0.5 * (get(FLUX + m, 2) + get(FLUX + m, 3) - aq[m]) for m in range(5)]
    chars = []
    for m in range(5):
        plus = weno_shift(up[0][m], up[1][m], up[2][m], up[3][m])
        minus = weno_shift(down[3][m], down[2][m], down[1][m], down[0][m])
        chars.append((1.0 / 6.0) * (plus - minus))
    ends = chars[0] + chars[4]
    total = ends + chars[1]
    along = c * (chars[4] - chars[0])
    energy = kinetic * total + (1.0 / (GAMMA - 1.0)) * c2 * ends + q * along + a * chars[2] + b * chars[3]
    return [
        middle[0] + total,
        middle[1] + (ua * total + na * along + la * chars[2] + ma * chars[3]),
        middle[2] + (ub * total + nb * along + mb * chars[3]),
        middle[3] + (uc * total + nc * along + lc * chars[2] + mc * chars[3]),
        middle[4] + energy,
    ]


def reversed_lanes(value):
    lane = lax.broadcasted_iota(jnp.int32, value.shape, 1)
    for bit in range(7):
        step = 1 << bit
        value = jnp.where((lane & step) == 0, pltpu.roll(value, 128 - step, 1), pltpu.roll(value, step, 1))
    return value


def kernel(
    q_hbm, s_hbm, inv_hbm, wake_hbm, rate_out, state_out,
    qv, sv, iv, wv, xl, xh, yl, yh, zl, zh, mir, held, ex, exh, ey, ez, fx, fy, fz, acc,
    send_sem, recv_sem, own_sem, far_send, far_recv, word,
):
    gx, gy, gz = lax.axis_index("gx"), lax.axis_index("gy"), lax.axis_index("gz")
    y = lax.rem(gz, 8)
    late = gz >= 8
    edge_low, edge_high = y == 0, y == 7
    edge = jnp.logical_or(edge_low, edge_high)
    far_late = jnp.logical_and(late, edge)
    far_early = jnp.logical_and(jnp.logical_not(late), edge)
    beside = jnp.logical_or(y == 1, y == 6)
    beside_far = jnp.logical_and(late, beside)
    corner = jnp.logical_and(gx == 0, gy == 0)
    lone, lone_far = jnp.logical_and(corner, gz == 0), jnp.logical_and(corner, gz == 15)
    by_x, by_y, by_z, by_mirror = [
        jnp.logical_and(jnp.logical_and(gx == i, gy == j), gz == k) for i, j, k in ((1, 0, 0), (0, 1, 0), (0, 0, 1), (3, 0, 0))
    ]
    adjacent = jnp.logical_or(jnp.logical_or(by_x, by_y), jnp.logical_or(by_z, by_mirror))
    relay = jnp.logical_and(jnp.logical_and(gz < 8, beside), jnp.logical_not(jnp.logical_and(corner, gz == 1)))
    wall, top = gy == 0, gy == 11
    inflow, outflow = gx == 0, gx == 3
    not_ = jnp.logical_not
    both = jnp.logical_and

    up_z = (gx, gy, lax.rem(gz + 1, 16))
    down_z = (gx, gy, lax.rem(gz + 15, 16))
    partner = (gx, gy, jnp.where(edge_low, down_z[2], up_z[2]))
    inner = (gx, gy, jnp.where(edge_low, up_z[2], down_z[2]))
    beyond = (gx, gy, jnp.where(jnp.logical_or(edge_low, y == 1), lax.rem(gz + 14, 16), lax.rem(gz + 2, 16)))
    outer = (gx, gy, jnp.where(y == 1, down_z[2], up_z[2]))
    row = [
        (not_(inflow), (gx - 1, gy, gz)),
        (not_(outflow), (gx + 1, gy, gz)),
        (not_(wall), (gx, gy - 1, gz)),
        (not_(top), (gx, gy + 1, gz)),
        (both(wall, jnp.logical_or(inflow, outflow)), (3 - gx, gy, gz)),
    ]
    spans = [(not_(edge_high), up_z, y + 1), (not_(edge_low), down_z, y - 1)]
    barrier = pltpu.get_barrier_semaphore()

    def signal(semaphore, target):
        pl.semaphore_signal(semaphore, inc=1, device_id=target, device_id_type=MESH)

    buffers = (xl, xh, yl, yh, zl, zh, mir, zl, zh)

    direction_of = {XL: 0, XH: 0, YL: 1, YH: 1, MIR: 1, ZL: 2, ZH: 2, ZLX: 2, ZHX: 2}

    def copies(slot):
        target = {
            XL: (gx + 1, gy, gz),
            XH: (gx - 1, gy, gz),
            YL: (gx, gy + 1, gz),
            YH: (gx, gy - 1, gz),
            ZL: up_z,
            ZH: down_z,
            MIR: (3 - gx, gy, gz),
            ZLX: up_z,
            ZHX: down_z,
        }[slot]
        direction = direction_of[slot]
        low, amount = {ZL: (1, 3), ZH: (0, 3), ZLX: (0, 1), ZHX: (3, 1)}.get(slot, (0, 4))
        pieces = [
            (q_hbm.at[:, pl.ds(low, amount)], buffers[slot].at[pl.ds(0, 5), pl.ds(low, amount)]),
            (s_hbm.at[pl.ds(3 * direction, 3), pl.ds(low, amount)], buffers[slot].at[pl.ds(5, 3), pl.ds(low, amount)]),
        ]
        return [
            pltpu.make_async_remote_copy(
                src_ref=source,
                dst_ref=landing,
                send_sem=send_sem.at[direction_of[slot]],
                recv_sem=recv_sem.at[direction_of[slot]],
                device_id=target,
                device_id_type=MESH,
            )
            for source, landing in pieces
        ]

    def far_copies(slot, flow, metric, target, into=None, stages=(0, 1, 2)):
        listed = []
        into = buffers[slot] if into is None else into
        for stage in stages:
            plane = {ZL: 3 - stage, ZH: stage}[slot]
            for source, landing in (
                (flow.at[:, plane], into.at[pl.ds(0, 5), plane]),
                (metric.at[:, plane], into.at[pl.ds(5, 3), plane]),
            ):
                listed.append(
                    pltpu.make_async_remote_copy(
                        src_ref=source,
                        dst_ref=landing,
                        send_sem=far_send,
                        recv_sem=far_recv.at[stage],
                        device_id=target,
                        device_id_type=MESH,
                    )
                )
        return listed

    def far_arrive(slot, stage):
        plane = 3 - stage if slot == ZL else stage
        pltpu.make_async_remote_copy(
            src_ref=buffers[slot].at[:, plane],
            dst_ref=buffers[slot].at[:, plane],
            send_sem=far_send,
            recv_sem=far_recv.at[stage],
            device_id=partner,
            device_id_type=MESH,
        ).wait_recv()

    def far_sent():
        pltpu.make_async_remote_copy(
            src_ref=zl.at[:, pl.ds(0, 3)],
            dst_ref=zl.at[:, pl.ds(0, 3)],
            send_sem=far_send,
            recv_sem=far_recv.at[0],
            device_id=partner,
            device_id_type=MESH,
        ).wait_send()

    turn = gy // 2
    detour_from = both(both(late, edge_high), gy == 9)
    detour_at = both(both(late, y == 6), gy == 9)
    detour_to = both(both(not_(late), edge_low), gy == 9)

    def send_far():
        flow, metric = q_hbm, s_hbm.at[pl.ds(6, 3)]

        @pl.when(both(edge_high, not_(detour_from)))
        def _():
            for copy in far_copies(ZL, flow, metric, partner):
                copy.start()

        @pl.when(detour_from)
        def _():
            for copy in far_copies(ZL, flow, metric, inner, held):
                copy.start()

        @pl.when(edge_low)
        def _():
            for copy in far_copies(ZH, flow, metric, partner):
                copy.start()

    @pl.when(far_late)
    def _():
        pl.semaphore_wait(barrier, jnp.where(lone_far, 1, 2))

    @pl.when(far_late)
    def _():
        signal(word, (gx, gy, jnp.where(lone_far, partner[2], beyond[2])))

    @pl.when(both(far_late, both(edge_high, turn == 3)))
    def _():
        pl.delay(1000)

    @pl.when(both(far_late, both(edge_high, turn == 5)))
    def _():
        pl.delay(2000)

    @pl.when(far_late)
    def _():
        send_far()

    @pl.when(far_early)
    def _():
        signal(barrier, (gx, gy, jnp.where(detour_to, lax.rem(gz + 14, 16), partner[2])))

    @pl.when(detour_at)
    def _():
        signal(barrier, outer)

    @pl.when(relay)
    def _():
        signal(barrier, beyond)

    @pl.when(far_late)
    def _():
        signal(barrier, inner)

    @pl.when(not_(jnp.logical_or(far_late, lone)))
    def _():
        for there, target in row:
            @pl.when(there)
            def _():
                signal(barrier, target)
        for there, target, row_of in spans:
            target_far_late = both(late, jnp.logical_or(row_of == 0, row_of == 7))

            @pl.when(both(there, not_(target_far_late)))
            def _():
                signal(barrier, target)

    near_row = sum(there.astype(jnp.int32) for there, _ in row)
    near_span = sum(there.astype(jnp.int32) for there, _, _ in spans)

    @pl.when(not_(far_late))
    def _():
        pl.semaphore_wait(barrier, near_row + near_span - adjacent.astype(jnp.int32) + detour_at.astype(jnp.int32))


    own = [
        pltpu.make_async_copy(q_hbm, qv, own_sem.at[0]),
        pltpu.make_async_copy(s_hbm, sv, own_sem.at[0]),
        pltpu.make_async_copy(inv_hbm, iv, own_sem.at[0]),
        pltpu.make_async_copy(wake_hbm, wv, own_sem.at[1]),
    ]
    for copy in own:
        copy.start()

    @pl.when(far_late)
    def _():
        pl.semaphore_wait(word, 1)

    sends = [
        (XL, not_(outflow)),
        (XH, not_(inflow)),
        (YL, not_(top)),
        (YH, not_(wall)),
        (MIR, wall),
        (ZL, not_(edge_high)),
        (ZH, not_(edge_low)),
        (ZLX, both(both(edge_low, not_(late)), not_(lone))),
        (ZHX, both(edge_high, not_(late))),
    ]
    to_lone = {XH: by_x, YH: by_y, ZH: by_z, MIR: by_mirror}
    for slot, there in sends:
        @pl.when(both(there, not_(to_lone[slot])) if slot in to_lone else there)
        def _():
            for copy in copies(slot):
                copy.start()

    @pl.when(lone)
    def _():
        for target in ((1, 0, 0), (0, 1, 0), (0, 0, 1), (3, 0, 0)):
            signal(word, target)

    @pl.when(beside_far)
    def _():
        for there, target in row:
            @pl.when(there)
            def _():
                signal(word, target)

    @pl.when(detour_at)
    def _():
        for stage in range(3):
            landed = held.at[:, 3 - stage]
            pltpu.make_async_remote_copy(
                src_ref=landed,
                dst_ref=landed,
                send_sem=far_send,
                recv_sem=far_recv.at[stage],
                device_id=beyond,
                device_id_type=MESH,
            ).wait_recv()
            for copy in far_copies(ZL, held.at[pl.ds(0, 5)], held.at[pl.ds(5, 3)], beyond, None, (stage,)):
                copy.start()

    @pl.when(beside_far)
    def _():
        pl.semaphore_wait(word, near_row)
        signal(word, outer)

    pltpu.make_async_copy(ex.at[pl.ds(0, 15), pl.ds(0, 4)], exh.at[pl.ds(0, 15), pl.ds(0, 4)], own_sem.at[0]).wait()
    own[3].wait()

    def all_of(direction, fields, amount):
        ref = ex.at[pl.ds(0, fields), pl.ds(0, amount)]
        return pltpu.make_async_remote_copy(
            src_ref=ref,
            dst_ref=ref,
            send_sem=send_sem.at[direction],
            recv_sem=recv_sem.at[direction],
            device_id=up_z,
            device_id_type=MESH,
        )

    def arrive(direction, counts):
        for fields, amount, there in counts:
            @pl.when(there)
            def _():
                all_of(direction, fields, amount).wait_recv()

    lane = lax.broadcasted_iota(jnp.int32, (8, 128), 1)

    def fill(array, index):
        fields = [array[(m,) + index] for m in range(5)]
        metric = [array[(ROW + m,) + index] for m in range(3)]
        fluxes, speed, velocity, pressure = cell_terms(fields, metric)
        for m in range(5):
            array[(FLUX + m,) + index] = fluxes[m]
        array[(SPEED,) + index] = speed
        for m in range(3):
            array[(VEL + m,) + index] = velocity[m]
        array[(PRES,) + index] = pressure

    def raw_rows(direction):
        cyclic = order_of(direction)
        listed = [(0, 0, None), (4, 4, None)]
        for m in range(3):
            listed.append((1 + m, 1 + cyclic[m], None))
            listed.append((ROW + m, None, cyclic[m]))
        return listed

    @pl.when(adjacent)
    def _():
        pl.semaphore_wait(word, 1)
        for slot, there in to_lone.items():
            @pl.when(there)
            def _():
                for copy in copies(slot):
                    copy.start()

    x_end = jnp.logical_or(inflow, outflow)
    arrive(0, ((16, 4, not_(x_end)), (8, 4, x_end)))

    @pl.when(inflow)
    def _():
        for k in range(4):
            for f in range(5):
                xl[f, k] = jnp.broadcast_to(qv[f, k, :, 0:1], (8, 128))
            for f in range(3):
                xl[5 + f, k] = jnp.broadcast_to(sv[f, k, :, 0:1], (8, 128))

    @pl.when(outflow)
    def _():
        for k in range(4):
            for f in range(5):
                xh[f, k] = jnp.broadcast_to(qv[f, k, :, 127:128], (8, 128))
            for f in range(3):
                xh[5 + f, k] = jnp.broadcast_to(sv[f, k, :, 127:128], (8, 128))

    for out, flow, metric in raw_rows(0):
        halo = flow if flow is not None else 5 + metric
        packed = None
        for k in range(4):
            centre = qv[flow, k] if flow is not None else sv[metric, k]
            ring = jnp.where(lane < 64, xh[halo, k], xl[halo, k])
            ex[out, k] = centre
            exh[out, k] = ring
            moved = pltpu.roll(jnp.where(lane < 64, ring, centre), (32 * k + 3) % 128, 1)
            packed = moved if packed is None else jnp.where(lane < 32 * k, packed, moved)
        ex[out, 4] = packed
        exh[out, 4] = packed

    def fill_x(k, carry):
        fill(ex, (k,))
        fill(exh, (k,))
        return carry

    lax.fori_loop(0, 5, fill_x, 0)

    def face_x(k, carry):
        cache = {}

        def get(r, cell):
            if (r, cell) not in cache:
                shift = 3 - cell
                centre = ex[r, k]
                if shift > 0:
                    centre = pltpu.roll(jnp.where(lane >= 128 - shift, exh[r, k], centre), shift, 1)
                elif shift < 0:
                    centre = pltpu.roll(jnp.where(lane < -shift, exh[r, k], centre), 128 + shift, 1)
                cache[(r, cell)] = centre
            return cache[(r, cell)]

        flux = face_flux(get)
        for m in range(5):
            fx[m, k] = flux[m]
        return carry

    lax.fori_loop(0, 5, face_x, 0)
    for k in range(4):
        for m in range(5):
            upper = pltpu.roll(fx[m, k], 127, 1)
            last = pltpu.roll(fx[m, 4], (124 - 32 * k) % 128, 1)
            acc[m, k] = jnp.where(lane == 127, last, upper) - fx[m, k]

    arrive(1, ((16, 4, not_(top)), (8, 4, top)))

    @pl.when(wall)
    def _():
        is_wake = jnp.broadcast_to(wv[0:1, :], (8, 128)) >= 0
        for f in range(8):
            for k in range(4):
                mirrored = reversed_lanes(mir[f, k])
                beside = qv[f, k] if f < 5 else sv[f - 2, k]
                if f in (1, 2, 3):
                    beside = -beside
                ghost = jnp.where(is_wake, mirrored, beside)
                for g in range(3):
                    yl[f, k, 7 - g : 8 - g, :] = ghost[g : g + 1, :]

    @pl.when(top)
    def _():
        for f in range(8):
            for k in range(4):
                source = qv[f, k, 7:8, :] if f < 5 else sv[f - 2, k, 7:8, :]
                yh[f, k] = jnp.broadcast_to(source, (8, 128))

    for out, flow, metric in raw_rows(1):
        halo = flow if flow is not None else 5 + metric
        for k in range(4):
            base = 14 * k
            ey[out, base : base + 3, :] = yl[halo, k, 5:8, :]
            ey[out, base + 3 : base + 11, :] = qv[flow, k] if flow is not None else sv[3 + metric, k]
            ey[out, base + 11 : base + 14, :] = yh[halo, k, 0:3, :]
        ey[out, 56:64, :] = qv[flow, 3] if flow is not None else sv[3 + metric, 3]

    def fill_y(k, carry):
        fill(ey, (pl.ds(pl.multiple_of(8 * k, 8), 8),))
        return carry

    lax.fori_loop(0, 8, fill_y, 0)

    def face_y(k, carry):
        cache = {}

        def get(r, cell):
            if (r, cell) not in cache:
                cache[(r, cell)] = ey[r, pl.ds(8 * k + cell, 8), :]
            return cache[(r, cell)]

        flux = face_flux(get)
        for m in range(5):
            fy[m, pl.ds(pl.multiple_of(8 * k, 8), 8), :] = flux[m]
        return carry

    lax.fori_loop(0, 7, face_y, 0)
    cyclic = order_of(1)
    for k in range(4):
        for m in range(5):
            target = 1 + cyclic[m - 1] if 1 <= m <= 3 else m
            acc[target, k] += fy[m, 14 * k + 1 : 14 * k + 9, :] - fy[m, 14 * k : 14 * k + 8, :]

    def fill_z(first, last):
        def body(k, carry):
            fill(ez, (k,))
            return carry

        lax.fori_loop(first, last, body, 0)

    def take_plane(halo_ref, cell, plane):
        for out, flow, metric in raw_rows(2):
            halo = flow if flow is not None else 5 + metric
            ez[out, cell] = halo_ref[halo, plane]

    def take_z(halo_ref, base, low):
        for k in range(3):
            take_plane(halo_ref, base + k, low + k)

    def face_z(k, carry):
        cache = {}

        def get(r, cell):
            if (r, cell) not in cache:
                cache[(r, cell)] = ez[r, k + cell]
            return cache[(r, cell)]

        flux = face_flux(get)
        for m in range(5):
            fz[m, k] = flux[m]
        return carry

    for out, flow, metric in raw_rows(2):
        for k in range(4):
            ez[out, 3 + k] = qv[flow, k] if flow is not None else sv[6 + metric, k]
    fill_z(3, 7)

    def low_z():
        take_z(zl, 0, 1)
        fill_z(0, 3)

    def high_z():
        take_z(zh, 7, 0)
        fill_z(7, 10)

    arrive(2, ((14, 4, relay), (16, 3, not_(jnp.logical_or(relay, edge))), (8, 3, edge)))

    @pl.when(not_(edge_low))
    def _():
        low_z()

    @pl.when(not_(edge_high))
    def _():
        high_z()

    early_first = jnp.where(edge_low, 3, 0)
    early_last = jnp.where(edge_low, 5, jnp.where(edge_high, 2, 5))
    lax.fori_loop(early_first, early_last, face_z, 0)

    @pl.when(lone)
    def _():
        pl.semaphore_wait(word, 1)
        send_far()

    extra = both(edge, both(not_(late), not_(lone)))
    for direction, fields, amount, there in (
        (0, 16, 4, not_(x_end)),
        (0, 8, 4, x_end),
        (1, 16, 4, not_(top)),
        (1, 8, 4, top),
        (2, 16, 3, not_(edge)),
        (2, 8, 4, extra),
        (2, 8, 3, both(edge, not_(extra))),
    ):
        @pl.when(there)
        def _():
            all_of(direction, fields, amount).wait_send()

    spanwise = order_of(2)

    def finish(k):
        for m in range(5):
            target = 1 + spanwise[m - 1] if 1 <= m <= 3 else m
            rate = -iv[k] * (acc[target, k] + (fz[m, k + 1] - fz[m, k]))
            rate_out[target, k] = rate
            state_out[target, k] = qv[target, k] + STEP_SIZE * rate

    @pl.when(not_(edge))
    def _():
        for k in range(4):
            finish(k)

    @pl.when(edge)
    def _():
        finish(jnp.where(edge_low, 3, 0))

        def body(stage, carry):
            @pl.when(edge_low)
            def _():
                far_arrive(ZL, stage)
                take_plane(zl, 2 - stage, 3 - stage)
                fill(ez, (2 - stage,))

            @pl.when(edge_high)
            def _():
                far_arrive(ZH, stage)
                take_plane(zh, 7 + stage, stage)
                fill(ez, (7 + stage,))

            carry = face_z(jnp.where(edge_low, 2 - stage, 2 + stage), carry)
            finish(jnp.where(edge_low, 2 - stage, 1 + stage))
            return carry

        lax.fori_loop(0, 3, body, 0)

    @pl.when(both(relay, y == 1))
    def _():
        pl.semaphore_wait(word, 1)

        @pl.when(turn == 3)
        def _():
            pl.delay(1000)

        @pl.when(turn == 5)
        def _():
            pl.delay(2000)

        for copy in far_copies(ZH, zl.at[pl.ds(0, 5)], zl.at[pl.ds(5, 3)], beyond):
            copy.start()

    @pl.when(both(relay, y == 6))
    def _():
        pl.semaphore_wait(word, 1)
        for copy in far_copies(ZL, zh.at[pl.ds(0, 5)], zh.at[pl.ds(5, 3)], beyond):
            copy.start()

    @pl.when(jnp.logical_or(jnp.logical_or(relay, detour_at), jnp.logical_or(far_late, lone)))
    def _():
        far_sent()


def deliver(state, rate, state_out, rate_out, sem):
    whole = [
        pltpu.make_async_copy(state, state_out, sem.at[0]),
        pltpu.make_async_copy(rate, rate_out, sem.at[1]),
    ]
    for m in range(state.shape[0]):
        pltpu.make_async_copy(state.at[m], state_out.at[m], sem.at[0]).start()
        pltpu.make_async_copy(rate.at[m], rate_out.at[m], sem.at[1]).start()
    for copy in whole:
        copy.wait()


def local(conserved, metrics, inv_volume, wake_donor):
    block = conserved.shape
    planes, rows, lanes = block[1:]
    wide = pltpu.VMEM(block, jnp.float32)
    f32 = lambda *shape: pltpu.VMEM(shape, jnp.float32)
    rate, state = pl.pallas_call(
        kernel,
        out_shape=(wide, wide),
        in_specs=[pl.BlockSpec(memory_space=pltpu.HBM)] * 4,
        out_specs=[pl.BlockSpec(memory_space=pltpu.VMEM)] * 2,
        scratch_shapes=[
            f32(*block),
            f32(9, planes, rows, lanes),
            f32(planes, rows, lanes),
            pltpu.VMEM((1, lanes), jnp.int32),
            *[f32(8, planes, rows, lanes)] * 4,
            *[f32(8, planes, rows, lanes)] * 2,
            *[f32(8, planes, rows, lanes)] * 2,
            f32(CELL_ROWS, 5, rows, lanes),
            f32(CELL_ROWS, 5, rows, lanes),
            f32(CELL_ROWS, 64, lanes),
            f32(CELL_ROWS, 10, rows, lanes),
            f32(5, 5, rows, lanes),
            f32(5, 56, lanes),
            f32(5, 5, rows, lanes),
            f32(*block),
            pltpu.SemaphoreType.DMA((3,)),
            pltpu.SemaphoreType.DMA((3,)),
            pltpu.SemaphoreType.DMA((2,)),
            pltpu.SemaphoreType.DMA,
            pltpu.SemaphoreType.DMA((3,)),
            pltpu.SemaphoreType.REGULAR,
        ],
        compiler_params=pltpu.CompilerParams(collective_id=0, has_side_effects=True),
    )(conserved, metrics, inv_volume, wake_donor[None])
    return pl.pallas_call(
        deliver,
        out_shape=(jax.ShapeDtypeStruct(block, jnp.float32),) * 2,
        in_specs=[pl.BlockSpec(memory_space=pl.ANY)] * 2,
        out_specs=[pl.BlockSpec(memory_space=pltpu.HBM)] * 2,
        scratch_shapes=[pltpu.SemaphoreType.DMA((2,))],
    )(pltpu.with_memory_space_constraint(state, pltpu.VMEM), pltpu.with_memory_space_constraint(rate, pltpu.VMEM))


def solution(mesh):
    placed = (P(None, "gz", "gy", "gx"), P(None, "gz", "gy", "gx"), P("gz", "gy", "gx"), P("gx"))
    return jax.shard_map(
        local,
        mesh=mesh,
        in_specs=placed,
        out_specs=(P(None, "gz", "gy", "gx"), P(None, "gz", "gy", "gx")),
        check_vma=False,
    )
```

```python
import jax
import jax.numpy as jnp
from jax import lax
from jax.experimental import pallas as pl
from jax.experimental.pallas import tpu as pltpu
from jax.sharding import PartitionSpec as P

GAMMA = 1.4
WENO_EPS = 1e-06
STEP_SIZE = 0.08
MESH = pl.DeviceIdType.MESH

XL, XH, YL, YH, ZL, ZH, MIR, ZLX, ZHX = range(9)
FLUX, SPEED, VEL, PRES, ROW = 5, 10, 11, 14, 15
CELL_ROWS = 18


def order_of(direction):
    return [direction % 3, (direction + 1) % 3, (direction + 2) % 3]


def cell_terms(fields, row):
    inverse = 1.0 / fields[0]
    velocity = [fields[1 + member] * inverse for member in range(3)]
    kinetic = 0.5 * sum(fields[1 + member] * velocity[member] for member in range(3))
    pressure = (GAMMA - 1.0) * (fields[4] - kinetic)
    contra = sum(row[member] * velocity[member] for member in range(3))
    fluxes = [fields[0] * contra]
    fluxes += [fields[1 + member] * contra + row[member] * pressure for member in range(3)]
    fluxes += [(fields[4] + pressure) * contra]
    size = sum(row[member] * row[member] for member in range(3))
    speed = jnp.abs(contra) + jnp.sqrt(GAMMA * pressure * inverse * size)
    return fluxes, speed, velocity, pressure


def weno_shift(d1, d2, d3, d4):
    s0, s1, s2 = d2 - d1, d3 - d2, d4 - d3
    q2 = d2 * d2 + WENO_EPS
    q3 = d3 * d3 + WENO_EPS
    b0 = s0 * ((4.0 / 3.0) * s0 + d2) + q2
    b1 = s1 * ((4.0 / 3.0) * s1 + d2) + q2
    b2 = s2 * ((4.0 / 3.0) * s2 - d3) + q3
    p01, p02, p12 = b0 * b1, b0 * b2, b1 * b2
    w0 = p12 * p12
    w1 = 6.0 * (p02 * p02)
    w2 = 3.0 * (p01 * p01)
    g0 = 2.0 * s0 + 3.0 * d2
    g1 = d2 + 2.0 * d3
    g2 = 3.0 * d3 - s2
    return (w0 * g0 + w1 * g1 + w2 * g2) / (w0 + w1 + w2)


def face_flux(get):
    alpha = get(SPEED, 0)
    for cell in range(1, 6):
        alpha = jnp.maximum(alpha, get(SPEED, cell))
    rho = 0.5 * (get(0, 2) + get(0, 3))
    ua, ub, uc = [0.5 * (get(VEL + m, 2) + get(VEL + m, 3)) for m in range(3)]
    pressure = 0.5 * (get(PRES, 2) + get(PRES, 3))
    sa, sb, sc = [get(ROW + m, 2) + get(ROW + m, 3) for m in range(3)]
    flat = sa * sa + sc * sc
    inv_flat = lax.rsqrt(flat)
    inv_size = lax.rsqrt(flat + sb * sb)
    na, nb, nc = sa * inv_size, sb * inv_size, sc * inv_size
    la, lc = -sc * inv_flat, sa * inv_flat
    ma, mb, mc = nb * lc, nc * la - na * lc, -nb * la
    c2 = GAMMA * pressure / rho
    ic = lax.rsqrt(c2)
    c = c2 * ic
    f = (GAMMA - 1.0) * ic * ic
    kinetic = 0.5 * (ua * ua + ub * ub + uc * uc)
    q = na * ua + nb * ub + nc * uc
    a = la * ua + lc * uc
    b = ma * ua + mb * ub + mc * uc
    f4 = 0.25 * f
    g4 = f4 * kinetic
    fa, fb, fc = f4 * ua, f4 * ub, f4 * uc
    i4 = 0.25 * ic
    q4, ia, ib, jc = i4 * q, i4 * na, i4 * nb, i4 * nc
    la2, lc2, a2 = 0.5 * la, 0.5 * lc, 0.5 * a
    ma2, mb2, mc2, b2 = 0.5 * ma, 0.5 * mb, 0.5 * mc, 0.5 * b

    def left(v):
        s = g4 * v[0] - (fa * v[1] + fb * v[2] + fc * v[3]) + f4 * v[4]
        t = q4 * v[0] - (ia * v[1] + ib * v[2] + jc * v[3])
        return [
            s + t,
            0.5 * v[0] - 2.0 * s,
            la2 * v[1] + lc2 * v[3] - a2 * v[0],
            ma2 * v[1] + mb2 * v[2] + mc2 * v[3] - b2 * v[0],
            s - t,
        ]

    up, down, middle = [], [], None
    for step in range(5):
        dq = [get(m, step + 1) - get(m, step) for m in range(5)]
        dg = [get(FLUX + m, step + 1) - get(FLUX + m, step) for m in range(5)]
        aq = [alpha * dq[m] for m in range(5)]
        if step < 4:
            up.append(left([dg[m] + aq[m] for m in range(5)]))
        if step > 0:
            down.append(left([dg[m] - aq[m] for m in range(5)]))
        if step == 2:
            middle = [0.5 * (get(FLUX + m, 2) + get(FLUX + m, 3) - aq[m]) for m in range(5)]
    chars = []
    for m in range(5):
        plus = weno_shift(up[0][m], up[1][m], up[2][m], up[3][m])
        minus = weno_shift(down[3][m], down[2][m], down[1][m], down[0][m])
        chars.append((1.0 / 6.0) * (plus - minus))
    ends = chars[0] + chars[4]
    total = ends + chars[1]
    along = c * (chars[4] - chars[0])
    energy = kinetic * total + (1.0 / (GAMMA - 1.0)) * c2 * ends + q * along + a * chars[2] + b * chars[3]
    return [
        middle[0] + total,
        middle[1] + (ua * total + na * along + la * chars[2] + ma * chars[3]),
        middle[2] + (ub * total + nb * along + mb * chars[3]),
        middle[3] + (uc * total + nc * along + lc * chars[2] + mc * chars[3]),
        middle[4] + energy,
    ]


def reversed_lanes(value):
    lane = lax.broadcasted_iota(jnp.int32, value.shape, 1)
    for bit in range(7):
        step = 1 << bit
        value = jnp.where((lane & step) == 0, pltpu.roll(value, 128 - step, 1), pltpu.roll(value, step, 1))
    return value


def kernel(
    q_hbm, s_hbm, inv_hbm, wake_hbm, rate_out, state_out,
    qv, sv, iv, wv, xl, xh, yl, yh, zl, zh, mir, held, ex, exh, ey, ez, fx, fy, fz, acc,
    send_sem, recv_sem, own_sem, far_send, far_recv, word,
):
    gx, gy, gz = lax.axis_index("gx"), lax.axis_index("gy"), lax.axis_index("gz")
    y = lax.rem(gz, 8)
    late = gz >= 8
    edge_low, edge_high = y == 0, y == 7
    edge = jnp.logical_or(edge_low, edge_high)
    far_late = jnp.logical_and(late, edge)
    far_early = jnp.logical_and(jnp.logical_not(late), edge)
    beside = jnp.logical_or(y == 1, y == 6)
    beside_far = jnp.logical_and(late, beside)
    corner = jnp.logical_and(gx == 0, gy == 0)
    lone, lone_far = jnp.logical_and(corner, gz == 0), jnp.logical_and(corner, gz == 15)
    by_x, by_y, by_z, by_mirror = [
        jnp.logical_and(jnp.logical_and(gx == i, gy == j), gz == k) for i, j, k in ((1, 0, 0), (0, 1, 0), (0, 0, 1), (3, 0, 0))
    ]
    adjacent = jnp.logical_or(jnp.logical_or(by_x, by_y), jnp.logical_or(by_z, by_mirror))
    relay = jnp.logical_and(jnp.logical_and(gz < 8, beside), jnp.logical_not(jnp.logical_and(corner, gz == 1)))
    wall, top = gy == 0, gy == 11
    inflow, outflow = gx == 0, gx == 3
    not_ = jnp.logical_not
    both = jnp.logical_and

    up_z = (gx, gy, lax.rem(gz + 1, 16))
    down_z = (gx, gy, lax.rem(gz + 15, 16))
    partner = (gx, gy, jnp.where(edge_low, down_z[2], up_z[2]))
    inner = (gx, gy, jnp.where(edge_low, up_z[2], down_z[2]))
    beyond = (gx, gy, jnp.where(jnp.logical_or(edge_low, y == 1), lax.rem(gz + 14, 16), lax.rem(gz + 2, 16)))
    outer = (gx, gy, jnp.where(y == 1, down_z[2], up_z[2]))
    row = [
        (not_(inflow), (gx - 1, gy, gz)),
        (not_(outflow), (gx + 1, gy, gz)),
        (not_(wall), (gx, gy - 1, gz)),
        (not_(top), (gx, gy + 1, gz)),
        (both(wall, jnp.logical_or(inflow, outflow)), (3 - gx, gy, gz)),
    ]
    spans = [(not_(edge_high), up_z, y + 1), (not_(edge_low), down_z, y - 1)]
    barrier = pltpu.get_barrier_semaphore()

    def signal(semaphore, target):
        pl.semaphore_signal(semaphore, inc=1, device_id=target, device_id_type=MESH)

    buffers = (xl, xh, yl, yh, zl, zh, mir, zl, zh)

    direction_of = {XL: 0, XH: 0, YL: 1, YH: 1, MIR: 1, ZL: 2, ZH: 2, ZLX: 2, ZHX: 2}

    def copies(slot):
        target = {
            XL: (gx + 1, gy, gz),
            XH: (gx - 1, gy, gz),
            YL: (gx, gy + 1, gz),
            YH: (gx, gy - 1, gz),
            ZL: up_z,
            ZH: down_z,
            MIR: (3 - gx, gy, gz),
            ZLX: up_z,
            ZHX: down_z,
        }[slot]
        direction = direction_of[slot]
        low, amount = {ZL: (1, 3), ZH: (0, 3), ZLX: (0, 1), ZHX: (3, 1)}.get(slot, (0, 4))
        pieces = [
            (q_hbm.at[:, pl.ds(low, amount)], buffers[slot].at[pl.ds(0, 5), pl.ds(low, amount)]),
            (s_hbm.at[pl.ds(3 * direction, 3), pl.ds(low, amount)], buffers[slot].at[pl.ds(5, 3), pl.ds(low, amount)]),
        ]
        return [
            pltpu.make_async_remote_copy(
                src_ref=source,
                dst_ref=landing,
                send_sem=send_sem.at[direction_of[slot]],
                recv_sem=recv_sem.at[direction_of[slot]],
                device_id=target,
                device_id_type=MESH,
            )
            for source, landing in pieces
        ]

    def far_copies(slot, flow, metric, target, into=None, stages=(0, 1, 2)):
        listed = []
        into = buffers[slot] if into is None else into
        for stage in stages:
            plane = {ZL: 3 - stage, ZH: stage}[slot]
            for source, landing in (
                (flow.at[:, plane], into.at[pl.ds(0, 5), plane]),
                (metric.at[:, plane], into.at[pl.ds(5, 3), plane]),
            ):
                listed.append(
                    pltpu.make_async_remote_copy(
                        src_ref=source,
                        dst_ref=landing,
                        send_sem=far_send,
                        recv_sem=far_recv.at[stage],
                        device_id=target,
                        device_id_type=MESH,
                    )
                )
        return listed

    def far_arrive(slot, stage):
        plane = 3 - stage if slot == ZL else stage
        pltpu.make_async_remote_copy(
            src_ref=buffers[slot].at[:, plane],
            dst_ref=buffers[slot].at[:, plane],
            send_sem=far_send,
            recv_sem=far_recv.at[stage],
            device_id=partner,
            device_id_type=MESH,
        ).wait_recv()

    def far_sent():
        pltpu.make_async_remote_copy(
            src_ref=zl.at[:, pl.ds(0, 3)],
            dst_ref=zl.at[:, pl.ds(0, 3)],
            send_sem=far_send,
            recv_sem=far_recv.at[0],
            device_id=partner,
            device_id_type=MESH,
        ).wait_send()

    turn = gy // 2
    detour_from = both(both(late, edge_high), gy == 9)
    detour_at = both(both(late, y == 6), gy == 9)
    detour_to = both(both(not_(late), edge_low), gy == 9)

    def send_far():
        flow, metric = q_hbm, s_hbm.at[pl.ds(6, 3)]

        @pl.when(both(edge_high, not_(detour_from)))
        def _():
            for copy in far_copies(ZL, flow, metric, partner):
                copy.start()

        @pl.when(detour_from)
        def _():
            for copy in far_copies(ZL, flow, metric, inner, held):
                copy.start()

        @pl.when(edge_low)
        def _():
            for copy in far_copies(ZH, flow, metric, partner):
                copy.start()

    @pl.when(far_late)
    def _():
        pl.semaphore_wait(barrier, jnp.where(lone_far, 1, 2))

    @pl.when(far_late)
    def _():
        signal(word, (gx, gy, jnp.where(lone_far, partner[2], beyond[2])))

    @pl.when(both(far_late, both(edge_high, turn == 3)))
    def _():
        pl.delay(1000)

    @pl.when(both(far_late, both(edge_high, turn == 5)))
    def _():
        pl.delay(2000)

    @pl.when(far_late)
    def _():
        send_far()

    @pl.when(far_early)
    def _():
        signal(barrier, (gx, gy, jnp.where(detour_to, lax.rem(gz + 14, 16), partner[2])))

    @pl.when(detour_at)
    def _():
        signal(barrier, outer)

    @pl.when(relay)
    def _():
        signal(barrier, beyond)

    @pl.when(far_late)
    def _():
        signal(barrier, inner)

    @pl.when(not_(jnp.logical_or(far_late, lone)))
    def _():
        for there, target in row:
            @pl.when(there)
            def _():
                signal(barrier, target)
        for there, target, row_of in spans:
            target_far_late = both(late, jnp.logical_or(row_of == 0, row_of == 7))

            @pl.when(both(there, not_(target_far_late)))
            def _():
                signal(barrier, target)

    near_row = sum(there.astype(jnp.int32) for there, _ in row)
    near_span = sum(there.astype(jnp.int32) for there, _, _ in spans)

    @pl.when(not_(far_late))
    def _():
        pl.semaphore_wait(barrier, near_row + near_span - adjacent.astype(jnp.int32) + detour_at.astype(jnp.int32))


    own = [
        pltpu.make_async_copy(q_hbm, qv, own_sem.at[0]),
        pltpu.make_async_copy(s_hbm, sv, own_sem.at[0]),
        pltpu.make_async_copy(inv_hbm, iv, own_sem.at[0]),
        pltpu.make_async_copy(wake_hbm, wv, own_sem.at[1]),
    ]
    for copy in own:
        copy.start()

    @pl.when(far_late)
    def _():
        pl.semaphore_wait(word, 1)

    sends = [
        (XL, not_(outflow)),
        (XH, not_(inflow)),
        (YL, not_(top)),
        (YH, not_(wall)),
        (MIR, wall),
        (ZL, not_(edge_high)),
        (ZH, not_(edge_low)),
        (ZLX, both(both(edge_low, not_(late)), not_(lone))),
        (ZHX, both(edge_high, not_(late))),
    ]
    to_lone = {XH: by_x, YH: by_y, ZH: by_z, MIR: by_mirror}
    for slot, there in sends:
        @pl.when(both(there, not_(to_lone[slot])) if slot in to_lone else there)
        def _():
            for copy in copies(slot):
                copy.start()

    @pl.when(lone)
    def _():
        for target in ((1, 0, 0), (0, 1, 0), (0, 0, 1), (3, 0, 0)):
            signal(word, target)

    @pl.when(beside_far)
    def _():
        for there, target in row:
            @pl.when(there)
            def _():
                signal(word, target)

    @pl.when(detour_at)
    def _():
        for stage in range(3):
            landed = held.at[:, 3 - stage]
            pltpu.make_async_remote_copy(
                src_ref=landed,
                dst_ref=landed,
                send_sem=far_send,
                recv_sem=far_recv.at[stage],
                device_id=beyond,
                device_id_type=MESH,
            ).wait_recv()
            for copy in far_copies(ZL, held.at[pl.ds(0, 5)], held.at[pl.ds(5, 3)], beyond, None, (stage,)):
                copy.start()

    @pl.when(beside_far)
    def _():
        pl.semaphore_wait(word, near_row)
        signal(word, outer)

    pltpu.make_async_copy(ex.at[pl.ds(0, 15), pl.ds(0, 4)], exh.at[pl.ds(0, 15), pl.ds(0, 4)], own_sem.at[0]).wait()
    own[3].wait()

    def all_of(direction, fields, amount):
        ref = ex.at[pl.ds(0, fields), pl.ds(0, amount)]
        return pltpu.make_async_remote_copy(
            src_ref=ref,
            dst_ref=ref,
            send_sem=send_sem.at[direction],
            recv_sem=recv_sem.at[direction],
            device_id=up_z,
            device_id_type=MESH,
        )

    def arrive(direction, counts):
        for fields, amount, there in counts:
            @pl.when(there)
            def _():
                all_of(direction, fields, amount).wait_recv()

    lane = lax.broadcasted_iota(jnp.int32, (8, 128), 1)

    def fill(array, index):
        fields = [array[(m,) + index] for m in range(5)]
        metric = [array[(ROW + m,) + index] for m in range(3)]
        put_terms(array, index, fields, metric)

    def put_terms(array, index, fields, metric):
        fluxes, speed, velocity, pressure = cell_terms(fields, metric)
        for m in range(5):
            array[(FLUX + m,) + index] = fluxes[m]
        array[(SPEED,) + index] = speed
        for m in range(3):
            array[(VEL + m,) + index] = velocity[m]
        array[(PRES,) + index] = pressure

    def raw_rows(direction):
        cyclic = order_of(direction)
        listed = [(0, 0, None), (4, 4, None)]
        for m in range(3):
            listed.append((1 + m, 1 + cyclic[m], None))
            listed.append((ROW + m, None, cyclic[m]))
        return listed

    @pl.when(adjacent)
    def _():
        pl.semaphore_wait(word, 1)
        for slot, there in to_lone.items():
            @pl.when(there)
            def _():
                for copy in copies(slot):
                    copy.start()

    x_end = jnp.logical_or(inflow, outflow)
    arrive(0, ((16, 4, not_(x_end)), (8, 4, x_end)))

    @pl.when(inflow)
    def _():
        for k in range(4):
            for f in range(5):
                xl[f, k] = jnp.broadcast_to(qv[f, k, :, 0:1], (8, 128))
            for f in range(3):
                xl[5 + f, k] = jnp.broadcast_to(sv[f, k, :, 0:1], (8, 128))

    @pl.when(outflow)
    def _():
        for k in range(4):
            for f in range(5):
                xh[f, k] = jnp.broadcast_to(qv[f, k, :, 127:128], (8, 128))
            for f in range(3):
                xh[5 + f, k] = jnp.broadcast_to(sv[f, k, :, 127:128], (8, 128))

    for out, flow, metric in raw_rows(0):
        halo = flow if flow is not None else 5 + metric
        packed = None
        for k in range(4):
            centre = qv[flow, k] if flow is not None else sv[metric, k]
            ring = jnp.where(lane < 64, xh[halo, k], xl[halo, k])
            ex[out, k] = centre
            exh[out, k] = ring
            moved = pltpu.roll(jnp.where(lane < 64, ring, centre), (32 * k + 3) % 128, 1)
            packed = moved if packed is None else jnp.where(lane < 32 * k, packed, moved)
        ex[out, 4] = packed
        exh[out, 4] = packed

    def fill_x(k, carry):
        fill(ex, (k,))
        fill(exh, (k,))
        return carry

    lax.fori_loop(0, 5, fill_x, 0)

    def face_x(k, carry):
        cache = {}

        def get(r, cell):
            if (r, cell) not in cache:
                shift = 3 - cell
                centre = ex[r, k]
                if shift > 0:
                    centre = pltpu.roll(jnp.where(lane >= 128 - shift, exh[r, k], centre), shift, 1)
                elif shift < 0:
                    centre = pltpu.roll(jnp.where(lane < -shift, exh[r, k], centre), 128 + shift, 1)
                cache[(r, cell)] = centre
            return cache[(r, cell)]

        flux = face_flux(get)
        for m in range(5):
            fx[m, k] = flux[m]
        return carry

    lax.fori_loop(0, 5, face_x, 0)
    for k in range(4):
        for m in range(5):
            upper = pltpu.roll(fx[m, k], 127, 1)
            last = pltpu.roll(fx[m, 4], (124 - 32 * k) % 128, 1)
            acc[m, k] = jnp.where(lane == 127, last, upper) - fx[m, k]

    arrive(1, ((16, 4, not_(top)), (8, 4, top)))

    @pl.when(wall)
    def _():
        is_wake = jnp.broadcast_to(wv[0:1, :], (8, 128)) >= 0
        for f in range(8):
            for k in range(4):
                mirrored = reversed_lanes(mir[f, k])
                beside = qv[f, k] if f < 5 else sv[f - 2, k]
                if f in (1, 2, 3):
                    beside = -beside
                ghost = jnp.where(is_wake, mirrored, beside)
                for g in range(3):
                    yl[f, k, 7 - g : 8 - g, :] = ghost[g : g + 1, :]

    @pl.when(top)
    def _():
        for f in range(8):
            for k in range(4):
                source = qv[f, k, 7:8, :] if f < 5 else sv[f - 2, k, 7:8, :]
                yh[f, k] = jnp.broadcast_to(source, (8, 128))

    for out, flow, metric in raw_rows(1):
        halo = flow if flow is not None else 5 + metric
        for k in range(4):
            base = 14 * k
            ey[out, base : base + 3, :] = yl[halo, k, 5:8, :]
            ey[out, base + 3 : base + 11, :] = qv[flow, k] if flow is not None else sv[3 + metric, k]
            ey[out, base + 11 : base + 14, :] = yh[halo, k, 0:3, :]
        ey[out, 56:64, :] = qv[flow, 3] if flow is not None else sv[3 + metric, 3]

    def fill_y(k, carry):
        fill(ey, (pl.ds(pl.multiple_of(8 * k, 8), 8),))
        return carry

    lax.fori_loop(0, 8, fill_y, 0)

    def face_y(k, carry):
        cache = {}

        def get(r, cell):
            if (r, cell) not in cache:
                cache[(r, cell)] = ey[r, pl.ds(8 * k + cell, 8), :]
            return cache[(r, cell)]

        flux = face_flux(get)
        for m in range(5):
            fy[m, pl.ds(pl.multiple_of(8 * k, 8), 8), :] = flux[m]
        return carry

    lax.fori_loop(0, 7, face_y, 0)
    cyclic = order_of(1)
    for k in range(4):
        for m in range(5):
            target = 1 + cyclic[m - 1] if 1 <= m <= 3 else m
            acc[target, k] += fy[m, 14 * k + 1 : 14 * k + 9, :] - fy[m, 14 * k : 14 * k + 8, :]

    def fill_z(first, last):
        def body(k, carry):
            fill(ez, (k,))
            return carry

        lax.fori_loop(first, last, body, 0)

    def take_plane(halo_ref, cell, plane):
        for out, flow, metric in raw_rows(2):
            halo = flow if flow is not None else 5 + metric
            ez[out, cell] = halo_ref[halo, plane]

    def land(halo_ref, cell, plane):
        cyclic = order_of(2)
        fields = [halo_ref[m, plane] for m in (0, 1 + cyclic[0], 1 + cyclic[1], 1 + cyclic[2], 4)]
        metric = [halo_ref[5 + member, plane] for member in cyclic]
        for m in range(5):
            ez[m, cell] = fields[m]
        for m in range(3):
            ez[ROW + m, cell] = metric[m]
        put_terms(ez, (cell,), fields, metric)

    def take_z(halo_ref, base, low):
        for k in range(3):
            take_plane(halo_ref, base + k, low + k)

    def face_z(k, carry):
        cache = {}

        def get(r, cell):
            if (r, cell) not in cache:
                cache[(r, cell)] = ez[r, k + cell]
            return cache[(r, cell)]

        flux = face_flux(get)
        for m in range(5):
            fz[m, k] = flux[m]
        return carry

    for out, flow, metric in raw_rows(2):
        for k in range(4):
            ez[out, 3 + k] = qv[flow, k] if flow is not None else sv[6 + metric, k]
    fill_z(3, 7)

    def low_z():
        take_z(zl, 0, 1)
        fill_z(0, 3)

    def high_z():
        take_z(zh, 7, 0)
        fill_z(7, 10)

    arrive(2, ((14, 4, relay), (16, 3, not_(jnp.logical_or(relay, edge))), (8, 3, edge)))

    @pl.when(not_(edge_low))
    def _():
        low_z()

    @pl.when(not_(edge_high))
    def _():
        high_z()

    early_first = jnp.where(edge_low, 3, 0)
    early_last = jnp.where(edge_low, 5, jnp.where(edge_high, 2, 5))
    lax.fori_loop(early_first, early_last, face_z, 0)

    @pl.when(lone)
    def _():
        pl.semaphore_wait(word, 1)
        send_far()

    extra = both(edge, both(not_(late), not_(lone)))
    for direction, fields, amount, there in (
        (0, 16, 4, not_(x_end)),
        (0, 8, 4, x_end),
        (1, 16, 4, not_(top)),
        (1, 8, 4, top),
        (2, 16, 3, not_(edge)),
        (2, 8, 4, extra),
        (2, 8, 3, both(edge, not_(extra))),
    ):
        @pl.when(there)
        def _():
            all_of(direction, fields, amount).wait_send()

    spanwise = order_of(2)

    def finish(k):
        for m in range(5):
            target = 1 + spanwise[m - 1] if 1 <= m <= 3 else m
            rate = -iv[k] * (acc[target, k] + (fz[m, k + 1] - fz[m, k]))
            rate_out[target, k] = rate
            state_out[target, k] = qv[target, k] + STEP_SIZE * rate

    @pl.when(not_(edge))
    def _():
        for k in range(4):
            finish(k)

    @pl.when(edge)
    def _():
        finish(jnp.where(edge_low, 3, 0))

        def body(stage, carry):
            @pl.when(edge_low)
            def _():
                far_arrive(ZL, stage)
                land(zl, 2 - stage, 3 - stage)

            @pl.when(edge_high)
            def _():
                far_arrive(ZH, stage)
                land(zh, 7 + stage, stage)

            carry = face_z(jnp.where(edge_low, 2 - stage, 2 + stage), carry)
            finish(jnp.where(edge_low, 2 - stage, 1 + stage))
            return carry

        lax.fori_loop(0, 3, body, 0)

    @pl.when(both(relay, y == 1))
    def _():
        pl.semaphore_wait(word, 1)

        @pl.when(turn == 3)
        def _():
            pl.delay(1000)

        @pl.when(turn == 5)
        def _():
            pl.delay(2000)

        for copy in far_copies(ZH, zl.at[pl.ds(0, 5)], zl.at[pl.ds(5, 3)], beyond):
            copy.start()

    @pl.when(both(relay, y == 6))
    def _():
        pl.semaphore_wait(word, 1)
        for copy in far_copies(ZL, zh.at[pl.ds(0, 5)], zh.at[pl.ds(5, 3)], beyond):
            copy.start()

    @pl.when(jnp.logical_or(jnp.logical_or(relay, detour_at), jnp.logical_or(far_late, lone)))
    def _():
        far_sent()


def deliver(state, rate, state_out, rate_out, sem):
    whole = [
        pltpu.make_async_copy(state, state_out, sem.at[0]),
        pltpu.make_async_copy(rate, rate_out, sem.at[1]),
    ]
    for m in range(state.shape[0]):
        pltpu.make_async_copy(state.at[m], state_out.at[m], sem.at[0]).start()
        pltpu.make_async_copy(rate.at[m], rate_out.at[m], sem.at[1]).start()
    for copy in whole:
        copy.wait()


def local(conserved, metrics, inv_volume, wake_donor):
    block = conserved.shape
    planes, rows, lanes = block[1:]
    wide = pltpu.VMEM(block, jnp.float32)
    f32 = lambda *shape: pltpu.VMEM(shape, jnp.float32)
    rate, state = pl.pallas_call(
        kernel,
        out_shape=(wide, wide),
        in_specs=[pl.BlockSpec(memory_space=pltpu.HBM)] * 4,
        out_specs=[pl.BlockSpec(memory_space=pltpu.VMEM)] * 2,
        scratch_shapes=[
            f32(*block),
            f32(9, planes, rows, lanes),
            f32(planes, rows, lanes),
            pltpu.VMEM((1, lanes), jnp.int32),
            *[f32(8, planes, rows, lanes)] * 4,
            *[f32(8, planes, rows, lanes)] * 2,
            *[f32(8, planes, rows, lanes)] * 2,
            f32(CELL_ROWS, 5, rows, lanes),
            f32(CELL_ROWS, 5, rows, lanes),
            f32(CELL_ROWS, 64, lanes),
            f32(CELL_ROWS, 10, rows, lanes),
            f32(5, 5, rows, lanes),
            f32(5, 56, lanes),
            f32(5, 5, rows, lanes),
            f32(*block),
            pltpu.SemaphoreType.DMA((3,)),
            pltpu.SemaphoreType.DMA((3,)),
            pltpu.SemaphoreType.DMA((2,)),
            pltpu.SemaphoreType.DMA,
            pltpu.SemaphoreType.DMA((3,)),
            pltpu.SemaphoreType.REGULAR,
        ],
        compiler_params=pltpu.CompilerParams(collective_id=0, has_side_effects=True),
    )(conserved, metrics, inv_volume, wake_donor[None])
    return pl.pallas_call(
        deliver,
        out_shape=(jax.ShapeDtypeStruct(block, jnp.float32),) * 2,
        in_specs=[pl.BlockSpec(memory_space=pl.ANY)] * 2,
        out_specs=[pl.BlockSpec(memory_space=pltpu.HBM)] * 2,
        scratch_shapes=[pltpu.SemaphoreType.DMA((2,))],
    )(pltpu.with_memory_space_constraint(state, pltpu.VMEM), pltpu.with_memory_space_constraint(rate, pltpu.VMEM))


def solution(mesh):
    placed = (P(None, "gz", "gy", "gx"), P(None, "gz", "gy", "gx"), P("gz", "gy", "gx"), P("gx"))
    return jax.shard_map(
        local,
        mesh=mesh,
        in_specs=placed,
        out_specs=(P(None, "gz", "gy", "gx"), P(None, "gz", "gy", "gx")),
        check_vma=False,
    )
```
